256 devices in a mesh: grp: 2 (over core), slab: 4 (over z_hi), col: 32 (over x, z_lo, y).
Axes of the slice: x: 4, y: 4, z: 8 (z_hi: 4, z_lo: 2; z = z_hi * 2 + z_lo), core: 2. Of those that a mesh axis runs over, the one named last changes fastest.
Arguments:
- solution: float32 [512, 65536], P('slab', ('grp', 'col')), may hold values from -6 to 6
- residual: float32 [512, 65536], P('slab', ('grp', 'col')), may hold values from -0.6 to 0.6
- direction: float32 [512, 65536], P('slab', ('grp', 'col')), may hold values from -6 to 6
- row_taps: float32 [31], replicated, may hold values from 0.2 to 1
- col_taps: float32 [31], replicated, may hold values from 0.2 to 1
- damping: float32 [], replicated, may hold values from 0.01 to 0.05
- rho: float32 [], replicated, may hold values from 671088.6 to 2013265.9
- coarse_diag: float32 [4], replicated, may hold values from 0.9 to 1.6
- coarse_coupling: float32 [4], replicated, may hold values from 0.05 to 0.2
Outputs:
- new_solution: float32 [512, 65536], P('slab', ('grp', 'col'))
- new_residual: float32 [512, 65536], P('slab', ('grp', 'col'))
- precond: float32 [512, 65536], P('slab', ('grp', 'col'))
- new_direction: float32 [512, 65536], P('slab', ('grp', 'col'))
- energy: float32 [], replicated
The draws below stay inside these ranges and needn't reach their ends.
All inputs are finite; a program needn't handle non-finite values.
Results may differ from the reference program's by a relative error of at most 0.0001.
Values sent between devices are 32-bit elements; how exact they have to be, the bound alone decides.
No kernel may reach another device: no remote copies, remote signals or barrier semaphores. Data moves between devices by JAX's collectives and lax.ppermute only.
A program may use at most 128 MiB of HBM per device.

```python
import math
import jax
import jax.numpy as jnp
from jax import lax

TAPS = 31
SWEEPS = 3
LEVELS = 4
COARSE_SWEEPS = 4
ROWS = 512
COLS = 65536


def shard_levels(own_key, dims, shards, smallest, largest):
    loudness = 1.0
    for dim, shards_of in shards:
        steps = jax.random.uniform(jax.random.fold_in(jax.random.fold_in(own_key, 6), dim), (shards_of,), jnp.float32, smallest / len(shards), largest / len(shards))
        loudness = loudness * jnp.repeat(jnp.exp(steps), dims[dim] // shards_of).reshape((-1,) + (1,) * (len(dims) - 1 - dim))
    return loudness


def centred(key, extent, scale, bound, pieces=(), kind=jnp.bfloat16):
    entries = jax.random.normal(key, extent, jnp.float32) * scale
    if len(pieces) > 0:
        entries = shard_levels(key, extent, pieces, -0.22, 0.18) * entries
    return jnp.clip(entries, min=-bound, max=bound).astype(kind)


def setup_inputs(seed: int = 0) -> dict:
    seeds = jax.random.split(jax.random.key(seed), 10)
    return {
        "solution": centred(seeds[0], (ROWS, COLS), 1.0, 6.0, ((0, 4), (1, 64)), jnp.float32),
        "residual": centred(seeds[1], (ROWS, COLS), 0.1, 0.6, ((0, 4), (1, 64)), jnp.float32),
        "direction": centred(seeds[2], (ROWS, COLS), 1.0, 6.0, ((0, 4), (1, 64)), jnp.float32),
        "row_taps": jnp.clip(jnp.exp(jax.random.uniform(seeds[3], (TAPS,), jnp.float32, math.log(0.2), math.log(1.0))), 0.2, 1.0),
        "col_taps": jnp.clip(jnp.exp(jax.random.uniform(seeds[4], (TAPS,), jnp.float32, math.log(0.2), math.log(1.0))), 0.2, 1.0),
        "damping": jnp.clip(jnp.exp(jax.random.uniform(seeds[5], (), jnp.float32, math.log(0.01), math.log(0.05))), 0.01, 0.05),
        "rho": jnp.clip(jnp.exp(jax.random.uniform(seeds[6], (), jnp.float32, math.log(671088.6), math.log(2013265.9))), 671088.6, 2013265.9),
        "coarse_diag": jnp.clip(jnp.exp(jax.random.uniform(seeds[7], (LEVELS,), jnp.float32, math.log(0.9), math.log(1.6))), 0.9, 1.6),
        "coarse_coupling": jnp.clip(jax.random.uniform(seeds[8], (LEVELS,), jnp.float32, 0.05, 0.2), 0.05, 0.2),
    }


relaxation = 2.0 / 3.0


def band_matrix(taps, out_len, in_len):
    offsets = jnp.arange(in_len)[None, :] - jnp.arange(out_len)[:, None]
    onehot = (offsets[:, :, None] == jnp.arange(taps.shape[0])[None, None, :]).astype(taps.dtype)
    return jnp.einsum("ijt,t->ij", onehot, taps, precision=lax.Precision.HIGHEST)


def blur_cols(padded, taps, length):
    height = padded.shape[0]
    blocks = -(-length // 128)
    extra = blocks * 128 + 128 - padded.shape[1]
    padded = jnp.pad(padded, ((0, 0), (0, extra)))
    main = padded[:, :blocks * 128].reshape(height, blocks, 128)
    tail = padded[:, 128:blocks * 128 + 128].reshape(height, blocks, 128)[:, :, :taps.shape[0] - 1]
    window = jnp.concatenate([main, tail], axis=2)
    matrix = band_matrix(taps, 128, 128 + taps.shape[0] - 1).T
    result = jnp.einsum("rbk,kc->rbc", window, matrix, precision=lax.Precision.HIGHEST)
    return result.reshape(height, blocks * 128)[:, :length]


def blur_rows(padded, taps, length):
    matrix = band_matrix(taps, length, length + taps.shape[0] - 1)
    return jnp.dot(matrix, padded, precision=lax.Precision.HIGHEST)


def apply_operator(field, row_norm, col_norm, damping):
    reach = row_norm.shape[0] // 2
    height, width = field.shape
    section = blur_cols(jnp.pad(field, ((0, 0), (reach, reach))), col_norm, width)
    section = blur_cols(jnp.pad(section, ((0, 0), (reach, reach))), col_norm[::-1], width)
    section = blur_rows(jnp.pad(section, ((reach, reach), (0, 0))), row_norm, height)
    section = blur_rows(jnp.pad(section, ((reach, reach), (0, 0))), row_norm[::-1], height)
    return section + damping * field


def coarse_operator(field, diag_value, coupling):
    padded = jnp.pad(field, 1)
    beside_all = padded[2:, 1:-1] + padded[:-2, 1:-1] + padded[1:-1, 2:] + padded[1:-1, :-2]
    return diag_value * field - coupling * beside_all


def restrict_by(field, factor, divisor):
    height, width = field.shape
    return field.reshape(height // factor, factor, width // factor, factor).sum(axis=(1, 3)) / divisor


def prolong_by(field, factor):
    height, width = field.shape
    spread = jnp.broadcast_to(field[:, None, :, None], (height, factor, width, factor))
    return spread.reshape(height * factor, width * factor)


def cycle(rhs, level, coarse_diag, coarse_coupling):
    diag_value = coarse_diag[level]
    coupling = coarse_coupling[level]
    guess = relaxation * rhs / diag_value
    if level == LEVELS - 1:
        for sweep in range(COARSE_SWEEPS - 1):
            guess = guess + relaxation * (rhs - coarse_operator(guess, diag_value, coupling)) / diag_value
        return guess
    lower = restrict_by(rhs - coarse_operator(guess, diag_value, coupling), 2, 2.0)
    guess = guess + prolong_by(cycle(lower, level + 1, coarse_diag, coarse_coupling), 2)
    return guess + relaxation * (rhs - coarse_operator(guess, diag_value, coupling)) / diag_value


def reference(solution, residual, direction, row_taps, col_taps, damping, rho, coarse_diag, coarse_coupling):
    row_norm = row_taps / jnp.sum(row_taps)
    col_norm = col_taps / jnp.sum(col_taps)
    image = apply_operator(direction, row_norm, col_norm, damping)
    alpha = rho / jnp.sum(direction * image)
    new_solution = solution + alpha * direction
    new_residual = residual - alpha * image
    scale = relaxation / (1.0 + damping)
    smooth = scale * new_residual
    for sweep in range(SWEEPS - 1):
        smooth = smooth + scale * (new_residual - apply_operator(smooth, row_norm, col_norm, damping))
    coarse = cycle(restrict_by(new_residual, 4, 4.0), 0, coarse_diag, coarse_coupling)
    precond = smooth + prolong_by(coarse, 4)
    energy = jnp.sum(new_residual * precond)
    new_direction = precond + (energy / rho) * direction
    return new_solution, new_residual, precond, new_direction, energy
```

```python
import jax
import jax.numpy as jnp
from jax import lax
from jax.experimental import pallas as pl
from jax.experimental.pallas import tpu as pltpu
from jax.sharding import PartitionSpec as P

INTERPRET = False
W = 2.0 / 3.0
TAPS = 31
H = TAPS // 2
ROWS, COLS = 128, 1024
EXT = COLS + 256
WIN = ROWS + 128
DR, RR = 64, 32
IN0 = (0, 128, 384, 640, 768)
VARIANT = (0, 1, 1, 1, 2)
GC = ("grp", "col")
ALL = ("grp", "slab", "col")
F32, BF16 = jnp.float32, jnp.bfloat16


def iota(shape, dim):
    return lax.broadcasted_iota(jnp.int32, shape, dim)


def split(x):
    high = x.astype(BF16)
    return high, (x - high.astype(F32)).astype(BF16)


def dot(a, b):
    return jnp.dot(a, b, preferred_element_type=F32)


def dot3(a, b):
    (ah, al), (bh, bl) = a, b
    return dot(ah, bh) + (dot(ah, bl) + dot(al, bh))


def dot2(a, b):
    return dot(a[0], b) + dot(a[1], b)


def dot2r(a, b):
    return dot(a, b[0]) + dot(a, b[1])


def hot(cond):
    return jnp.where(cond, 1.0, 0.0).astype(BF16)


def total(x):
    return jnp.sum(jnp.sum(x, axis=0, keepdims=True), axis=1, keepdims=True)


def gram(taps, nwin, base, limit, k_ref, kt_ref):
    nm = nwin + 256
    row, lane = iota((128, 384), 0), iota((128, 384), 1)
    off = lane - 128 - row
    block = jnp.zeros((128, 384), F32)
    block_t = jnp.zeros((128, 384), F32)
    for t in range(TAPS):
        block = jnp.where(off == t - H, taps[t], block)
        block_t = jnp.where(off == H - t, taps[t], block_t)
    k_ref[0:nm, 0:nwin] = jnp.zeros((nm, nwin), F32)
    kt_ref[0:nwin, 0:nm] = jnp.zeros((nwin, nm), F32)
    for b in range(nm // 128):
        lo, hi = max(0, 128 * b - 256), min(nwin, 128 * b + 128)
        first = 128 * b - 256
        k_ref[128 * b : 128 * b + 128, lo:hi] = block[:, lo - first : hi - first]
    for b in range(nwin // 128):
        kt_ref[128 * b : 128 * b + 128, 128 * b : 128 * b + 384] = block_t


def gram_at(nwin, base, limit, k_ref, kt_ref):
    nm = nwin + 256
    kt = kt_ref[0:nwin, 0:nm]
    k = k_ref[0:nm, 0:nwin]
    if base is None:
        return dot3(split(kt), split(k))
    m = iota((nwin, nm), 1) + (base - 128)
    kt = jnp.where((m >= 0) & (m < limit), kt, 0.0)
    g = dot3(split(kt), split(k))
    i, o = iota((nwin, nwin), 0) + base, iota((nwin, nwin), 1) + base
    return jnp.where((i >= 0) & (i < limit) & (o >= 0) & (o < limit), g, 0.0)


def matrices_kernel(n_slab, n_gc):
    def kernel(idx, rt, ct, lh, ll, gh, gl, rc0, rc1, rc2, rc3, pc0, pc1, pc2, pc3, k_ref, kt_ref):
        slab, gc = idx[0], idx[1]
        gram(rt, WIN, None, None, k_ref, kt_ref)
        g1 = gram_at(WIN, slab * ROWS - 64, n_slab * ROWS, k_ref, kt_ref)
        g1s = split(g1)
        lh[0:128, :], ll[0:128, :] = g1s[0][64:192, :], g1s[1][64:192, :]
        c, i = iota((48, WIN), 0), iota((48, WIN), 1)
        rr = jnp.where((i - 32 >= 4 * c) & (i - 32 < 4 * c + 4), 0.25, 0.0).astype(BF16)
        lh[128:176, :], ll[128:176, :] = split(dot2r(rr, g1s))
        lh[176:224, :], ll[176:224, :] = rr, jnp.zeros_like(rr)
        tile = (g1s[0][64:192, :], g1s[1][64:192, :])
        lh[224:352, :], ll[224:352, :] = split(dot3(tile, g1s))
        gram(ct, 512, None, None, k_ref, kt_ref)
        start = gc * COLS - 128
        for v, (base, off) in enumerate(((start, 0), (None, 128), (start + 768, 256))):
            g1 = gram_at(512, base, n_gc * COLS, k_ref, kt_ref)
            g1s = split(g1)
            out = (g1s[0][:, off : off + 256], g1s[1][:, off : off + 256])
            gh[2 * v], gl[2 * v] = out
            gh[2 * v + 1], gl[2 * v + 1] = split(dot3(g1s, out))
        rc0[...] = hot((iota((EXT, 384), 0) >> 2) + 32 == iota((EXT, 384), 1))
        rc1[...] = hot((iota((384, 256), 0) >> 1) == iota((384, 256), 1))
        rc2[...] = hot((iota((256, 128), 0) >> 1) == iota((256, 128), 1))
        rc3[...] = hot((iota((128, 128), 0) >> 1) - 8 == (iota((128, 128), 1) & 31))
        pc0[...] = hot(iota((384, COLS), 0) == (iota((384, COLS), 1) >> 2) + 64)
        pc1[...] = hot(iota((256, 384), 0) == (iota((256, 384), 1) >> 1))
        pc2[...] = hot(iota((128, 256), 0) == (iota((128, 256), 1) >> 1))
        pc3[...] = hot(iota((128, 128), 0) == (iota((128, 128), 1) >> 1))

    return kernel


def level_mask(level, shape, slab, gc, n_slab, n_gc):
    height, width = 32 >> level, 256 >> level
    i = iota(shape, 0) - (8 >> level) + slab * height
    j = iota(shape, 1) - (64 >> level) + gc * width
    return (i >= 0) & (i < n_slab * height) & (j >= 0) & (j < n_gc * width)


def tile_mask(level, shape):
    i, j = iota(shape, 0) - (8 >> level), iota(shape, 1) - (64 >> level)
    return (i >= 0) & (i < 32 >> level) & (j >= 0) & (j < 256 >> level)


def beside(v):
    n, m = v.shape
    rows = pltpu.roll(v, 1, 0) + pltpu.roll(v, n - 1, 0)
    return rows + pltpu.roll(v, 1, 1) + pltpu.roll(v, m - 1, 1)


def operator(v, dg, cp):
    return dg * v - cp * beside(v)


def halo_kernel(n_slab, n_gc):
    n_dev = n_slab * n_gc

    def kernel(idx, par, d, r, row_u, row_d, col_l, col_r, cor_u, cor_d, lh, ll, gh, gl, rc0, rc1, rc2, rc3,
               q, d2, r1, e_up, e_dn, f0, f1, f2, pay, dh, dl, rh, rl, sh, sl, th, tl, c1):
        slab, gc = idx[0], idx[1]
        delta = par[0]
        c = par[1]

        def put(hi_ref, lo_ref, r0, c0, x):
            hi, lo = split(x)
            hi_ref[r0 : r0 + x.shape[0], c0 : c0 + x.shape[1]] = hi
            lo_ref[r0 : r0 + x.shape[0], c0 : c0 + x.shape[1]] = lo

        zero = jnp.zeros((32, EXT), BF16)
        for ref in (rh, rl):
            ref[0:32, :] = zero
            ref[WIN - 32 : WIN, :] = zero
        for at, n, hi, lo in ((0, DR, dh, dl), (1, RR, rh, rl)):
            tile = (d, r)[at]
            cols = slice(128 * at, 128 * at + 128)
            rows = (slice(0, DR), slice(DR, DR + RR))[at]
            put(hi, lo, 64, 128, tile[...])
            put(hi, lo, 64, 0, col_l[:, cols])
            put(hi, lo, 64, 128 + COLS, col_r[:, cols])
            for first, main, corner in ((64 - n, row_u, cor_u), (192, row_d, cor_d)):
                put(hi, lo, first, 128, main[rows, :])
                put(hi, lo, first, 0, corner[rows, 0:128])
                put(hi, lo, first, 128 + COLS, corner[rows, 128:256])
        ds, rs = (dh[...], dl[...]), (rh[...], rl[...])

        def left(a, b):
            return (lh[a:b, :], ll[a:b, :])

        put(sh, sl, 0, 0, dot3(left(0, 176), ds))
        put(sh, sl, 176, 0, dot3(left(0, 128), rs))
        put(th, tl, 0, 0, dot3(left(224, 352), ds))
        rd = dot2r(lh[176:224, :], ds)
        rres = dot2r(lh[176:224, :], rs)
        for g in range(5):
            a, v, o = IN0[g], VARIANT[g], slice(256 * g, 256 * g + 256)
            c1[:, o] = dot3((sh[:, a : a + 512], sl[:, a : a + 512]), (gh[2 * v], gl[2 * v]))
            d2[:, o] = dot3((th[:, a : a + 512], tl[:, a : a + 512]), (gh[2 * v + 1], gl[2 * v + 1]))
        for o, dx, rx in (
            (slice(0, 128), col_l[:, 0:128], col_l[:, 128:256]),
            (slice(128, 128 + COLS), d[...], r[...]),
            (slice(128 + COLS, EXT), col_r[:, 0:128], col_r[:, 128:256]),
        ):
            p1 = c1[0:128, o]
            if o.start == 128:
                q[...] = p1 + delta * dx
            d2[:, o] = d2[:, o] + delta * (2.0 * p1 + delta * dx)
            r1[:, o] = c1[176:304, o] + delta * rx
        e_dn[0:32, :], e_dn[32:64, :] = d2[96:128, :], r1[96:128, :]
        e_up[0:32, :], e_up[32:64, :] = d2[0:32, :], r1[0:32, :]
        t = slice(128, 128 + COLS)
        qv, rv, aq, ar = q[...], r[...], d2[:, t], r1[:, t]
        s_dq = total(d[...] * qv)
        e_rr = total(rv * (3.0 * rv - 3.0 * c * ar) + c * c * (ar * ar)) * c
        e_qq = total(qv * (3.0 * qv - 3.0 * c * aq) + c * c * (aq * aq)) * c
        e_rq = total(rv * (3.0 * qv - 3.0 * c * aq) + c * c * (ar * aq)) * c
        fq = c1[128:176, :] + delta * rd
        f = dot2(split(jnp.concatenate([fq, rres], axis=0)), rc0[...])
        f0[...] = f
        pair = (f[0:48], f[48:96])
        weight = 4.0
        for level, cols in ((0, rc1), (1, rc2), (2, rc3)):
            dg, cp, sm = par[2 + level], par[6 + level], par[10 + level]
            shape = pair[0].shape
            inside = level_mask(level, shape, slab, gc, n_slab, n_gc)
            own = tile_mask(level, shape)
            bq, br = operator(pair[0], dg, cp), operator(pair[1], dg, cp)
            own_q, own_r = jnp.where(own, pair[0], 0.0), jnp.where(own, pair[1], 0.0)
            e_rr = e_rr + weight * total(own_r * (2.0 * sm * pair[1] - (sm * sm) * br))
            e_qq = e_qq + weight * total(own_q * (2.0 * sm * pair[0] - (sm * sm) * bq))
            e_rq = e_rq + weight * total(own_r * (2.0 * sm * pair[0] - (sm * sm) * bq))
            weight = 2.0 * weight
            rest_q = jnp.where(inside, pair[0] - sm * bq, 0.0)
            rest_r = jnp.where(inside, pair[1] - sm * br, 0.0)
            low = dot2(split(jnp.concatenate([rest_q, rest_r], axis=0)), cols[...])
            if level < 2:
                n, m = (24, 48) if level == 0 else (16, 24)
                half = jnp.where((iota((n, m), 1) >> 1) == iota((n, m), 0), 0.5, 0.0).astype(BF16)
                pair = (dot2r(half, split(low[0:m])), dot2r(half, split(low[m : 2 * m])))
                keep = level_mask(level + 1, pair[0].shape, slab, gc, n_slab, n_gc)
                pair = (jnp.where(keep, pair[0], 0.0), jnp.where(keep, pair[1], 0.0))
                out = (f1, f2)[level]
                out[0:n, :], out[n : 2 * n, :] = pair
        for ref in (e_up, e_dn):
            ref[64:72, 0:128], ref[64:72, 128:256] = pair[0][2:10, :], pair[1][2:10, :]
            ref[64:72, 256:EXT] = jnp.zeros((8, EXT - 256), F32)
        i, lane = iota((16, 128), 0), iota((16, 128), 1)
        pick = (i >= 2) & (i < 10) & (((i - 2) >> 1) == (lane >> 5))
        gq = jnp.sum(jnp.where(pick, low[0:16], 0.0), axis=0, keepdims=True) * 0.5
        gr = jnp.sum(jnp.where(pick, low[16:32], 0.0), axis=0, keepdims=True) * 0.5
        lane = iota((1, 128), 1)
        sums = jnp.zeros((1, 128), F32)
        for k, x in enumerate((s_dq, e_rr, e_rq, e_qq)):
            sums = jnp.where(lane == k, x, sums)
        pay[:, 0:128] = jnp.broadcast_to(gq, (n_dev, 128))
        pay[:, 128:256] = jnp.broadcast_to(gr, (n_dev, 128))
        pay[:, 256:384] = jnp.broadcast_to(sums, (n_dev, 128))

    return kernel


def final_kernel(n_slab, n_gc, n_grp):
    n_col = n_gc // n_grp

    def kernel(idx, par, got, sol, r, d, q, d2, r1, e_u, e_d, f0, f1, f2, lh, ll, gh, gl, pc0, pc1, pc2, pc3,
               o_sol, o_res, o_pre, o_dir, o_energy, uh, ul, yh, yl, vs, kk):
        slab, gc = idx[0], idx[1]
        delta, c, rho = par[0], par[1], par[14]
        lane = iota((1, 128), 1)
        sums = jnp.sum(got[:, 256:384], axis=0, keepdims=True)
        s_dq, e_rr, e_rq, e_qq = (
            jnp.sum(jnp.where(lane == k, sums, 0.0), axis=1, keepdims=True) for k in range(4)
        )
        alpha = rho / s_dq
        for ref in (uh, ul):
            ref[0:32, :] = jnp.zeros((32, EXT), BF16)
            ref[WIN - 32 : WIN, :] = jnp.zeros((32, EXT), BF16)
        for at, n, x in (
            (32, 32, e_u[32:64, :] - alpha * e_u[0:32, :]),
            (64, 128, r1[...] - alpha * d2[...]),
            (192, 32, e_d[32:64, :] - alpha * e_d[0:32, :]),
        ):
            uh[at : at + n, :], ul[at : at + n, :] = split(x)
        yh[...], yl[...] = split(dot3((lh[0:128, :], ll[0:128, :]), (uh[...], ul[...])))
        for g in range(5):
            a, v, o = IN0[g], VARIANT[g], slice(256 * g, 256 * g + 256)
            kk[:, o] = dot3((yh[:, a : a + 512], yl[:, a : a + 512]), (gh[2 * v], gl[2 * v]))
        dg, cp = par[5], par[9]
        first = (iota((n_gc, 128), 1) & 31) == 0
        last = (iota((n_gc, 128), 1) & 31) == 31
        top, bottom = iota((n_gc, 128), 1) < 32, iota((n_gc, 128), 1) >= 96
        left_end, right_end = iota((n_gc, 128), 0) == 0, iota((n_gc, 128), 0) == n_gc - 1
        rhs = []
        for s in range(n_slab):
            rows = []
            for g in range(n_grp):
                at = (g * n_slab + s) * n_col
                rows.append(got[at : at + n_col, 128:256] - alpha * got[at : at + n_col, 0:128])
            rhs.append(jnp.concatenate(rows, axis=0))
        zero = jnp.zeros((n_gc, 128), F32)
        v = [W * x / dg for x in rhs]
        for _ in range(3):
            ups = [pltpu.roll(x, 32, 1) for x in v]
            downs = [pltpu.roll(x, 96, 1) for x in v]
            new = []
            for s in range(n_slab):
                x = v[s]
                low = jnp.where(left_end, 0.0, pltpu.roll(pltpu.roll(x, 97, 1), 1, 0))
                high = jnp.where(right_end, 0.0, pltpu.roll(pltpu.roll(x, 31, 1), n_gc - 1, 0))
                near = jnp.where(first, low, pltpu.roll(x, 1, 1))
                near = near + jnp.where(last, high, pltpu.roll(x, 127, 1))
                near = near + jnp.where(top, ups[s - 1] if s > 0 else zero, ups[s])
                near = near + jnp.where(bottom, downs[s + 1] if s < n_slab - 1 else zero, downs[s])
                new.append(x + W * (rhs[s] - (dg * x - cp * near)) / dg)
            v = new
        e3 = total(sum(a * b for a, b in zip(rhs, v)))
        energy = e_rr - alpha * (2.0 * e_rq) + (alpha * alpha) * e_qq + 32.0 * e3
        o_energy[...] = energy
        pitch = n_gc + 16
        vs[...] = jnp.zeros(vs.shape, F32)
        for s in range(n_slab):
            at = (s + 1) * pitch + 8
            vs[at : at + n_gc, :] = v[s]
        v3 = jnp.zeros((8, 128), F32)
        lanes, rows8 = iota((1, 128), 1), iota((8, 128), 0)
        for k, i in ((-1, 3), (0, 0), (0, 1), (0, 2), (0, 3), (1, 0)):
            at = (slab + 1 + k) * pitch + 8 + gc
            mid, lo, hi = (vs[pl.ds(at + x, 1), :] for x in (0, -1, 1))
            line = pltpu.roll(mid, (8 - 32 * i) % 128, 1)
            line = jnp.where(lanes == 7, pltpu.roll(lo, (8 - 32 * i - 32) % 128, 1), line)
            line = jnp.where(lanes == 40, pltpu.roll(hi, (8 - 32 * i + 32) % 128, 1), line)
            line = jnp.where((lanes >= 7) & (lanes <= 40), line, 0.0)
            v3 = jnp.where(rows8 == 4 * k + i + 1, line, v3)
        up_q, up_r = e_u[64:72, 0:128], e_u[64:72, 128:256]
        dn_q, dn_r = e_d[64:72, 0:128], e_d[64:72, 128:256]
        edge_u, edge_d = up_r - alpha * up_q, dn_r - alpha * dn_q
        own = f2[16:32, :] - alpha * f2[0:16, :]
        row = iota((16, 128), 0)
        own = jnp.where(row == 0, edge_u[6:7, :], jnp.where(row == 1, edge_u[7:8, :], own))
        own = jnp.where(row == 10, edge_d[0:1, :], jnp.where(row == 11, edge_d[1:2, :], own))
        own = jnp.where(row < 12, own, 0.0)
        f = [f0[48:96, :] - alpha * f0[0:48, :], f1[24:48, :] - alpha * f1[0:24, :], own]
        low = v3
        for level, cols in ((2, pc3), (1, pc2), (0, pc1)):
            dg, cp, sm = par[2 + level], par[6 + level], par[10 + level]
            n, m = f[level].shape[0], low.shape[0]
            double = hot((iota((n, m), 0) >> 1) == iota((n, m), 1))
            wide = dot2r(double, split(dot2(split(low), cols[...])))
            inside = level_mask(level, f[level].shape, slab, gc, n_slab, n_gc)
            x = jnp.where(inside, sm * f[level] + wide, 0.0)
            low = jnp.where(inside, x + sm * (f[level] - operator(x, dg, cp)), 0.0)
        four = hot((iota((ROWS, 48), 0) >> 2) + 8 == iota((ROWS, 48), 1))
        t = slice(128, 128 + COLS)
        spread = split(dot2r(four, split(low)))
        u = r[...] - alpha * q[...]
        o_res[...] = u
        au = r1[:, t] - alpha * d2[:, t]
        smooth = c * (3.0 * u - (3.0 * c) * au + (c * c) * (kk[:, t] + delta * au))
        pre = smooth + dot2(spread, pc0[...])
        o_pre[...] = pre
        o_sol[...] = sol[...] + alpha * d[...]
        o_dir[...] = pre + (energy / rho) * d[...]

    return kernel


def call(kernel, outs, scratch, n_smem, n_args, name):
    smem, vmem = pl.BlockSpec(memory_space=pltpu.SMEM), pl.BlockSpec(memory_space=pltpu.VMEM)
    return pl.pallas_call(
        kernel,
        out_shape=[jax.ShapeDtypeStruct(s, t) for s, t in outs],
        in_specs=[smem] * n_smem + [vmem] * (n_args - n_smem),
        out_specs=[vmem] * len(outs),
        scratch_shapes=[pltpu.VMEM(s, t) for s, t in scratch],
        compiler_params=pltpu.CompilerParams(vmem_limit_bytes=48 * 1024 * 1024),
        interpret=INTERPRET,
        name=name,
    )


def solution(mesh):
    n_grp, n_slab, n_col = mesh.shape["grp"], mesh.shape["slab"], mesh.shape["col"]
    n_gc = n_grp * n_col
    n_dev = n_slab * n_gc

    def forward(n):
        return [(i, i + 1) for i in range(n - 1)]

    def backward(n):
        return [(i + 1, i) for i in range(n - 1)]

    def on_device(sol, r, d, row_taps, col_taps, damping, rho, diag, coupling):
        idx = jnp.stack([lax.axis_index("slab"), lax.axis_index(GC)]).astype(jnp.int32)
        row_d = jnp.concatenate([d[ROWS - DR :], r[ROWS - RR :]], axis=0)
        row_u = jnp.concatenate([d[:DR], r[:RR]], axis=0)
        from_u = lax.ppermute(row_d, "slab", forward(n_slab))
        from_d = lax.ppermute(row_u, "slab", backward(n_slab))
        col_r = jnp.concatenate([d[:, COLS - 128 :], r[:, COLS - 128 :]], axis=1)
        col_l = jnp.concatenate([d[:, :128], r[:, :128]], axis=1)
        from_l = lax.ppermute(col_r, GC, forward(n_gc))
        from_r = lax.ppermute(col_l, GC, backward(n_gc))

        def corner(dr, rr):
            top = jnp.concatenate([from_l[dr, :128], from_r[dr, :128]], axis=1)
            low = jnp.concatenate([from_l[rr, 128:], from_r[rr, 128:]], axis=1)
            return jnp.concatenate([top, low], axis=0)

        cor_u = lax.ppermute(corner(slice(ROWS - DR, ROWS), slice(ROWS - RR, ROWS)), "slab", forward(n_slab))
        cor_d = lax.ppermute(corner(slice(0, DR), slice(0, RR)), "slab", backward(n_slab))
        par = jnp.concatenate(
            [
                damping[None],
                (W / (1.0 + damping))[None],
                diag,
                coupling,
                W / diag,
                rho[None],
                jnp.zeros((1,), F32),
            ]
        )
        mats = call(
            matrices_kernel(n_slab, n_gc),
            [((352, WIN), BF16)] * 2
            + [((6, 512, 256), BF16)] * 2
            + [((EXT, 384), BF16), ((384, 256), BF16), ((256, 128), BF16), ((128, 128), BF16)]
            + [((384, COLS), BF16), ((256, 384), BF16), ((128, 256), BF16), ((128, 128), BF16)],
            [((768, 512), F32), ((512, 768), F32)],
            3,
            3,
            "matrices",
        )(idx, row_taps / jnp.sum(row_taps), col_taps / jnp.sum(col_taps))
        lh, ll, gh, gl, rc0, rc1, rc2, rc3, pc0, pc1, pc2, pc3 = mats
        q, d2, r1, e_up, e_dn, f0, f1, f2, pay = call(
            halo_kernel(n_slab, n_gc),
            [
                ((ROWS, COLS), F32),
                ((ROWS, EXT), F32),
                ((ROWS, EXT), F32),
                ((72, EXT), F32),
                ((72, EXT), F32),
                ((96, 384), F32),
                ((48, 256), F32),
                ((32, 128), F32),
                ((n_dev, 384), F32),
            ],
            [((WIN, EXT), BF16)] * 4 + [((304, EXT), BF16)] * 2 + [((128, EXT), BF16)] * 2 + [((304, EXT), F32)],
            2,
            18,
            "halo",
        )(idx, par, d, r, from_u, from_d, from_l, from_r, cor_u, cor_d, lh, ll, gh, gl, rc0, rc1, rc2, rc3)
        edge_u = lax.ppermute(e_dn, "slab", forward(n_slab))
        edge_d = lax.ppermute(e_up, "slab", backward(n_slab))
        got = lax.all_to_all(pay, ALL, 0, 0, tiled=True)
        n_sol, n_res, pre, n_dir, energy = call(
            final_kernel(n_slab, n_gc, n_grp),
            [((ROWS, COLS), F32)] * 4 + [((1, 1), F32)],
            [((WIN, EXT), BF16)] * 2
            + [((ROWS, EXT), BF16)] * 2
            + [(((n_slab + 2) * (n_gc + 16), 128), F32), ((ROWS, EXT), F32)],
            2,
            22,
            "final",
        )(idx, par, got, sol, r, d, q, d2, r1, edge_u, edge_d, f0, f1, f2, lh, ll, gh, gl, pc0, pc1, pc2, pc3)
        return n_sol, n_res, pre, n_dir, energy[0, 0]

    tile, rep = P("slab", GC), P()
    return jax.shard_map(
        on_device,
        mesh=mesh,
        in_specs=(tile,) * 3 + (rep,) * 6,
        out_specs=(tile,) * 4 + (rep,),
        check_vma=False,
    )
```

```python
import jax
import jax.numpy as jnp
from jax import lax
from jax.experimental import pallas as pl
from jax.experimental.pallas import tpu as pltpu
from jax.sharding import PartitionSpec as P


INTERPRET = False
W = 2.0 / 3.0
TAPS = 31
H = TAPS // 2
ROWS, COLS = 128, 1024
EXT = COLS + 256
WIN = ROWS + 128
DR, RR = 64, 32
IN0 = (0, 128, 384, 640, 768)
VARIANT = (0, 1, 1, 1, 2)
GC = ("grp", "col")
ALL = ("grp", "slab", "col")
F32, BF16 = jnp.float32, jnp.bfloat16


def iota(shape, dim):
    return lax.broadcasted_iota(jnp.int32, shape, dim)


def split(x):
    high = x.astype(BF16)
    return high, (x - high.astype(F32)).astype(BF16)


def dot(a, b):
    return jnp.dot(a, b, preferred_element_type=F32)


def dot3(a, b):
    (ah, al), (bh, bl) = a, b
    return dot(ah, bh) + (dot(ah, bl) + dot(al, bh))


def dot2(a, b):
    return dot(a[0], b) + dot(a[1], b)


def dot2r(a, b):
    return dot(a, b[0]) + dot(a, b[1])


def hot(cond):
    return jnp.where(cond, 1.0, 0.0).astype(BF16)


def total(x):
    return jnp.sum(jnp.sum(x, axis=0, keepdims=True), axis=1, keepdims=True)


def gram(taps, nwin, k_ref, kt_ref):
    nm = nwin + 256
    row, lane = iota((128, 384), 0), iota((128, 384), 1)
    off = lane - 128 - row
    block = jnp.zeros((128, 384), F32)
    block_t = jnp.zeros((128, 384), F32)
    for t in range(TAPS):
        block = jnp.where(off == t - H, taps[t], block)
        block_t = jnp.where(off == H - t, taps[t], block_t)
    k_ref[0:nm, 0:nwin] = jnp.zeros((nm, nwin), F32)
    kt_ref[0:nwin, 0:nm] = jnp.zeros((nwin, nm), F32)
    for b in range(nm // 128):
        lo, hi = max(0, 128 * b - 256), min(nwin, 128 * b + 128)
        first = 128 * b - 256
        k_ref[128 * b : 128 * b + 128, lo:hi] = block[:, lo - first : hi - first]
    for b in range(nwin // 128):
        kt_ref[128 * b : 128 * b + 128, 128 * b : 128 * b + 384] = block_t


def gram_at(nwin, base, limit, k_ref, kt_ref):
    nm = nwin + 256
    kt = kt_ref[0:nwin, 0:nm]
    k = k_ref[0:nm, 0:nwin]
    if base is None:
        return dot3(split(kt), split(k))
    m = iota((nwin, nm), 1) + (base - 128)
    kt = jnp.where((m >= 0) & (m < limit), kt, 0.0)
    g = dot3(split(kt), split(k))
    i, o = iota((nwin, nwin), 0) + base, iota((nwin, nwin), 1) + base
    return jnp.where((i >= 0) & (i < limit) & (o >= 0) & (o < limit), g, 0.0)


def matrices_kernel(n_slab, n_gc):
    def kernel(idx, rt, ct, *refs):
        outs, (k_ref, kt_ref), scratch, sem = refs[:12], refs[12:14], refs[14:26], refs[26]
        lh, ll, gh, gl, rc0, rc1, rc2, rc3, pc0, pc1, pc2, pc3 = scratch
        slab, gc = idx[0], idx[1]
        gram(rt, WIN, k_ref, kt_ref)
        g1 = gram_at(WIN, slab * ROWS - 64, n_slab * ROWS, k_ref, kt_ref)
        g1s = split(g1)
        lh[0:128, :], ll[0:128, :] = g1s[0][64:192, :], g1s[1][64:192, :]
        c, i = iota((48, WIN), 0), iota((48, WIN), 1)
        rr = jnp.where((i - 32 >= 4 * c) & (i - 32 < 4 * c + 4), 0.25, 0.0).astype(BF16)
        lh[128:176, :], ll[128:176, :] = split(dot2r(rr, g1s))
        lh[176:224, :], ll[176:224, :] = rr, jnp.zeros_like(rr)
        tile = (g1s[0][64:192, :], g1s[1][64:192, :])
        lh[224:352, :], ll[224:352, :] = split(dot3(tile, g1s))
        gram(ct, 512, k_ref, kt_ref)
        start = gc * COLS - 128
        for v, (base, off) in enumerate(((start, 0), (None, 128), (start + 768, 256))):
            g1 = gram_at(512, base, n_gc * COLS, k_ref, kt_ref)
            g1s = split(g1)
            out = (g1s[0][:, off : off + 256], g1s[1][:, off : off + 256])
            gh[v], gl[v] = out
            gh[3 + v], gl[3 + v] = split(dot3(g1s, out))
        rc0[...] = hot((iota((EXT, 384), 0) >> 2) + 32 == iota((EXT, 384), 1))
        rc1[...] = hot((iota((384, 256), 0) >> 1) == iota((384, 256), 1))
        rc2[...] = hot((iota((256, 128), 0) >> 1) == iota((256, 128), 1))
        rc3[...] = hot((iota((128, 128), 0) >> 1) - 8 == (iota((128, 128), 1) & 31))
        pc0[...] = hot(iota((384, COLS), 0) == (iota((384, COLS), 1) >> 2) + 64)
        pc1[...] = hot(iota((256, 384), 0) == (iota((256, 384), 1) >> 1))
        pc2[...] = hot(iota((128, 256), 0) == (iota((128, 256), 1) >> 1))
        pc3[...] = hot(iota((128, 128), 0) == (iota((128, 128), 1) >> 1))
        run_copies(sem, list(zip(scratch, outs)))

    return kernel


def level_mask(level, shape, slab, gc, n_slab, n_gc):
    height, width = 32 >> level, 256 >> level
    i = iota(shape, 0) - (8 >> level) + slab * height
    j = iota(shape, 1) - (64 >> level) + gc * width
    return (i >= 0) & (i < n_slab * height) & (j >= 0) & (j < n_gc * width)


def tile_mask(level, shape):
    i, j = iota(shape, 0) - (8 >> level), iota(shape, 1) - (64 >> level)
    return (i >= 0) & (i < 32 >> level) & (j >= 0) & (j < 256 >> level)


def beside(v):
    n, m = v.shape
    rows = pltpu.roll(v, 1, 0) + pltpu.roll(v, n - 1, 0)
    return rows + pltpu.roll(v, 1, 1) + pltpu.roll(v, m - 1, 1)


def operator(v, dg, cp):
    return dg * v - cp * beside(v)


def halo_kernel(n_slab, n_gc):
    n_dev = n_slab * n_gc

    def kernel(idx, par, d_in, r_in, row_u, row_d, col_l, col_r, cor_u, cor_d,
               lh_in, ll_in, gh_in, gl_in, rc0_in, rc1_in, rc2_in, rc3_in,
               q_out, d2_out, r1_out, f0_out, f1_out, f2_out, e_up, e_dn, pay,
               d, r, lh, ll, gh, gl, rc0, rc1, rc2, rc3, q, d2, r1, f0, f1, f2,
               dh, dl, rh, rl, sh, sl, th, tl, c1, sem):
        slab, gc = idx[0], idx[1]
        delta = par[0]
        c = par[1]
        ins, outs = [], []

        def copy(src, dst, todo):
            done = pltpu.make_async_copy(src, dst, sem.at[len(ins) + len(outs)])
            done.start()
            todo.append(done)

        for n, ref, main in ((DR, d, d_in), (RR, r, r_in)):
            copy(main, ref.at[:, pl.ds(128, COLS)], ins)
        for src, dst in ((lh_in, lh), (ll_in, ll), (gh_in, gh), (gl_in, gl), (rc0_in, rc0), (rc1_in, rc1), (rc2_in, rc2), (rc3_in, rc3)):
            copy(src, dst, ins)

        def put(hi_ref, lo_ref, r0, c0, x):
            hi, lo = split(x)
            hi_ref[r0 : r0 + x.shape[0], c0 : c0 + x.shape[1]] = hi
            lo_ref[r0 : r0 + x.shape[0], c0 : c0 + x.shape[1]] = lo

        zero = jnp.zeros((32, EXT), BF16)
        for ref in (rh, rl):
            ref[0:32, :] = zero
            ref[WIN - 32 : WIN, :] = zero
        for at, n, ref, hi, lo in ((0, DR, d, dh, dl), (1, RR, r, rh, rl)):
            cols = slice(128 * at, 128 * at + 128)
            rows = slice(DR * at, DR * at + n)
            ref[:, 0:128] = col_l[:, cols]
            ref[:, 128 + COLS :] = col_r[:, cols]
            for first, main, corner in ((64 - n, row_u, cor_u), (192, row_d, cor_d)):
                put(hi, lo, first, 128, main[rows, :])
                put(hi, lo, first, 0, corner[rows, 0:128])
                put(hi, lo, first, 128 + COLS, corner[rows, 128:256])
            ins[at].wait()
            put(hi, lo, 64, 0, ref[...])
        for done in ins[2:]:
            done.wait()
        ds, rs = (dh[...], dl[...]), (rh[...], rl[...])

        def left(a, b):
            return (lh[a:b, :], ll[a:b, :])

        put(sh, sl, 0, 0, dot3(left(0, 176), ds))
        put(sh, sl, 176, 0, dot3(left(0, 128), rs))
        put(th, tl, 0, 0, dot3(left(224, 352), ds))
        rd = dot2r(lh[176:224, :], ds)
        rres = dot2r(lh[176:224, :], rs)
        for g in range(5):
            a, v, o = IN0[g], VARIANT[g], slice(256 * g, 256 * g + 256)
            c1[:, o] = dot3((sh[:, a : a + 512], sl[:, a : a + 512]), (gh[v], gl[v]))
            d2[:, o] = dot3((th[:, a : a + 512], tl[:, a : a + 512]), (gh[3 + v], gl[3 + v]))
        t = slice(128, 128 + COLS)
        p1 = c1[0:128, :]
        q[...] = c1[0:128, t] + delta * d[:, t]
        d2[...] = d2[...] + delta * (2.0 * p1 + delta * d[...])
        r1[...] = c1[176:304, :] + delta * r[...]
        copy(q, q_out, outs)
        copy(d2, d2_out, outs)
        copy(r1, r1_out, outs)
        e_dn[0:32, :], e_dn[32:64, :] = d2[96:128, :], r1[96:128, :]
        e_up[0:32, :], e_up[32:64, :] = d2[0:32, :], r1[0:32, :]
        qv, rv, aq, ar = q[...], r[:, t], d2[:, t], r1[:, t]
        s_dq = total(d[:, t] * qv)
        e_rr = total(rv * (3.0 * rv - 3.0 * c * ar) + c * c * (ar * ar)) * c
        e_qq = total(qv * (3.0 * qv - 3.0 * c * aq) + c * c * (aq * aq)) * c
        e_rq = total(rv * (3.0 * qv - 3.0 * c * aq) + c * c * (ar * aq)) * c
        fq = c1[128:176, :] + delta * rd
        f = dot2(split(jnp.concatenate([fq, rres], axis=0)), rc0[...])
        f0[...] = f
        pair = (f[0:48], f[48:96])
        weight = 4.0
        for level, cols in ((0, rc1), (1, rc2), (2, rc3)):
            dg, cp, sm = par[2 + level], par[6 + level], par[10 + level]
            shape = pair[0].shape
            inside = level_mask(level, shape, slab, gc, n_slab, n_gc)
            mine = tile_mask(level, shape)
            bq, br = operator(pair[0], dg, cp), operator(pair[1], dg, cp)
            own_q, own_r = jnp.where(mine, pair[0], 0.0), jnp.where(mine, pair[1], 0.0)
            e_rr = e_rr + weight * total(own_r * (2.0 * sm * pair[1] - (sm * sm) * br))
            e_qq = e_qq + weight * total(own_q * (2.0 * sm * pair[0] - (sm * sm) * bq))
            e_rq = e_rq + weight * total(own_r * (2.0 * sm * pair[0] - (sm * sm) * bq))
            weight = 2.0 * weight
            rest_q = jnp.where(inside, pair[0] - sm * bq, 0.0)
            rest_r = jnp.where(inside, pair[1] - sm * br, 0.0)
            low = dot2(split(jnp.concatenate([rest_q, rest_r], axis=0)), cols[...])
            if level < 2:
                n, m = (24, 48) if level == 0 else (16, 24)
                half = jnp.where((iota((n, m), 1) >> 1) == iota((n, m), 0), 0.5, 0.0).astype(BF16)
                pair = (dot2r(half, split(low[0:m])), dot2r(half, split(low[m : 2 * m])))
                keep = level_mask(level + 1, pair[0].shape, slab, gc, n_slab, n_gc)
                pair = (jnp.where(keep, pair[0], 0.0), jnp.where(keep, pair[1], 0.0))
                out = (f1, f2)[level]
                out[0:n, :], out[n : 2 * n, :] = pair
        for ref in (e_up, e_dn):
            ref[64:72, 0:128], ref[64:72, 128:256] = pair[0][2:10, :], pair[1][2:10, :]
            ref[64:72, 256:EXT] = jnp.zeros((8, EXT - 256), F32)
        for src, dst in ((f0, f0_out), (f1, f1_out), (f2, f2_out)):
            copy(src, dst, outs)
        i, lane = iota((16, 128), 0), iota((16, 128), 1)
        pick = (i >= 2) & (i < 10) & (((i - 2) >> 1) == (lane >> 5))
        gq = jnp.sum(jnp.where(pick, low[0:16], 0.0), axis=0, keepdims=True) * 0.5
        gr = jnp.sum(jnp.where(pick, low[16:32], 0.0), axis=0, keepdims=True) * 0.5
        lane = iota((1, 128), 1)
        sums = jnp.zeros((1, 128), F32)
        for k, x in enumerate((s_dq, e_rr, e_rq, e_qq)):
            sums = jnp.where(lane == k, x, sums)
        pay[:, 0:128] = jnp.broadcast_to(gq, (n_dev, 128))
        pay[:, 128:256] = jnp.broadcast_to(gr, (n_dev, 128))
        pay[:, 256:384] = jnp.broadcast_to(sums, (n_dev, 128))
        for done in outs:
            done.wait()

    return kernel


def final_kernel(n_slab, n_gc, n_grp):
    n_col = n_gc // n_grp

    def kernel(idx, par, got, e_u, e_d, d2_in, r1_in, lh_in, ll_in, gh_in, gl_in, q_in, r_in, d_in, sol_in,
               f0_in, f1_in, f2_in, pc0_in, pc1_in, pc2_in, pc3_in,
               o_sol, o_res, o_pre, o_dir, o_energy,
               d2, r1, lh, ll, gh, gl, q, r, d, sol, f0, f1, f2, pc0, pc1, pc2, pc3,
               uh, ul, yh, yl, vs, kk, v_sol, v_res, v_pre, v_dir, sem):
        ins, outs = [], []

        def copy(src, dst, todo):
            done = pltpu.make_async_copy(src, dst, sem.at[len(ins) + len(outs)])
            done.start()
            todo.append(done)

        for src, dst in (
            (d2_in, d2), (r1_in, r1), (lh_in.at[pl.ds(0, 128), :], lh), (ll_in.at[pl.ds(0, 128), :], ll),
            (gh_in.at[pl.ds(0, 3)], gh), (gl_in.at[pl.ds(0, 3)], gl), (r_in, r), (q_in, q), (sol_in, sol), (d_in, d),
            (f0_in, f0), (f1_in, f1), (f2_in, f2), (pc1_in, pc1), (pc2_in, pc2), (pc3_in, pc3), (pc0_in, pc0),
        ):
            copy(src, dst, ins)
        slab, gc = idx[0], idx[1]
        delta, c, rho = par[0], par[1], par[14]
        lane = iota((1, 128), 1)
        sums = jnp.sum(got[:, 256:384], axis=0, keepdims=True)
        s_dq, e_rr, e_rq, e_qq = (
            jnp.sum(jnp.where(lane == k, sums, 0.0), axis=1, keepdims=True) for k in range(4)
        )
        alpha = rho / s_dq
        for done in ins:
            done.wait()
        v_sol[...] = sol[...] + alpha * d[...]
        copy(v_sol, o_sol, outs)
        u = r[...] - alpha * q[...]
        v_res[...] = u
        copy(v_res, o_res, outs)
        for ref in (uh, ul):
            ref[0:32, :] = jnp.zeros((32, EXT), BF16)
            ref[WIN - 32 : WIN, :] = jnp.zeros((32, EXT), BF16)
        for at, n, x in (
            (32, 32, e_u[32:64, :] - alpha * e_u[0:32, :]),
            (64, 128, r1[...] - alpha * d2[...]),
            (192, 32, e_d[32:64, :] - alpha * e_d[0:32, :]),
        ):
            uh[at : at + n, :], ul[at : at + n, :] = split(x)
        yh[...], yl[...] = split(dot3((lh[...], ll[...]), (uh[...], ul[...])))
        for g in range(5):
            a, v, o = IN0[g], VARIANT[g], slice(256 * g, 256 * g + 256)
            kk[:, o] = dot3((yh[:, a : a + 512], yl[:, a : a + 512]), (gh[v], gl[v]))
        dg, cp = par[5], par[9]
        first = (iota((n_gc, 128), 1) & 31) == 0
        last = (iota((n_gc, 128), 1) & 31) == 31
        top, bottom = iota((n_gc, 128), 1) < 32, iota((n_gc, 128), 1) >= 96
        left_end, right_end = iota((n_gc, 128), 0) == 0, iota((n_gc, 128), 0) == n_gc - 1
        rhs = []
        for s in range(n_slab):
            rows = []
            for g in range(n_grp):
                at = (g * n_slab + s) * n_col
                rows.append(got[at : at + n_col, 128:256] - alpha * got[at : at + n_col, 0:128])
            rhs.append(jnp.concatenate(rows, axis=0))
        zero = jnp.zeros((n_gc, 128), F32)
        v = [W * x / dg for x in rhs]
        for _ in range(3):
            ups = [pltpu.roll(x, 32, 1) for x in v]
            downs = [pltpu.roll(x, 96, 1) for x in v]
            new = []
            for s in range(n_slab):
                x = v[s]
                low = jnp.where(left_end, 0.0, pltpu.roll(pltpu.roll(x, 97, 1), 1, 0))
                high = jnp.where(right_end, 0.0, pltpu.roll(pltpu.roll(x, 31, 1), n_gc - 1, 0))
                near = jnp.where(first, low, pltpu.roll(x, 1, 1))
                near = near + jnp.where(last, high, pltpu.roll(x, 127, 1))
                near = near + jnp.where(top, ups[s - 1] if s > 0 else zero, ups[s])
                near = near + jnp.where(bottom, downs[s + 1] if s < n_slab - 1 else zero, downs[s])
                new.append(x + W * (rhs[s] - (dg * x - cp * near)) / dg)
            v = new
        e3 = total(sum(a * b for a, b in zip(rhs, v)))
        energy = e_rr - alpha * (2.0 * e_rq) + (alpha * alpha) * e_qq + 32.0 * e3
        o_energy[...] = energy
        pitch = n_gc + 16
        vs[...] = jnp.zeros(vs.shape, F32)
        for s in range(n_slab):
            at = (s + 1) * pitch + 8
            vs[at : at + n_gc, :] = v[s]
        v3 = jnp.zeros((8, 128), F32)
        lanes, rows8 = iota((1, 128), 1), iota((8, 128), 0)
        for k, i in ((-1, 3), (0, 0), (0, 1), (0, 2), (0, 3), (1, 0)):
            at = (slab + 1 + k) * pitch + 8 + gc
            mid, lo, hi = (vs[pl.ds(at + x, 1), :] for x in (0, -1, 1))
            line = pltpu.roll(mid, (8 - 32 * i) % 128, 1)
            line = jnp.where(lanes == 7, pltpu.roll(lo, (8 - 32 * i - 32) % 128, 1), line)
            line = jnp.where(lanes == 40, pltpu.roll(hi, (8 - 32 * i + 32) % 128, 1), line)
            line = jnp.where((lanes >= 7) & (lanes <= 40), line, 0.0)
            v3 = jnp.where(rows8 == 4 * k + i + 1, line, v3)
        up_q, up_r = e_u[64:72, 0:128], e_u[64:72, 128:256]
        dn_q, dn_r = e_d[64:72, 0:128], e_d[64:72, 128:256]
        edge_u, edge_d = up_r - alpha * up_q, dn_r - alpha * dn_q
        own = f2[16:32, :] - alpha * f2[0:16, :]
        row = iota((16, 128), 0)
        own = jnp.where(row == 0, edge_u[6:7, :], jnp.where(row == 1, edge_u[7:8, :], own))
        own = jnp.where(row == 10, edge_d[0:1, :], jnp.where(row == 11, edge_d[1:2, :], own))
        own = jnp.where(row < 12, own, 0.0)
        f = [f0[48:96, :] - alpha * f0[0:48, :], f1[24:48, :] - alpha * f1[0:24, :], own]
        low = v3
        for level, cols in ((2, pc3), (1, pc2), (0, pc1)):
            dg, cp, sm = par[2 + level], par[6 + level], par[10 + level]
            n, m = f[level].shape[0], low.shape[0]
            double = hot((iota((n, m), 0) >> 1) == iota((n, m), 1))
            wide = dot2r(double, split(dot2(split(low), cols[...])))
            inside = level_mask(level, f[level].shape, slab, gc, n_slab, n_gc)
            x = jnp.where(inside, sm * f[level] + wide, 0.0)
            low = jnp.where(inside, x + sm * (f[level] - operator(x, dg, cp)), 0.0)
        four = hot((iota((ROWS, 48), 0) >> 2) + 8 == iota((ROWS, 48), 1))
        t = slice(128, 128 + COLS)
        spread = split(dot2r(four, split(low)))
        au = r1[:, t] - alpha * d2[:, t]
        smooth = c * (3.0 * v_res[...] - (3.0 * c) * au + (c * c) * (kk[:, t] + delta * au))
        pre = smooth + dot2(spread, pc0[...])
        v_pre[...] = pre
        copy(v_pre, o_pre, outs)
        v_dir[...] = pre + (energy / rho) * d[...]
        copy(v_dir, o_dir, outs)
        for done in outs:
            done.wait()

    return kernel


def call(kernel, specs, outs, out_specs, scratch, sems=0):
    where = {"s": pltpu.SMEM, "v": pltpu.VMEM, "h": pltpu.HBM}
    if INTERPRET:
        where["h"] = pl.ANY

    def out(x, shape, kind):
        if x == "h" and not INTERPRET:
            return pltpu.HBM(shape, kind)
        return jax.ShapeDtypeStruct(shape, kind)

    run = pl.pallas_call(
        kernel,
        out_shape=[out(x, s, t) for x, (s, t) in zip(out_specs, outs)],
        in_specs=[pl.BlockSpec(memory_space=where[x]) for x in specs],
        out_specs=[pl.BlockSpec(memory_space=where[x]) for x in out_specs],
        scratch_shapes=[pltpu.VMEM(s, t) for s, t in scratch] + ([pltpu.SemaphoreType.DMA((sems,))] if sems else []),
        compiler_params=pltpu.CompilerParams(vmem_limit_bytes=40 * 1024 * 1024),
        interpret=INTERPRET,
    )

    def apply(*args):
        if INTERPRET:
            return run(*args)
        return run(*(pltpu.with_memory_space_constraint(a, pltpu.HBM) if x == "h" else a for x, a in zip(specs, args)))

    return apply


def run_copies(sem, pairs):
    todo = []
    for k, (src, dst) in enumerate(pairs):
        todo.append(pltpu.make_async_copy(src, dst, sem.at[k]))
        todo[-1].start()
    for done in todo:
        done.wait()


def edges_kernel(d, r, row_u, row_d, col_l, col_r, sem):
    pairs = []
    for n, at, x in ((DR, 0, d), (RR, DR, r)):
        pairs.append((x.at[pl.ds(0, n), :], row_u.at[pl.ds(at, n), :]))
        pairs.append((x.at[pl.ds(ROWS - n, n), :], row_d.at[pl.ds(at, n), :]))
    for at, x in ((0, d), (128, r)):
        pairs.append((x.at[:, pl.ds(0, 128)], col_l.at[:, pl.ds(at, 128)]))
        pairs.append((x.at[:, pl.ds(COLS - 128, 128)], col_r.at[:, pl.ds(at, 128)]))
    run_copies(sem, pairs)


def corners_kernel(from_l, from_r, after, cor_u, cor_d):
    for n, at, lane in ((DR, 0, 0), (RR, DR, 128)):
        for side, x in ((0, from_l), (128, from_r)):
            for first, out in ((0, cor_u), (ROWS - n, cor_d)):
                out[at : at + n, side : side + 128] = x[first : first + n, lane : lane + 128]


def solution(mesh):
    n_grp, n_slab, n_col = mesh.shape["grp"], mesh.shape["slab"], mesh.shape["col"]
    n_gc = n_grp * n_col
    n_dev = n_slab * n_gc

    def forward(n):
        return [(i, i + 1) for i in range(n - 1)]

    def backward(n):
        return [(i + 1, i) for i in range(n - 1)]

    def body(sol, r, d, row_taps, col_taps, damping, rho, diag, coupling):
        idx = jnp.stack([lax.axis_index("slab"), lax.axis_index(GC)]).astype(jnp.int32)
        row_u, row_d, col_l, col_r = call(
            edges_kernel, "hh", [((DR + RR, COLS), F32)] * 2 + [((ROWS, 256), F32)] * 2, "vvvv", [], 8
        )(d, r)
        from_u = lax.ppermute(row_d, "slab", forward(n_slab))
        from_d = lax.ppermute(row_u, "slab", backward(n_slab))
        from_l = lax.ppermute(col_r, GC, forward(n_gc))
        from_r = lax.ppermute(col_l, GC, backward(n_gc))
        par = jnp.concatenate(
            [
                damping[None],
                (W / (1.0 + damping))[None],
                diag,
                coupling,
                W / diag,
                rho[None],
                jnp.zeros((1,), F32),
            ]
        )
        mat_shapes = [((352, WIN), BF16)] * 2 + [((6, 512, 256), BF16)] * 2
        mat_shapes += [((EXT, 384), BF16), ((384, 256), BF16), ((256, 128), BF16), ((128, 128), BF16)]
        back_shapes = [((384, COLS), BF16), ((256, 384), BF16), ((128, 256), BF16), ((128, 128), BF16)]
        mats = call(
            matrices_kernel(n_slab, n_gc),
            "sss",
            mat_shapes + back_shapes,
            "h" * 12,
            [((768, 512), F32), ((512, 768), F32)] + mat_shapes + back_shapes,
            12,
        )(idx, row_taps / jnp.sum(row_taps), col_taps / jnp.sum(col_taps))
        lh, ll, gh, gl, rc0, rc1, rc2, rc3, pc0, pc1, pc2, pc3 = mats
        send_u, send_d = call(corners_kernel, "vvh", [((DR + RR, 256), F32)] * 2, "vv", [])(from_l, from_r, rc3)
        cor_u = lax.ppermute(send_d, "slab", forward(n_slab))
        cor_d = lax.ppermute(send_u, "slab", backward(n_slab))
        results = [((ROWS, COLS), F32), ((ROWS, EXT), F32), ((ROWS, EXT), F32)]
        results += [((96, 384), F32), ((48, 256), F32), ((32, 128), F32)]
        q, d2, r1, f0, f1, f2, e_up, e_dn, pay = call(
            halo_kernel(n_slab, n_gc),
            "sshh" + "v" * 6 + "h" * 8,
            results + [((72, EXT), F32)] * 2 + [((n_dev, 384), F32)],
            "h" * 6 + "vvv",
            [((ROWS, EXT), F32)] * 2
            + mat_shapes
            + results
            + [((WIN, EXT), BF16)] * 4
            + [((304, EXT), BF16)] * 2
            + [((128, EXT), BF16)] * 2
            + [((304, EXT), F32)],
            40,
        )(idx, par, d, r, from_u, from_d, from_l, from_r, cor_u, cor_d, lh, ll, gh, gl, rc0, rc1, rc2, rc3)
        edge_u = lax.ppermute(e_dn, "slab", forward(n_slab))
        edge_d = lax.ppermute(e_up, "slab", backward(n_slab))
        got = lax.all_to_all(pay, ALL, 0, 0, tiled=True)
        tile = ((ROWS, COLS), F32)
        n_sol, n_res, pre, n_dir, energy = call(
            final_kernel(n_slab, n_gc, n_grp),
            "ssvvv" + "h" * 17,
            [tile] * 4 + [((1, 1), F32)],
            "hhhhv",
            [((ROWS, EXT), F32)] * 2
            + [((128, WIN), BF16)] * 2
            + [((3, 512, 256), BF16)] * 2
            + [tile] * 4
            + [((96, 384), F32), ((48, 256), F32), ((32, 128), F32)]
            + back_shapes
            + [((WIN, EXT), BF16)] * 2
            + [((ROWS, EXT), BF16)] * 2
            + [(((n_slab + 2) * (n_gc + 16), 128), F32), ((ROWS, EXT), F32)]
            + [tile] * 4,
            24,
        )(idx, par, got, edge_u, edge_d, d2, r1, lh, ll, gh, gl, q, r, d, sol, f0, f1, f2, pc0, pc1, pc2, pc3)
        return n_sol, n_res, pre, n_dir, energy[0, 0]

    tile, rep = P("slab", GC), P()
    return jax.shard_map(
        body,
        mesh=mesh,
        in_specs=(tile,) * 3 + (rep,) * 6,
        out_specs=(tile,) * 4 + (rep,),
        check_vma=False,
    )
```

```python
import jax
import jax.numpy as jnp
from jax import lax
from jax.experimental import pallas as pl
from jax.experimental.pallas import tpu as pltpu
from jax.sharding import PartitionSpec as P


INTERPRET = False
W = 2.0 / 3.0
TAPS = 31
H = TAPS // 2
ROWS, COLS = 128, 1024
EXT = COLS + 256
WIN = ROWS + 128
DR, RR = 64, 32
IN0 = (0, 128, 384, 640, 768)
VARIANT = (0, 1, 1, 1, 2)
GC = ("grp", "col")
F32, BF16 = jnp.float32, jnp.bfloat16


def iota(shape, dim):
    return lax.broadcasted_iota(jnp.int32, shape, dim)


def split(x):
    high = x.astype(BF16)
    return high, (x - high.astype(F32)).astype(BF16)


def dot(a, b):
    return jnp.dot(a, b, preferred_element_type=F32)


def dot3(a, b):
    (ah, al), (bh, bl) = a, b
    return dot(ah, bh) + (dot(ah, bl) + dot(al, bh))


def dot2(a, b):
    return dot(a[0], b) + dot(a[1], b)


def dot2r(a, b):
    return dot(a, b[0]) + dot(a, b[1])


def hot(cond):
    return jnp.where(cond, 1.0, 0.0).astype(BF16)


def total(x):
    return jnp.sum(jnp.sum(x, axis=0, keepdims=True), axis=1, keepdims=True)


def dot_t(a, b):
    def nt(x, y):
        return lax.dot_general(x, y, (((1,), (1,)), ((), ())), preferred_element_type=F32)

    (ah, al), (bh, bl) = a, b
    return nt(ah, bh) + (nt(ah, bl) + nt(al, bh))


def toeplitz(taps):
    sum_taps = taps[0]
    for t in range(1, TAPS):
        sum_taps = sum_taps + taps[t]
    lane = iota((8, 384), 1)
    base = jnp.zeros((8, 384), F32)
    for t in range(TAPS):
        base = jnp.where(lane == 64 + H - t, taps[t], base)
    base = base / jnp.full((8, 384), sum_taps, F32)
    return pltpu.roll(jnp.broadcast_to(base[0:1], (256, 384)), 0, 1, stride=1, stride_axis=0)


def gram(kt, first, limit):
    ks = split(kt)
    left = ks
    if first is not None:
        m = iota((256, 384), 1) + (first - 128)
        left = split(jnp.where((m >= 0) & (m < limit), kt, 0.0))
    return left, ks


def block_powers(kt, first, limit):
    left, ks = gram(kt, first, limit)
    wide = dot_t(left, ks)
    g1 = dot_t(left, (ks[0][64:192], ks[1][64:192]))
    if first is not None:
        i = iota((256, 128), 0) + (first - 64)
        g1 = jnp.where((i >= 0) & (i < limit), g1, 0.0)
    g1s = split(g1)
    return g1s, split(dot3(split(wide), g1s))


def matrices_kernel(n_slab, n_gc):
    def kernel(idx, rt, ct, *refs):
        outs, scratch, sem = refs[:12], refs[12:24], refs[24]
        lh, ll, gh, gl, rc0, rc1, rc2, rc3, pc0, pc1, pc2, pc3 = scratch
        slab, gc = idx[0], idx[1]
        gh[...], gl[...] = jnp.zeros(gh.shape, BF16), jnp.zeros(gl.shape, BF16)
        kt = toeplitz(ct)
        inner = block_powers(kt, None, None)
        low = block_powers(kt, gc * COLS, n_gc * COLS)
        high = block_powers(kt, gc * COLS + COLS - 128, n_gc * COLS)
        has_l = jnp.where(gc > 0, 1.0, 0.0).astype(F32)
        has_r = jnp.where(gc < n_gc - 1, 1.0, 0.0).astype(F32)
        for power in range(2):
            for at, ref in enumerate((gh, gl)):
                mid = inner[power][at]
                wide = mid.astype(F32)
                outer_l, outer_r = (wide * has_l).astype(BF16), (wide * has_r).astype(BF16)
                for v, off, blocks in (
                    (0, 0, (outer_l, low[power][at])),
                    (1, 128, (mid, mid)),
                    (2, 256, (high[power][at], outer_r)),
                ):
                    for b in range(2):
                        start = off + 128 * b - 64
                        lo, hi = max(0, start), min(512, start + 256)
                        ref[3 * power + v, lo:hi, 128 * b : 128 * b + 128] = blocks[b][lo - start : hi - start]
        first, limit = slab * ROWS, n_slab * ROWS
        left, ks = gram(toeplitz(rt), first, limit)
        g1 = dot_t(left, ks)
        g1s = split(g1)
        lh[0:128, :], ll[0:128, :] = g1s[0][64:192, :], g1s[1][64:192, :]
        c, i = iota((48, WIN), 0), iota((48, WIN), 1)
        inside = (i + (first - 64) >= 0) & (i + (first - 64) < limit)
        rr = jnp.where((i - 32 >= 4 * c) & (i - 32 < 4 * c + 4) & inside, 0.25, 0.0).astype(BF16)
        lh[128:176, :], ll[128:176, :] = split(dot2r(rr, g1s))
        lh[176:224, :], ll[176:224, :] = rr, jnp.zeros_like(rr)
        k = iota((128, WIN), 1) + (first - 64)
        tile = split(jnp.where((k >= 0) & (k < limit), g1[64:192, :], 0.0))
        lh[224:352, :], ll[224:352, :] = split(dot3(tile, g1s))
        rc0[...] = hot((iota((EXT, 384), 0) >> 2) + 32 == iota((EXT, 384), 1))
        rc1[...] = hot((iota((384, 256), 0) >> 1) == iota((384, 256), 1))
        rc2[...] = hot((iota((256, 128), 0) >> 1) == iota((256, 128), 1))
        rc3[...] = hot((iota((128, 128), 0) >> 1) - 8 == (iota((128, 128), 1) & 31))
        pc0[...] = hot(iota((384, COLS), 0) == (iota((384, COLS), 1) >> 2) + 64)
        pc1[...] = hot(iota((256, 384), 0) == (iota((256, 384), 1) >> 1))
        pc2[...] = hot(iota((128, 256), 0) == (iota((128, 256), 1) >> 1))
        pc3[...] = hot(iota((128, 128), 0) == (iota((128, 128), 1) >> 1))
        run_copies(sem, list(zip(scratch, outs)))

    return kernel


def level_mask(level, shape, slab, gc, n_slab, n_gc):
    height, width = 32 >> level, 256 >> level
    i = iota(shape, 0) - (8 >> level) + slab * height
    j = iota(shape, 1) - (64 >> level) + gc * width
    return (i >= 0) & (i < n_slab * height) & (j >= 0) & (j < n_gc * width)


def tile_mask(level, shape):
    i, j = iota(shape, 0) - (8 >> level), iota(shape, 1) - (64 >> level)
    return (i >= 0) & (i < 32 >> level) & (j >= 0) & (j < 256 >> level)


def beside(v):
    n, m = v.shape
    rows = pltpu.roll(v, 1, 0) + pltpu.roll(v, n - 1, 0)
    return rows + pltpu.roll(v, 1, 1) + pltpu.roll(v, m - 1, 1)


def operator(v, dg, cp):
    return dg * v - cp * beside(v)


def halo_kernel(n_slab, n_gc, n_grp):
    n_dev = n_slab * n_gc // n_grp

    def kernel(idx, damping, rho_in, diag, coupling, d_in, r_in, row_u, row_d, col_l, col_r, cor_u, cor_d,
               lh_in, ll_in, gh_in, gl_in, rc0_in, rc1_in, rc2_in, rc3_in,
               q_out, d2_out, r1_out, f0_out, f1_out, f2_out, e_up, e_dn, pay,
               d, r, lh, ll, gh, gl, rc0, rc1, rc2, rc3, q, d2, r1, f0, f1, f2,
               dh, dl, rh, rl, sh, sl, th, tl, c1, sem):
        slab, gc = idx[0], idx[1]
        delta = damping[0]
        c = W / (1.0 + delta)
        ins, outs = [], []

        def copy(src, dst, todo):
            done = pltpu.make_async_copy(src, dst, sem.at[len(ins) + len(outs)])
            done.start()
            todo.append(done)

        for n, ref, main in ((DR, d, d_in), (RR, r, r_in)):
            copy(main, ref.at[:, pl.ds(128, COLS)], ins)
        for src, dst in ((lh_in, lh), (ll_in, ll), (gh_in, gh), (gl_in, gl), (rc0_in, rc0), (rc1_in, rc1), (rc2_in, rc2), (rc3_in, rc3)):
            copy(src, dst, ins)

        def put(hi_ref, lo_ref, r0, c0, x):
            hi, lo = split(x)
            hi_ref[r0 : r0 + x.shape[0], c0 : c0 + x.shape[1]] = hi
            lo_ref[r0 : r0 + x.shape[0], c0 : c0 + x.shape[1]] = lo

        zero = jnp.zeros((32, EXT), BF16)
        for ref in (rh, rl):
            ref[0:32, :] = zero
            ref[WIN - 32 : WIN, :] = zero
        near16 = iota((16, 128), 1) < 64
        for at, n, ref, hi, lo in ((0, DR, d, dh, dl), (1, RR, r, rh, rl)):
            cols = slice(128 * at, 128 * at + 128)
            rows = slice(DR * at, DR * at + n)
            ref[:, 0:128] = col_l[:, cols]
            ref[:, 128 + COLS :] = col_r[:, cols]
            for first, main, corner in ((64 - n, row_u, cor_u), (192, row_d, cor_d)):
                put(hi, lo, first, 128, main[rows, :])
                if at == 0:
                    put(hi, lo, first, 0, corner[rows, 0:128])
                    put(hi, lo, first, 128 + COLS, corner[rows, 128:256])
                for k in range(2 * at):
                    both = corner[DR:, 128 * k : 128 * k + 128]
                    put(hi, lo, first + 16 * k, 0, jnp.where(near16, 0.0, both))
                    put(hi, lo, first + 16 * k, 128 + COLS, jnp.where(near16, both, 0.0))
            ins[at].wait()
            put(hi, lo, 64, 0, ref[...])
        for done in ins[2:]:
            done.wait()
        ds, rs = (dh[...], dl[...]), (rh[...], rl[...])

        def left(a, b):
            return (lh[a:b, :], ll[a:b, :])

        put(sh, sl, 0, 0, dot3(left(0, 176), ds))
        put(sh, sl, 176, 0, dot3(left(0, 128), rs))
        put(th, tl, 0, 0, dot3(left(224, 352), ds))
        rd = dot2r(lh[176:224, :], ds)
        rres = dot2r(lh[176:224, :], rs)
        for g in range(5):
            a, v, o = IN0[g], VARIANT[g], slice(256 * g, 256 * g + 256)
            c1[:, o] = dot3((sh[:, a : a + 512], sl[:, a : a + 512]), (gh[v], gl[v]))
            d2[:, o] = dot3((th[:, a : a + 512], tl[:, a : a + 512]), (gh[3 + v], gl[3 + v]))
        t = slice(128, 128 + COLS)
        p1 = c1[0:128, :]
        q[...] = c1[0:128, t] + delta * d[:, t]
        d2[...] = d2[...] + delta * (2.0 * p1 + delta * d[...])
        r1[...] = c1[176:304, :] + delta * r[...]
        copy(q, q_out, outs)
        copy(d2, d2_out, outs)
        copy(r1, r1_out, outs)
        near = iota((32, 128), 1) < 64
        for ref, rows in ((e_dn, slice(96, 128)), (e_up, slice(0, 32))):
            for at, x in ((0, d2), (32, r1)):
                ref[at : at + 32, 0:COLS] = x[rows, t]
                ref[at : at + 32, COLS:] = jnp.where(near, x[rows, 128 + COLS :], x[rows, 0:128])
        qv, rv, aq, ar = q[...], r[:, t], d2[:, t], r1[:, t]
        s_dq = total(d[:, t] * qv)
        e_rr = total(rv * (3.0 * rv - 3.0 * c * ar) + c * c * (ar * ar)) * c
        e_qq = total(qv * (3.0 * qv - 3.0 * c * aq) + c * c * (aq * aq)) * c
        e_rq = total(rv * (3.0 * qv - 3.0 * c * aq) + c * c * (ar * aq)) * c
        fq = c1[128:176, :] + delta * rd
        f = dot2(split(jnp.concatenate([fq, rres], axis=0)), rc0[...])
        f0[...] = f
        pair = (f[0:48], f[48:96])
        weight = 4.0
        for level, cols in ((0, rc1), (1, rc2), (2, rc3)):
            dg, cp = diag[level], coupling[level]
            sm = W / dg
            shape = pair[0].shape
            inside = level_mask(level, shape, slab, gc, n_slab, n_gc)
            mine = tile_mask(level, shape)
            bq, br = operator(pair[0], dg, cp), operator(pair[1], dg, cp)
            own_q, own_r = jnp.where(mine, pair[0], 0.0), jnp.where(mine, pair[1], 0.0)
            e_rr = e_rr + weight * total(own_r * (2.0 * sm * pair[1] - (sm * sm) * br))
            e_qq = e_qq + weight * total(own_q * (2.0 * sm * pair[0] - (sm * sm) * bq))
            e_rq = e_rq + weight * total(own_r * (2.0 * sm * pair[0] - (sm * sm) * bq))
            weight = 2.0 * weight
            rest_q = jnp.where(inside, pair[0] - sm * bq, 0.0)
            rest_r = jnp.where(inside, pair[1] - sm * br, 0.0)
            low = dot2(split(jnp.concatenate([rest_q, rest_r], axis=0)), cols[...])
            if level < 2:
                n, m = (24, 48) if level == 0 else (16, 24)
                half = jnp.where((iota((n, m), 1) >> 1) == iota((n, m), 0), 0.5, 0.0).astype(BF16)
                pair = (dot2r(half, split(low[0:m])), dot2r(half, split(low[m : 2 * m])))
                keep = level_mask(level + 1, pair[0].shape, slab, gc, n_slab, n_gc)
                pair = (jnp.where(keep, pair[0], 0.0), jnp.where(keep, pair[1], 0.0))
                out = (f1, f2)[level]
                out[0:n, :], out[n : 2 * n, :] = pair
        for ref in (e_up, e_dn):
            ref[64:72, 0:128], ref[64:72, 128:256] = pair[0][2:10, :], pair[1][2:10, :]
            ref[64:72, 256:] = jnp.zeros((8, COLS - 128), F32)
        for src, dst in ((f0, f0_out), (f1, f1_out), (f2, f2_out)):
            copy(src, dst, outs)
        i, lane = iota((16, 128), 0), iota((16, 128), 1)
        pick = (i >= 2) & (i < 10) & (((i - 2) >> 1) == (lane >> 5))
        gq = jnp.sum(jnp.where(pick, low[0:16], 0.0), axis=0, keepdims=True) * 0.5
        gr = jnp.sum(jnp.where(pick, low[16:32], 0.0), axis=0, keepdims=True) * 0.5
        lane = iota((1, 128), 1)
        sums = jnp.zeros((1, 128), F32)
        for k, x in enumerate((s_dq, e_rr, e_rq, e_qq)):
            sums = jnp.where(lane == k, x, sums)
        pay[:, 0:128] = jnp.broadcast_to(gq, (n_dev, 128))
        pay[:, 128:256] = jnp.broadcast_to(gr, (n_dev, 128))
        pay[:, 256:384] = jnp.broadcast_to(sums, (n_dev, 128))
        for done in outs:
            done.wait()

    return kernel


def final_kernel(n_slab, n_gc, n_grp):
    n_col = n_gc // n_grp

    def kernel(idx, damping, rho_in, diag, coupling, got, swap, e_u, e_d, d2_in, r1_in, lh_in, ll_in, gh_in, gl_in, q_in, r_in, d_in, sol_in,
               f0_in, f1_in, f2_in, pc0_in, pc1_in, pc2_in, pc3_in,
               o_sol, o_res, o_pre, o_dir, o_energy,
               d2, r1, lh, ll, gh, gl, q, r, d, sol, f0, f1, f2, pc0, pc1, pc2, pc3,
               uh, ul, yh, yl, vs, kk, v_sol, v_res, v_pre, v_dir, sem):
        ins, outs = [], []

        def copy(src, dst, todo):
            done = pltpu.make_async_copy(src, dst, sem.at[len(ins) + len(outs)])
            done.start()
            todo.append(done)

        for src, dst in (
            (d2_in, d2), (r1_in, r1), (lh_in.at[pl.ds(0, 128), :], lh), (ll_in.at[pl.ds(0, 128), :], ll),
            (gh_in.at[pl.ds(0, 3)], gh), (gl_in.at[pl.ds(0, 3)], gl), (r_in, r), (q_in, q), (sol_in, sol), (d_in, d),
            (f0_in, f0), (f1_in, f1), (f2_in, f2), (pc1_in, pc1), (pc2_in, pc2), (pc3_in, pc3), (pc0_in, pc0),
        ):
            copy(src, dst, ins)
        slab, gc = idx[0], idx[1]
        delta, rho = damping[0], rho_in[0]
        c = W / (1.0 + delta)
        lane = iota((1, 128), 1)
        sums = jnp.sum(got[:, 256:384] + swap[:, 256:384], axis=0, keepdims=True)
        s_dq, e_rr, e_rq, e_qq = (
            jnp.sum(jnp.where(lane == k, sums, 0.0), axis=1, keepdims=True) for k in range(4)
        )
        alpha = rho / s_dq
        dg, cp = diag[3], coupling[3]
        first = (iota((n_gc, 128), 1) & 31) == 0
        last = (iota((n_gc, 128), 1) & 31) == 31
        top, bottom = iota((n_gc, 128), 1) < 32, iota((n_gc, 128), 1) >= 96
        left_end, right_end = iota((n_gc, 128), 0) == 0, iota((n_gc, 128), 0) == n_gc - 1
        mine = gc < n_col
        rhs = []
        for s in range(n_slab):
            at = s * n_col
            a, b = (x[at : at + n_col, 128:256] - alpha * x[at : at + n_col, 0:128] for x in (got, swap))
            rhs.append(jnp.concatenate([jnp.where(mine, a, b), jnp.where(mine, b, a)], axis=0))
        zero = jnp.zeros((n_gc, 128), F32)
        v = [W * x / dg for x in rhs]
        for _ in range(3):
            ups = [pltpu.roll(x, 32, 1) for x in v]
            downs = [pltpu.roll(x, 96, 1) for x in v]
            new = []
            for s in range(n_slab):
                x = v[s]
                low = jnp.where(left_end, 0.0, pltpu.roll(pltpu.roll(x, 97, 1), 1, 0))
                high = jnp.where(right_end, 0.0, pltpu.roll(pltpu.roll(x, 31, 1), n_gc - 1, 0))
                beside_x = jnp.where(first, low, pltpu.roll(x, 1, 1))
                beside_x = beside_x + jnp.where(last, high, pltpu.roll(x, 127, 1))
                beside_x = beside_x + jnp.where(top, ups[s - 1] if s > 0 else zero, ups[s])
                beside_x = beside_x + jnp.where(bottom, downs[s + 1] if s < n_slab - 1 else zero, downs[s])
                new.append(x + W * (rhs[s] - (dg * x - cp * beside_x)) / dg)
            v = new
        e3 = total(sum(a * b for a, b in zip(rhs, v)))
        energy = e_rr - alpha * (2.0 * e_rq) + (alpha * alpha) * e_qq + 32.0 * e3
        o_energy[...] = energy
        pitch = n_gc + 16
        vs[...] = jnp.zeros(vs.shape, F32)
        for s in range(n_slab):
            at = (s + 1) * pitch + 8
            vs[at : at + n_gc, :] = v[s]
        v3 = jnp.zeros((8, 128), F32)
        lanes, rows8 = iota((1, 128), 1), iota((8, 128), 0)
        for k, i in ((-1, 3), (0, 0), (0, 1), (0, 2), (0, 3), (1, 0)):
            at = (slab + 1 + k) * pitch + 8 + gc
            mid, lo, hi = (vs[pl.ds(at + x, 1), :] for x in (0, -1, 1))
            line = pltpu.roll(mid, (8 - 32 * i) % 128, 1)
            line = jnp.where(lanes == 7, pltpu.roll(lo, (8 - 32 * i - 32) % 128, 1), line)
            line = jnp.where(lanes == 40, pltpu.roll(hi, (8 - 32 * i + 32) % 128, 1), line)
            line = jnp.where((lanes >= 7) & (lanes <= 40), line, 0.0)
            v3 = jnp.where(rows8 == 4 * k + i + 1, line, v3)
        for done in ins[:10]:
            done.wait()
        v_res[...] = r[...] - alpha * q[...]
        copy(v_res, o_res, outs)
        for ref in (uh, ul):
            ref[0:32, :] = jnp.zeros((32, EXT), BF16)
            ref[WIN - 32 : WIN, :] = jnp.zeros((32, EXT), BF16)
        near = iota((32, 128), 1) < 64
        for at, x in ((32, e_u), (192, e_d)):
            edge = x[32:64, :] - alpha * x[0:32, :]
            side = edge[:, COLS:]
            for first, part in ((128, edge[:, 0:COLS]), (0, jnp.where(near, 0.0, side)), (128 + COLS, jnp.where(near, side, 0.0))):
                hi, lo = split(part)
                uh[at : at + 32, first : first + part.shape[1]] = hi
                ul[at : at + 32, first : first + part.shape[1]] = lo
        uh[64:192, :], ul[64:192, :] = split(r1[...] - alpha * d2[...])
        yh[...], yl[...] = split(dot3((lh[...], ll[...]), (uh[...], ul[...])))
        for g in range(5):
            a, v, o = IN0[g], VARIANT[g], slice(256 * g, 256 * g + 256)
            kk[:, o] = dot3((yh[:, a : a + 512], yl[:, a : a + 512]), (gh[v], gl[v]))
        for done in ins[10:19]:
            done.wait()
        v_sol[...] = sol[...] + alpha * d[...]
        copy(v_sol, o_sol, outs)
        up_q, up_r = e_u[64:72, 0:128], e_u[64:72, 128:256]
        dn_q, dn_r = e_d[64:72, 0:128], e_d[64:72, 128:256]
        edge_u, edge_d = up_r - alpha * up_q, dn_r - alpha * dn_q
        own = f2[16:32, :] - alpha * f2[0:16, :]
        row = iota((16, 128), 0)
        own = jnp.where(row == 0, edge_u[6:7, :], jnp.where(row == 1, edge_u[7:8, :], own))
        own = jnp.where(row == 10, edge_d[0:1, :], jnp.where(row == 11, edge_d[1:2, :], own))
        own = jnp.where(row < 12, own, 0.0)
        f = [f0[48:96, :] - alpha * f0[0:48, :], f1[24:48, :] - alpha * f1[0:24, :], own]
        low = v3
        for level, cols in ((2, pc3), (1, pc2), (0, pc1)):
            dg, cp = diag[level], coupling[level]
            sm = W / dg
            n, m = f[level].shape[0], low.shape[0]
            double = hot((iota((n, m), 0) >> 1) == iota((n, m), 1))
            wide = dot2r(double, split(dot2(split(low), cols[...])))
            inside = level_mask(level, f[level].shape, slab, gc, n_slab, n_gc)
            x = jnp.where(inside, sm * f[level] + wide, 0.0)
            low = jnp.where(inside, x + sm * (f[level] - operator(x, dg, cp)), 0.0)
        four = hot((iota((ROWS, 48), 0) >> 2) + 8 == iota((ROWS, 48), 1))
        t = slice(128, 128 + COLS)
        spread = split(dot2r(four, split(low)))
        au = r1[:, t] - alpha * d2[:, t]
        smooth = c * (3.0 * v_res[...] - (3.0 * c) * au + (c * c) * (kk[:, t] + delta * au))
        pre = smooth + dot2(spread, pc0[...])
        v_pre[...] = pre
        copy(v_pre, o_pre, outs)
        v_dir[...] = pre + (energy / rho) * d[...]
        copy(v_dir, o_dir, outs)
        for done in outs:
            done.wait()

    return kernel


def call(kernel, specs, outs, out_specs, scratch, sems=0):
    where = {"s": pltpu.SMEM, "v": pltpu.VMEM, "h": pltpu.HBM}
    if INTERPRET:
        where["h"] = pl.ANY

    def out(x, shape, kind):
        if x == "h" and not INTERPRET:
            return pltpu.HBM(shape, kind)
        return jax.ShapeDtypeStruct(shape, kind)

    run = pl.pallas_call(
        kernel,
        out_shape=[out(x, s, t) for x, (s, t) in zip(out_specs, outs)],
        in_specs=[pl.BlockSpec(memory_space=where[x]) for x in specs],
        out_specs=[pl.BlockSpec(memory_space=where[x]) for x in out_specs],
        scratch_shapes=[pltpu.VMEM(s, t) for s, t in scratch] + ([pltpu.SemaphoreType.DMA((sems,))] if sems else []),
        compiler_params=pltpu.CompilerParams(vmem_limit_bytes=40 * 1024 * 1024),
        interpret=INTERPRET,
    )

    def apply(*args):
        if INTERPRET:
            return run(*args)
        return run(*(pltpu.with_memory_space_constraint(a, pltpu.HBM) if x == "h" else a for x, a in zip(specs, args)))

    return apply


def run_copies(sem, pairs):
    todo = []
    for k, (src, dst) in enumerate(pairs):
        todo.append(pltpu.make_async_copy(src, dst, sem.at[k]))
        todo[-1].start()
    for done in todo:
        done.wait()


def edges_kernel(d, r, row_u, row_d, col_l, col_r, sem):
    pairs = []
    for n, at, x in ((DR, 0, d), (RR, DR, r)):
        pairs.append((x.at[pl.ds(0, n), :], row_u.at[pl.ds(at, n), :]))
        pairs.append((x.at[pl.ds(ROWS - n, n), :], row_d.at[pl.ds(at, n), :]))
    for at, x in ((0, d), (128, r)):
        pairs.append((x.at[:, pl.ds(0, 128)], col_l.at[:, pl.ds(at, 128)]))
        pairs.append((x.at[:, pl.ds(COLS - 128, 128)], col_r.at[:, pl.ds(at, 128)]))
    run_copies(sem, pairs)


def corners_kernel(from_l, from_r, after, cor_u, cor_d):
    near = iota((16, 128), 1) < 64
    for first, ref in ((0, cor_u), (ROWS - DR, cor_d)):
        ref[0:DR, 0:128] = from_l[first : first + DR, 0:128]
        ref[0:DR, 128:256] = from_r[first : first + DR, 0:128]
    for first, ref in ((0, cor_u), (ROWS - RR, cor_d)):
        for k in range(2):
            rows = slice(first + 16 * k, first + 16 * k + 16)
            ref[DR:, 128 * k : 128 * k + 128] = jnp.where(near, from_r[rows, 128:256], from_l[rows, 128:256])


def solution(mesh):
    n_grp, n_slab, n_col = mesh.shape["grp"], mesh.shape["slab"], mesh.shape["col"]
    n_gc = n_grp * n_col
    n_dev = n_slab * n_col

    def forward(n):
        return [(i, i + 1) for i in range(n - 1)]

    def backward(n):
        return [(i + 1, i) for i in range(n - 1)]

    def body(sol, r, d, row_taps, col_taps, damping, rho, diag, coupling):
        idx = jnp.stack([lax.axis_index("slab"), lax.axis_index(GC)]).astype(jnp.int32)
        row_u, row_d, col_l, col_r = call(
            edges_kernel, "hh", [((DR + RR, COLS), F32)] * 2 + [((ROWS, 256), F32)] * 2, "vvvv", [], 8
        )(d, r)
        from_u = lax.ppermute(row_d, "slab", forward(n_slab))
        from_d = lax.ppermute(row_u, "slab", backward(n_slab))
        from_l = lax.ppermute(col_r, GC, forward(n_gc))
        from_r = lax.ppermute(col_l, GC, backward(n_gc))
        par = (damping[None], rho[None], diag, coupling)
        mat_shapes = [((352, WIN), BF16)] * 2 + [((6, 512, 256), BF16)] * 2
        mat_shapes += [((EXT, 384), BF16), ((384, 256), BF16), ((256, 128), BF16), ((128, 128), BF16)]
        back_shapes = [((384, COLS), BF16), ((256, 384), BF16), ((128, 256), BF16), ((128, 128), BF16)]
        mats = call(
            matrices_kernel(n_slab, n_gc), "sss", mat_shapes + back_shapes, "h" * 12, mat_shapes + back_shapes, 12
        )(idx, row_taps, col_taps)
        lh, ll, gh, gl, rc0, rc1, rc2, rc3, pc0, pc1, pc2, pc3 = mats
        send_u, send_d = call(corners_kernel, "vvh", [((DR + RR // 2, 256), F32)] * 2, "vv", [])(from_l, from_r, rc3)
        cor_u = lax.ppermute(send_d, "slab", forward(n_slab))
        cor_d = lax.ppermute(send_u, "slab", backward(n_slab))
        results = [((ROWS, COLS), F32), ((ROWS, EXT), F32), ((ROWS, EXT), F32)]
        results += [((96, 384), F32), ((48, 256), F32), ((32, 128), F32)]
        q, d2, r1, f0, f1, f2, e_up, e_dn, pay = call(
            halo_kernel(n_slab, n_gc, n_grp),
            "s" * 5 + "hh" + "v" * 6 + "h" * 8,
            results + [((72, COLS + 128), F32)] * 2 + [((n_dev, 384), F32)],
            "h" * 6 + "vvv",
            [((ROWS, EXT), F32)] * 2
            + mat_shapes
            + results
            + [((WIN, EXT), BF16)] * 4
            + [((304, EXT), BF16)] * 2
            + [((128, EXT), BF16)] * 2
            + [((304, EXT), F32)],
            40,
        )(idx, *par, d, r, from_u, from_d, from_l, from_r, cor_u, cor_d, lh, ll, gh, gl, rc0, rc1, rc2, rc3)
        edge_u = lax.ppermute(e_dn, "slab", forward(n_slab))
        edge_d = lax.ppermute(e_up, "slab", backward(n_slab))
        got = lax.all_to_all(pay, ("slab", "col"), 0, 0, tiled=True)
        swap = lax.ppermute(got, "grp", [(i, (i + 1) % n_grp) for i in range(n_grp)])
        tile = ((ROWS, COLS), F32)
        n_sol, n_res, pre, n_dir, energy = call(
            final_kernel(n_slab, n_gc, n_grp),
            "s" * 5 + "vvvv" + "h" * 17,
            [tile] * 4 + [((1, 1), F32)],
            "hhhhv",
            [((ROWS, EXT), F32)] * 2
            + [((128, WIN), BF16)] * 2
            + [((3, 512, 256), BF16)] * 2
            + [tile] * 4
            + [((96, 384), F32), ((48, 256), F32), ((32, 128), F32)]
            + back_shapes
            + [((WIN, EXT), BF16)] * 2
            + [((ROWS, EXT), BF16)] * 2
            + [(((n_slab + 2) * (n_gc + 16), 128), F32), ((ROWS, EXT), F32)]
            + [tile] * 4,
            24,
        )(idx, *par, got, swap, edge_u, edge_d, d2, r1, lh, ll, gh, gl, q, r, d, sol, f0, f1, f2, pc0, pc1, pc2, pc3)
        return n_sol, n_res, pre, n_dir, energy[0, 0]

    tile, rep = P("slab", GC), P()
    return jax.shard_map(
        body,
        mesh=mesh,
        in_specs=(tile,) * 3 + (rep,) * 6,
        out_specs=(tile,) * 4 + (rep,),
        check_vma=False,
    )
```

```python
import jax
import jax.numpy as jnp
from jax import lax
from jax.experimental import pallas as pl
from jax.experimental.pallas import tpu as pltpu
from jax.sharding import PartitionSpec as P


INTERPRET = False
W = 2.0 / 3.0
TAPS = 31
H = TAPS // 2
ROWS, COLS = 128, 1024
EXT = COLS + 256
WIN = ROWS + 128
DR, RR = 64, 32
BAND = 32
VARIANT = (0, 1, 1, 2)
GC = ("grp", "col")
F32, BF16 = jnp.float32, jnp.bfloat16


def iota(shape, dim):
    return lax.broadcasted_iota(jnp.int32, shape, dim)


def split(x):
    high = x.astype(BF16)
    return high, (x - high.astype(F32)).astype(BF16)


def dot(a, b):
    return jnp.dot(a, b, preferred_element_type=F32)


def dot3(a, b):
    (ah, al), (bh, bl) = a, b
    return dot(ah, bh) + (dot(ah, bl) + dot(al, bh))


def dot2(a, b):
    return dot(a[0], b) + dot(a[1], b)


def dot2r(a, b):
    return dot(a, b[0]) + dot(a, b[1])


def hot(cond):
    return jnp.where(cond, 1.0, 0.0).astype(BF16)


def total(x):
    return jnp.sum(jnp.sum(x, axis=0, keepdims=True), axis=1, keepdims=True)


def dot_t(a, b):
    def nt(x, y):
        return lax.dot_general(x, y, (((1,), (1,)), ((), ())), preferred_element_type=F32)

    (ah, al), (bh, bl) = a, b
    return nt(ah, bh) + (nt(ah, bl) + nt(al, bh))


def toeplitz(taps):
    sum_taps = taps[0]
    for t in range(1, TAPS):
        sum_taps = sum_taps + taps[t]
    lane = iota((8, 512), 1)
    base = jnp.zeros((8, 512), F32)
    for t in range(TAPS):
        base = jnp.where(lane == 64 + H - t, taps[t], base)
    base = base / jnp.full((8, 512), sum_taps, F32)
    return pltpu.roll(jnp.broadcast_to(base[0:1], (384, 512)), 0, 1, stride=1, stride_axis=0)


def truncated(kt, first, limit):
    if first is None:
        return split(kt)
    m = iota((384, 512), 1) + (first - 192)
    return split(jnp.where((m >= 0) & (m < limit), kt, 0.0))


def rows_of(pair, *cuts):
    return tuple(jnp.concatenate([x[c] for c in cuts], axis=0) if len(cuts) > 1 else x[cuts[0]] for x in pair)


def block_powers(kt, first, limit):
    left, ks = truncated(kt, first, limit), split(kt)
    wide = split(dot_t(left, ks))
    i = iota((384, 128), 0) + ((first if first is not None else 128) - 128)

    def inside(x):
        return x if first is None else jnp.where((i >= 0) & (i < limit), x, 0.0)

    out = [split(inside(dot_t(left, rows_of(ks, slice(128, 256)))))]
    for _ in range(2):
        out.append(split(inside(dot3(wide, out[-1]))))
    return out


def matrices_kernel(n_slab, n_gc):
    def kernel(idx, rt, ct, *refs):
        outs, scratch, sem = refs[:16], refs[16:32], refs[32]
        lh, ll, gh, gl, sh, sl, oh, ol, rc0, rc1, rc2, rc3, pc0, pc1, pc2, pc3 = scratch
        slab, gc = idx[0], idx[1]
        todo = []

        def send(k):
            todo.append(pltpu.make_async_copy(scratch[k], outs[k], sem.at[k]))
            todo[-1].start()

        gh[...], gl[...] = jnp.zeros(gh.shape, BF16), jnp.zeros(gl.shape, BF16)
        kt = toeplitz(ct)
        inner = block_powers(kt, None, None)
        low = block_powers(kt, gc * COLS, n_gc * COLS)
        high = block_powers(kt, gc * COLS + COLS - 128, n_gc * COLS)
        for at, ref in enumerate((gh, gl)):
            for power in range(3):
                lo, mid, hi = low[power][at], inner[power][at], high[power][at]
                for v, blocks in ((0, (lo, mid)), (1, (mid, mid)), (2, (mid, hi))):
                    ref[3 * power + v, 0:384, 0:128] = blocks[0]
                    ref[3 * power + v, 128:512, 128:256] = blocks[1]
        has_l = jnp.where(gc > 0, 1.0, 0.0).astype(F32)
        has_r = jnp.where(gc < n_gc - 1, 1.0, 0.0).astype(F32)
        for at, ref in enumerate((sh, sl)):
            wide = inner[0][at].astype(F32)
            ref[0], ref[1] = (wide[128:384] * has_l).astype(BF16), (wide[0:256] * has_r).astype(BF16)
        for k in range(2, 6):
            send(k)
        first, limit = slab * ROWS, n_slab * ROWS
        kt = toeplitz(rt)
        left, ks = truncated(kt, first, limit), split(kt)
        near = slice(64, 320)
        tile = rows_of(left, slice(128, 256))
        k = iota((128, 384), 1) + (first - 128)
        keep = (k >= 0) & (k < limit)
        wide = dot_t(left, ks)
        one = split(jnp.where(keep, wide[128:256], 0.0))
        two = split(jnp.where(keep, dot3(one, split(wide)), 0.0))
        window = split(dot_t(left, rows_of(ks, near)))
        nothing = jnp.zeros((64, 512), BF16)
        out_d = tuple(jnp.concatenate([x[32:64], x[320:352], nothing], axis=0) for x in ks)
        out_r = tuple(jnp.concatenate([x[64:96], x[288:320], nothing], axis=0) for x in ks)
        lh[0:128, :], ll[0:128, :] = split(dot_t(tile, rows_of(ks, near)))
        c, i = iota((48, 384), 0), iota((48, 384), 1)
        at = i + (first - 128)
        sums = jnp.where((i - 96 >= 4 * c) & (i - 96 < 4 * c + 4) & (at >= 0) & (at < limit), 0.25, 0.0)
        lh[128:176, :], ll[128:176, :] = split(dot2r(sums.astype(BF16), window))
        c, i = iota((48, WIN), 0), iota((48, WIN), 1)
        sums = jnp.where((i - 32 >= 4 * c) & (i - 32 < 4 * c + 4), 0.25, 0.0).astype(BF16)
        lh[176:224, :], ll[176:224, :] = sums, jnp.zeros_like(sums)
        lh[224:352, :], ll[224:352, :] = split(dot3(one, window))
        lh[352:480, :], ll[352:480, :] = split(dot3(two, window))
        oh[0:128, :], ol[0:128, :] = split(dot3(two, split(dot_t(left, out_d))))
        oh[128:256, :], ol[128:256, :] = split(dot3(one, split(dot_t(left, out_r))))
        for k in (0, 1, 6, 7):
            send(k)
        rc0[...] = hot((iota((EXT, 384), 0) >> 2) + 32 == iota((EXT, 384), 1))
        rc1[...] = hot((iota((384, 256), 0) >> 1) == iota((384, 256), 1))
        rc2[...] = hot((iota((256, 128), 0) >> 1) == iota((256, 128), 1))
        rc3[...] = hot((iota((128, 128), 0) >> 1) - 8 == (iota((128, 128), 1) & 31))
        pc0[...] = hot(iota((384, COLS), 0) == (iota((384, COLS), 1) >> 2) + 64)
        pc1[...] = hot(iota((256, 384), 0) == (iota((256, 384), 1) >> 1))
        pc2[...] = hot(iota((128, 256), 0) == (iota((128, 256), 1) >> 1))
        pc3[...] = hot(iota((128, 128), 0) == (iota((128, 128), 1) >> 1))
        for k in range(8, 16):
            send(k)
        for done in todo:
            done.wait()

    return kernel


def level_mask(level, shape, slab, gc, n_slab, n_gc):
    height, width = 32 >> level, 256 >> level
    i = iota(shape, 0) - (8 >> level) + slab * height
    j = iota(shape, 1) - (64 >> level) + gc * width
    return (i >= 0) & (i < n_slab * height) & (j >= 0) & (j < n_gc * width)


def tile_mask(level, shape):
    i, j = iota(shape, 0) - (8 >> level), iota(shape, 1) - (64 >> level)
    return (i >= 0) & (i < 32 >> level) & (j >= 0) & (j < 256 >> level)


def beside(v):
    n, m = v.shape
    rows = pltpu.roll(v, 1, 0) + pltpu.roll(v, n - 1, 0)
    return rows + pltpu.roll(v, 1, 1) + pltpu.roll(v, m - 1, 1)


def operator(v, dg, cp):
    return dg * v - cp * beside(v)


def halo_kernel(n_slab, n_gc, n_grp):
    n_dev = n_slab * n_gc // n_grp

    def kernel(idx, damping, rho_in, diag, coupling, d_in, r_in, row_u, row_d, col_l, col_r, cor_u, cor_d,
               lh_in, ll_in, gh_in, gl_in, gsh_in, gsl_in, rc0_in, rc1_in, rc2_in, rc3_in,
               q_out, d2_out, r1_out, y3_out, y2_out, f0_out, f1_out, f2_out, e_up, e_dn, pay,
               d, r, lh, ll, gh, gl, gsh, gsl, rc0, rc1, rc2, rc3, q, d2, r1, y3, y2, f0, f1, f2,
               dh, dl, rh, rl, sh, sl, th, tl, c1, sem):
        slab, gc = idx[0], idx[1]
        delta = damping[0]
        c = W / (1.0 + delta)
        ins, outs = [], []

        def copy(src, dst, todo):
            done = pltpu.make_async_copy(src, dst, sem.at[len(ins) + len(outs)])
            done.start()
            todo.append(done)

        for n, ref, main in ((DR, d, d_in), (RR, r, r_in)):
            copy(main, ref.at[:, pl.ds(128, COLS)], ins)
        for src, dst in ((lh_in, lh), (ll_in, ll), (gh_in.at[pl.ds(0, 6)], gh), (gl_in.at[pl.ds(0, 6)], gl), (gsh_in, gsh), (gsl_in, gsl), (rc0_in, rc0), (rc1_in, rc1), (rc2_in, rc2), (rc3_in, rc3)):
            copy(src, dst, ins)

        def put(hi_ref, lo_ref, r0, c0, x):
            hi, lo = split(x)
            hi_ref[r0 : r0 + x.shape[0], c0 : c0 + x.shape[1]] = hi
            lo_ref[r0 : r0 + x.shape[0], c0 : c0 + x.shape[1]] = lo

        zero = jnp.zeros((32, EXT), BF16)
        for ref in (rh, rl):
            ref[0:32, :] = zero
            ref[WIN - 32 : WIN, :] = zero
        near16 = iota((16, 128), 1) < 64
        for at, n, ref, hi, lo in ((0, DR, d, dh, dl), (1, RR, r, rh, rl)):
            cols = slice(128 * at, 128 * at + 128)
            rows = slice(DR * at, DR * at + n)
            ref[:, 0:128] = col_l[:, cols]
            ref[:, 128 + COLS :] = col_r[:, cols]
            for first, main, corner in ((64 - n, row_u, cor_u), (192, row_d, cor_d)):
                put(hi, lo, first, 128, main[rows, :])
                if at == 0:
                    put(hi, lo, first, 0, corner[rows, 0:128])
                    put(hi, lo, first, 128 + COLS, corner[rows, 128:256])
                for k in range(2 * at):
                    both = corner[DR:, 128 * k : 128 * k + 128]
                    put(hi, lo, first + 16 * k, 0, jnp.where(near16, 0.0, both))
                    put(hi, lo, first + 16 * k, 128 + COLS, jnp.where(near16, both, 0.0))
            ins[at].wait()
            put(hi, lo, 64, 0, ref[...])
        for done in ins[2:]:
            done.wait()
        ds, rs = (dh[...], dl[...]), (rh[...], rl[...])

        def left(a, b):
            return (lh[a:b, :], ll[a:b, :])

        put(sh, sl, 0, 0, dot3(left(0, 176), ds))
        put(sh, sl, 176, 0, dot3(left(0, 128), rs))
        put(th, tl, 0, 0, dot3(left(224, 352), ds))
        rd = dot2r(lh[176:224, :], ds)
        rres = dot2r(lh[176:224, :], rs)
        y3[...] = dot3(left(352, 480), ds)
        y2[...] = dot3(left(224, 352), rs)
        copy(y3, y3_out, outs)
        copy(y2, y2_out, outs)
        for g in range(4):
            v, i, o = VARIANT[g], slice(256 * g, 256 * g + 512), slice(256 * g, 256 * g + 256)
            c1[:, o] = dot3((sh[:, i], sl[:, i]), (gh[v], gl[v]))
            d2[:, o] = dot3((th[:, i], tl[:, i]), (gh[3 + v], gl[3 + v]))
        t = slice(128, 128 + COLS)
        p1 = c1[0:128, :]
        q[...] = p1 + delta * d[:, t]
        d2[...] = d2[...] + delta * (2.0 * p1 + delta * d[:, t])
        r1[...] = c1[176:304, :] + delta * r[:, t]
        copy(q, q_out, outs)
        copy(d2, d2_out, outs)
        copy(r1, r1_out, outs)
        qv, rv, aq, ar = q[...], r[:, t], d2[...], r1[...]
        s_dq = total(d[:, t] * qv)
        e_rr = total(rv * (3.0 * rv - 3.0 * c * ar) + c * c * (ar * ar)) * c
        e_qq = total(qv * (3.0 * qv - 3.0 * c * aq) + c * c * (aq * aq)) * c
        e_rq = total(rv * (3.0 * qv - 3.0 * c * aq) + c * c * (ar * aq)) * c
        sides = [
            dot3((sh[128:176, i], sl[128:176, i]), (gsh[k], gsl[k])) for k, i in ((0, slice(0, 256)), (1, slice(COLS, EXT)))
        ]
        fq = jnp.concatenate([sides[0], c1[128:176, :], sides[1]], axis=1) + delta * rd
        f = dot2(split(jnp.concatenate([fq, rres], axis=0)), rc0[...])
        f0[...] = f
        pair = (f[0:48], f[48:96])
        weight = 4.0
        for level, cols in ((0, rc1), (1, rc2), (2, rc3)):
            dg, cp = diag[level], coupling[level]
            sm = W / dg
            shape = pair[0].shape
            inside = level_mask(level, shape, slab, gc, n_slab, n_gc)
            mine = tile_mask(level, shape)
            bq, br = operator(pair[0], dg, cp), operator(pair[1], dg, cp)
            own_q, own_r = jnp.where(mine, pair[0], 0.0), jnp.where(mine, pair[1], 0.0)
            e_rr = e_rr + weight * total(own_r * (2.0 * sm * pair[1] - (sm * sm) * br))
            e_qq = e_qq + weight * total(own_q * (2.0 * sm * pair[0] - (sm * sm) * bq))
            e_rq = e_rq + weight * total(own_r * (2.0 * sm * pair[0] - (sm * sm) * bq))
            weight = 2.0 * weight
            rest_q = jnp.where(inside, pair[0] - sm * bq, 0.0)
            rest_r = jnp.where(inside, pair[1] - sm * br, 0.0)
            low = dot2(split(jnp.concatenate([rest_q, rest_r], axis=0)), cols[...])
            if level < 2:
                n, m = (24, 48) if level == 0 else (16, 24)
                half = jnp.where((iota((n, m), 1) >> 1) == iota((n, m), 0), 0.5, 0.0).astype(BF16)
                pair = (dot2r(half, split(low[0:m])), dot2r(half, split(low[m : 2 * m])))
                keep = level_mask(level + 1, pair[0].shape, slab, gc, n_slab, n_gc)
                pair = (jnp.where(keep, pair[0], 0.0), jnp.where(keep, pair[1], 0.0))
                out = (f1, f2)[level]
                out[0:n, :], out[n : 2 * n, :] = pair
        for ref in (e_up, e_dn):
            ref[:, 0:128], ref[:, 128:256] = pair[0][2:10, :], pair[1][2:10, :]
        for src, dst in ((f0, f0_out), (f1, f1_out), (f2, f2_out)):
            copy(src, dst, outs)
        i, lane = iota((16, 128), 0), iota((16, 128), 1)
        pick = (i >= 2) & (i < 10) & (((i - 2) >> 1) == (lane >> 5))
        gq = jnp.sum(jnp.where(pick, low[0:16], 0.0), axis=0, keepdims=True) * 0.5
        gr = jnp.sum(jnp.where(pick, low[16:32], 0.0), axis=0, keepdims=True) * 0.5
        lane = iota((1, 128), 1)
        sums = jnp.zeros((1, 128), F32)
        for k, x in enumerate((s_dq, e_rr, e_rq, e_qq)):
            sums = jnp.where(lane == k, x, sums)
        pay[:, 0:128] = jnp.broadcast_to(gq, (n_dev, 128))
        pay[:, 128:256] = jnp.broadcast_to(gr, (n_dev, 128))
        pay[:, 256:384] = jnp.broadcast_to(sums, (n_dev, 128))
        for done in outs:
            done.wait()

    return kernel


def outer_kernel(y3_in, y2_in, oh_in, ol_in, gh_in, gl_in, band_u, band_d, p3_out, p2_out,
                 y3, y2, oh, ol, gh, gl, p3, p2, th, tl, sem):
    ins, outs = [], []

    def copy(src, dst, todo):
        todo.append(pltpu.make_async_copy(src, dst, sem.at[len(ins) + len(outs)]))
        todo[-1].start()

    for src, dst in ((oh_in, oh), (ol_in, ol), (y3_in, y3), (y2_in, y2), (gh_in.at[pl.ds(3, 6)], gh), (gl_in.at[pl.ds(3, 6)], gl)):
        copy(src, dst, ins)
    nothing = jnp.zeros((64, EXT), BF16)
    for done in ins[:4]:
        done.wait()
    for at, y in ((0, y3), (1, y2)):
        rows = slice(BAND * at, BAND * at + BAND)
        hi, lo = split(jnp.concatenate([band_u[rows, :], band_d[rows, :]], axis=0))
        outer = (jnp.concatenate([hi, nothing], axis=0), jnp.concatenate([lo, nothing], axis=0))
        left = slice(128 * at, 128 * at + 128)
        th[at], tl[at] = split(y[...] + dot3((oh[left], ol[left]), outer))
    for done in ins[4:]:
        done.wait()
    for at, p, out, power in ((0, p3, p3_out, 3), (1, p2, p2_out, 0)):
        for g in range(4):
            v, i, o = power + VARIANT[g], slice(256 * g, 256 * g + 512), slice(256 * g, 256 * g + 256)
            p[:, o] = dot3((th[at, :, i], tl[at, :, i]), (gh[v], gl[v]))
        copy(p, out, outs)
    for done in outs:
        done.wait()


def final_kernel(n_slab, n_gc, n_grp):
    n_col = n_gc // n_grp

    def kernel(idx, damping, rho_in, diag, coupling, got, swap, e_u, e_d, d2_in, r1_in, p3_in, p2_in, q_in, r_in, d_in, sol_in,
               f0_in, f1_in, f2_in, pc0_in, pc1_in, pc2_in, pc3_in,
               o_sol, o_res, o_pre, o_dir, o_energy,
               d2, r1, p3, p2, q, r, d, sol, f0, f1, f2, pc0, pc1, pc2, pc3,
               vs, v_sol, v_res, v_pre, v_dir, sem):
        ins, outs = [], []

        def copy(src, dst, todo):
            done = pltpu.make_async_copy(src, dst, sem.at[len(ins) + len(outs)])
            done.start()
            todo.append(done)

        for src, dst in (
            (r_in, r), (q_in, q), (sol_in, sol), (d_in, d), (f0_in, f0), (f1_in, f1), (f2_in, f2), (pc1_in, pc1), (pc2_in, pc2),
            (pc3_in, pc3), (pc0_in, pc0), (d2_in, d2), (r1_in, r1), (p3_in, p3), (p2_in, p2),
        ):
            copy(src, dst, ins)
        slab, gc = idx[0], idx[1]
        delta, rho = damping[0], rho_in[0]
        c = W / (1.0 + delta)
        lane = iota((1, 128), 1)
        sums = jnp.sum(got[:, 256:384] + swap[:, 256:384], axis=0, keepdims=True)
        s_dq, e_rr, e_rq, e_qq = (
            jnp.sum(jnp.where(lane == k, sums, 0.0), axis=1, keepdims=True) for k in range(4)
        )
        alpha = rho / s_dq
        dg, cp = diag[3], coupling[3]
        first = (iota((n_gc, 128), 1) & 31) == 0
        last = (iota((n_gc, 128), 1) & 31) == 31
        top, bottom = iota((n_gc, 128), 1) < 32, iota((n_gc, 128), 1) >= 96
        left_end, right_end = iota((n_gc, 128), 0) == 0, iota((n_gc, 128), 0) == n_gc - 1
        mine = gc < n_col
        rhs = []
        for s in range(n_slab):
            at = s * n_col
            a, b = (x[at : at + n_col, 128:256] - alpha * x[at : at + n_col, 0:128] for x in (got, swap))
            rhs.append(jnp.concatenate([jnp.where(mine, a, b), jnp.where(mine, b, a)], axis=0))
        zero = jnp.zeros((n_gc, 128), F32)
        v = [W * x / dg for x in rhs]
        for _ in range(3):
            ups = [pltpu.roll(x, 32, 1) for x in v]
            downs = [pltpu.roll(x, 96, 1) for x in v]
            new = []
            for s in range(n_slab):
                x = v[s]
                low = jnp.where(left_end, 0.0, pltpu.roll(pltpu.roll(x, 97, 1), 1, 0))
                high = jnp.where(right_end, 0.0, pltpu.roll(pltpu.roll(x, 31, 1), n_gc - 1, 0))
                beside_x = jnp.where(first, low, pltpu.roll(x, 1, 1))
                beside_x = beside_x + jnp.where(last, high, pltpu.roll(x, 127, 1))
                beside_x = beside_x + jnp.where(top, ups[s - 1] if s > 0 else zero, ups[s])
                beside_x = beside_x + jnp.where(bottom, downs[s + 1] if s < n_slab - 1 else zero, downs[s])
                new.append(x + W * (rhs[s] - (dg * x - cp * beside_x)) / dg)
            v = new
        e3 = total(sum(a * b for a, b in zip(rhs, v)))
        energy = e_rr - alpha * (2.0 * e_rq) + (alpha * alpha) * e_qq + 32.0 * e3
        o_energy[...] = energy
        pitch = n_gc + 16
        vs[...] = jnp.zeros(vs.shape, F32)
        for s in range(n_slab):
            at = (s + 1) * pitch + 8
            vs[at : at + n_gc, :] = v[s]
        v3 = jnp.zeros((8, 128), F32)
        lanes, rows8 = iota((1, 128), 1), iota((8, 128), 0)
        for k, i in ((-1, 3), (0, 0), (0, 1), (0, 2), (0, 3), (1, 0)):
            at = (slab + 1 + k) * pitch + 8 + gc
            mid, lo, hi = (vs[pl.ds(at + x, 1), :] for x in (0, -1, 1))
            line = pltpu.roll(mid, (8 - 32 * i) % 128, 1)
            line = jnp.where(lanes == 7, pltpu.roll(lo, (8 - 32 * i - 32) % 128, 1), line)
            line = jnp.where(lanes == 40, pltpu.roll(hi, (8 - 32 * i + 32) % 128, 1), line)
            line = jnp.where((lanes >= 7) & (lanes <= 40), line, 0.0)
            v3 = jnp.where(rows8 == 4 * k + i + 1, line, v3)
        for done in ins[:4]:
            done.wait()
        v_res[...] = r[...] - alpha * q[...]
        copy(v_res, o_res, outs)
        v_sol[...] = sol[...] + alpha * d[...]
        copy(v_sol, o_sol, outs)
        for done in ins[4:15]:
            done.wait()
        up_q, up_r = e_u[:, 0:128], e_u[:, 128:256]
        dn_q, dn_r = e_d[:, 0:128], e_d[:, 128:256]
        edge_u, edge_d = up_r - alpha * up_q, dn_r - alpha * dn_q
        own = f2[16:32, :] - alpha * f2[0:16, :]
        row = iota((16, 128), 0)
        own = jnp.where(row == 0, edge_u[6:7, :], jnp.where(row == 1, edge_u[7:8, :], own))
        own = jnp.where(row == 10, edge_d[0:1, :], jnp.where(row == 11, edge_d[1:2, :], own))
        own = jnp.where(row < 12, own, 0.0)
        f = [f0[48:96, :] - alpha * f0[0:48, :], f1[24:48, :] - alpha * f1[0:24, :], own]
        low = v3
        for level, cols in ((2, pc3), (1, pc2), (0, pc1)):
            dg, cp = diag[level], coupling[level]
            sm = W / dg
            n, m = f[level].shape[0], low.shape[0]
            double = hot((iota((n, m), 0) >> 1) == iota((n, m), 1))
            wide = dot2r(double, split(dot2(split(low), cols[...])))
            inside = level_mask(level, f[level].shape, slab, gc, n_slab, n_gc)
            x = jnp.where(inside, sm * f[level] + wide, 0.0)
            low = jnp.where(inside, x + sm * (f[level] - operator(x, dg, cp)), 0.0)
        four = hot((iota((ROWS, 48), 0) >> 2) + 8 == iota((ROWS, 48), 1))
        spread = split(dot2r(four, split(low)))
        au = r1[...] - alpha * d2[...]
        a2r = p2[...] + (2.0 * delta) * r1[...] - (delta * delta) * r[...]
        a3d = p3[...] + delta * (3.0 * d2[...] - delta * (3.0 * q[...] - delta * d[...]))
        smooth = c * (3.0 * v_res[...] - (3.0 * c) * au + (c * c) * (a2r - alpha * a3d))
        pre = smooth + dot2(spread, pc0[...])
        v_pre[...] = pre
        copy(v_pre, o_pre, outs)
        v_dir[...] = pre + (energy / rho) * d[...]
        copy(v_dir, o_dir, outs)
        for done in outs:
            done.wait()

    return kernel


def call(kernel, specs, outs, out_specs, scratch, sems=0):
    where = {"s": pltpu.SMEM, "v": pltpu.VMEM, "h": pltpu.HBM}
    if INTERPRET:
        where["h"] = pl.ANY

    def out(x, shape, kind):
        if x == "h" and not INTERPRET:
            return pltpu.HBM(shape, kind)
        return jax.ShapeDtypeStruct(shape, kind)

    run = pl.pallas_call(
        kernel,
        out_shape=[out(x, s, t) for x, (s, t) in zip(out_specs, outs)],
        in_specs=[pl.BlockSpec(memory_space=where[x]) for x in specs],
        out_specs=[pl.BlockSpec(memory_space=where[x]) for x in out_specs],
        scratch_shapes=[pltpu.VMEM(s, t) for s, t in scratch] + ([pltpu.SemaphoreType.DMA((sems,))] if sems else []),
        compiler_params=pltpu.CompilerParams(vmem_limit_bytes=40 * 1024 * 1024),
        interpret=INTERPRET,
    )

    def apply(*args):
        if INTERPRET:
            return run(*args)
        return run(*(pltpu.with_memory_space_constraint(a, pltpu.HBM) if x == "h" else a for x, a in zip(specs, args)))

    return apply


def run_copies(sem, pairs):
    todo = []
    for k, (src, dst) in enumerate(pairs):
        todo.append(pltpu.make_async_copy(src, dst, sem.at[k]))
        todo[-1].start()
    for done in todo:
        done.wait()


def edges_kernel(d, r, row_u, row_d, col_l, col_r, sem):
    pairs = []
    for n, at, x in ((DR, 0, d), (RR, DR, r)):
        pairs.append((x.at[pl.ds(0, n), :], row_u.at[pl.ds(at, n), :]))
        pairs.append((x.at[pl.ds(ROWS - n, n), :], row_d.at[pl.ds(at, n), :]))
    for at, x in ((0, d), (128, r)):
        pairs.append((x.at[:, pl.ds(0, 128)], col_l.at[:, pl.ds(at, 128)]))
        pairs.append((x.at[:, pl.ds(COLS - 128, 128)], col_r.at[:, pl.ds(at, 128)]))
    run_copies(sem, pairs)


def corners_kernel(from_l, from_r, after, cor_u, cor_d):
    near = iota((16, 128), 1) < 64
    for first, ref in ((0, cor_u), (ROWS - DR, cor_d)):
        ref[0:DR, 0:128] = from_l[first : first + DR, 0:128]
        ref[0:DR, 128:256] = from_r[first : first + DR, 0:128]
    for first, ref in ((0, cor_u), (ROWS - RR, cor_d)):
        for k in range(2):
            rows = slice(first + 16 * k, first + 16 * k + 16)
            ref[DR:, 128 * k : 128 * k + 128] = jnp.where(near, from_r[rows, 128:256], from_l[rows, 128:256])


def bands_kernel(d, r, from_l, from_r, after, band_u, band_d, sem):
    main, todo = pl.ds(128, COLS), []
    for ref, first_d, first_r in ((band_u, DR, RR), (band_d, ROWS - DR - BAND, ROWS - RR - BAND)):
        for at, first, x in ((0, first_d, d), (BAND, first_r, r)):
            todo.append(pltpu.make_async_copy(x.at[pl.ds(first, BAND), :], ref.at[pl.ds(at, BAND), main], sem.at[len(todo)]))
            todo[-1].start()
            lanes = slice(128 * at // BAND, 128 * at // BAND + 128)
            ref[at : at + BAND, 0:128] = from_l[first : first + BAND, lanes]
            ref[at : at + BAND, 128 + COLS :] = from_r[first : first + BAND, lanes]
    for done in todo:
        done.wait()


def solution(mesh):
    n_grp, n_slab, n_col = mesh.shape["grp"], mesh.shape["slab"], mesh.shape["col"]
    n_gc = n_grp * n_col
    n_dev = n_slab * n_col

    def forward(n):
        return [(i, i + 1) for i in range(n - 1)]

    def backward(n):
        return [(i + 1, i) for i in range(n - 1)]

    def body(sol, r, d, row_taps, col_taps, damping, rho, diag, coupling):
        idx = jnp.stack([lax.axis_index("slab"), lax.axis_index(GC)]).astype(jnp.int32)
        row_u, row_d, col_l, col_r = call(
            edges_kernel, "hh", [((DR + RR, COLS), F32)] * 2 + [((ROWS, 256), F32)] * 2, "vvvv", [], 8
        )(d, r)
        from_u = lax.ppermute(row_d, "slab", forward(n_slab))
        from_d = lax.ppermute(row_u, "slab", backward(n_slab))
        from_l = lax.ppermute(col_r, GC, forward(n_gc))
        from_r = lax.ppermute(col_l, GC, backward(n_gc))
        par = (damping[None], rho[None], diag, coupling)
        mat_shapes = [((480, WIN), BF16)] * 2 + [((9, 512, 256), BF16)] * 2 + [((2, 256, 128), BF16)] * 2
        mat_shapes += [((256, 128), BF16)] * 2
        mat_shapes += [((EXT, 384), BF16), ((384, 256), BF16), ((256, 128), BF16), ((128, 128), BF16)]
        back_shapes = [((384, COLS), BF16), ((256, 384), BF16), ((128, 256), BF16), ((128, 128), BF16)]
        mats = call(
            matrices_kernel(n_slab, n_gc), "sss", mat_shapes + back_shapes, "h" * 16, mat_shapes + back_shapes, 16
        )(idx, row_taps, col_taps)
        lh, ll, gh, gl, gsh, gsl, oh, ol, rc0, rc1, rc2, rc3, pc0, pc1, pc2, pc3 = mats
        send_u, send_d = call(corners_kernel, "vvh", [((DR + RR // 2, 256), F32)] * 2, "vv", [])(from_l, from_r, rc3)
        cor_u = lax.ppermute(send_d, "slab", forward(n_slab))
        cor_d = lax.ppermute(send_u, "slab", backward(n_slab))
        send_up, send_dn = call(
            bands_kernel, "hhvvh", [((2 * BAND, EXT), F32)] * 2, "vv", [], 4
        )(d, r, from_l, from_r, rc3)
        band_u = lax.ppermute(send_dn, "slab", forward(n_slab))
        band_d = lax.ppermute(send_up, "slab", backward(n_slab))
        results = [((ROWS, COLS), F32)] * 3 + [((ROWS, EXT), F32)] * 2
        results += [((96, 384), F32), ((48, 256), F32), ((32, 128), F32)]
        q, d2, r1, y3, y2, f0, f1, f2, e_up, e_dn, pay = call(
            halo_kernel(n_slab, n_gc, n_grp),
            "s" * 5 + "hh" + "v" * 6 + "h" * 10,
            results + [((8, 256), F32)] * 2 + [((n_dev, 384), F32)],
            "h" * 8 + "vvv",
            [((ROWS, EXT), F32)] * 2
            + [((480, WIN), BF16)] * 2
            + [((6, 512, 256), BF16)] * 2
            + [((2, 256, 128), BF16)] * 2
            + mat_shapes[8:]
            + results
            + [((WIN, EXT), BF16)] * 4
            + [((304, EXT), BF16)] * 2
            + [((128, EXT), BF16)] * 2
            + [((304, COLS), F32)],
            24,
        )(idx, *par, d, r, from_u, from_d, from_l, from_r, cor_u, cor_d, lh, ll, gh, gl, gsh, gsl, rc0, rc1, rc2, rc3)
        edge_u = lax.ppermute(e_dn, "slab", forward(n_slab))
        edge_d = lax.ppermute(e_up, "slab", backward(n_slab))
        got = lax.all_to_all(pay, ("slab", "col"), 0, 0, tiled=True)
        swap = lax.ppermute(got, "grp", [(i, (i + 1) % n_grp) for i in range(n_grp)])
        tile = ((ROWS, COLS), F32)
        p3, p2 = call(
            outer_kernel,
            "h" * 6 + "vv",
            [tile] * 2,
            "hh",
            [((ROWS, EXT), F32)] * 2
            + [((256, 128), BF16)] * 2
            + [((6, 512, 256), BF16)] * 2
            + [tile] * 2
            + [((2, ROWS, EXT), BF16)] * 2,
            8,
        )(y3, y2, oh, ol, gh, gl, band_u, band_d)
        n_sol, n_res, pre, n_dir, energy = call(
            final_kernel(n_slab, n_gc, n_grp),
            "s" * 5 + "vvvv" + "h" * 15,
            [tile] * 4 + [((1, 1), F32)],
            "hhhhv",
            [tile] * 8
            + [((96, 384), F32), ((48, 256), F32), ((32, 128), F32)]
            + back_shapes
            + [(((n_slab + 2) * (n_gc + 16), 128), F32)]
            + [tile] * 4,
            20,
        )(idx, *par, got, swap, edge_u, edge_d, d2, r1, p3, p2, q, r, d, sol, f0, f1, f2, pc0, pc1, pc2, pc3)
        return n_sol, n_res, pre, n_dir, energy[0, 0]

    tile, rep = P("slab", GC), P()
    return jax.shard_map(
        body,
        mesh=mesh,
        in_specs=(tile,) * 3 + (rep,) * 6,
        out_specs=(tile,) * 4 + (rep,),
        check_vma=False,
    )
```

```python
import jax
import jax.numpy as jnp
from jax import lax
from jax.experimental import pallas as pl
from jax.experimental.pallas import tpu as pltpu
from jax.sharding import PartitionSpec as P


INTERPRET = False
W = 2.0 / 3.0
TAPS = 31
H = TAPS // 2
ROWS, COLS = 128, 1024
EXT = COLS + 256
WIN = ROWS + 128
DR, RR = 64, 32
BAND = 32
VARIANT = (0, 1, 1, 2)
GC = ("grp", "col")
F32, BF16 = jnp.float32, jnp.bfloat16


def iota(shape, dim):
    return lax.broadcasted_iota(jnp.int32, shape, dim)


def split(x):
    high = x.astype(BF16)
    return high, (x - high.astype(F32)).astype(BF16)


def dot(a, b):
    return jnp.dot(a, b, preferred_element_type=F32)


def dot3(a, b):
    (ah, al), (bh, bl) = a, b
    return dot(ah, bh) + (dot(ah, bl) + dot(al, bh))


def dot2(a, b):
    return dot(a[0], b) + dot(a[1], b)


def dot2r(a, b):
    return dot(a, b[0]) + dot(a, b[1])


def hot(cond):
    return jnp.where(cond, 1.0, 0.0).astype(BF16)


def total(x):
    return jnp.sum(jnp.sum(x, axis=0, keepdims=True), axis=1, keepdims=True)


def dot_t(a, b):
    def nt(x, y):
        return lax.dot_general(x, y, (((1,), (1,)), ((), ())), preferred_element_type=F32)

    (ah, al), (bh, bl) = a, b
    return nt(ah, bh) + (nt(ah, bl) + nt(al, bh))


def toeplitz(taps):
    sum_taps = taps[0]
    for t in range(1, TAPS):
        sum_taps = sum_taps + taps[t]
    lane = iota((8, 512), 1)
    base = jnp.zeros((8, 512), F32)
    for t in range(TAPS):
        base = jnp.where(lane == 64 + H - t, taps[t], base)
    base = base / jnp.full((8, 512), sum_taps, F32)
    return pltpu.roll(jnp.broadcast_to(base[0:1], (384, 512)), 0, 1, stride=1, stride_axis=0)


def truncated(kt, first, limit):
    if first is None:
        return split(kt)
    m = iota((384, 512), 1) + (first - 192)
    return split(jnp.where((m >= 0) & (m < limit), kt, 0.0))


def rows_of(pair, *cuts):
    return tuple(jnp.concatenate([x[c] for c in cuts], axis=0) if len(cuts) > 1 else x[cuts[0]] for x in pair)


def block_powers(kt, first, limit):
    left, ks = truncated(kt, first, limit), split(kt)
    wide = split(dot_t(left, ks))
    i = iota((384, 128), 0) + ((first if first is not None else 128) - 128)

    def inside(x):
        return x if first is None else jnp.where((i >= 0) & (i < limit), x, 0.0)

    out = [split(inside(dot_t(left, rows_of(ks, slice(128, 256)))))]
    for _ in range(2):
        out.append(split(inside(dot3(wide, out[-1]))))
    return out


def matrices_kernel(n_slab, n_gc):
    def kernel(idx, rt, ct, *refs):
        outs, scratch, sem = refs[:16], refs[16:32], refs[32]
        lh, ll, gh, gl, sh, sl, oh, ol, rc0, rc1, rc2, rc3, pc0, pc1, pc2, pc3 = scratch
        slab, gc = idx[0], idx[1]
        todo = []

        def send(k):
            todo.append(pltpu.make_async_copy(scratch[k], outs[k], sem.at[k]))
            todo[-1].start()

        gh[...], gl[...] = jnp.zeros(gh.shape, BF16), jnp.zeros(gl.shape, BF16)
        kt = toeplitz(ct)
        inner = block_powers(kt, None, None)
        end = block_powers(kt, jnp.where(gc == 0, 0, gc * COLS + COLS - 128), n_gc * COLS)
        at_l, at_r = gc == 0, gc == n_gc - 1
        for at, ref in enumerate((gh, gl)):
            for power in range(3):
                mid = inner[power][at]
                a, b = mid.astype(F32), end[power][at].astype(F32)
                lo, hi = jnp.where(at_l, b, a).astype(BF16), jnp.where(at_r, b, a).astype(BF16)
                for v, blocks in ((0, (lo, mid)), (1, (mid, mid)), (2, (mid, hi))):
                    ref[3 * power + v, 0:384, 0:128] = blocks[0]
                    ref[3 * power + v, 128:512, 128:256] = blocks[1]
        has_l = jnp.where(gc > 0, 1.0, 0.0).astype(F32)
        has_r = jnp.where(gc < n_gc - 1, 1.0, 0.0).astype(F32)
        for at, ref in enumerate((sh, sl)):
            wide = inner[0][at].astype(F32)
            ref[0], ref[1] = (wide[128:384] * has_l).astype(BF16), (wide[0:256] * has_r).astype(BF16)
        for k in range(2, 6):
            send(k)
        first, limit = slab * ROWS, n_slab * ROWS
        kt = toeplitz(rt)
        left, ks = truncated(kt, first, limit), split(kt)
        near = slice(64, 320)
        tile = rows_of(left, slice(128, 256))
        k = iota((128, 384), 1) + (first - 128)
        keep = (k >= 0) & (k < limit)
        wide = dot_t(left, ks)
        one = split(jnp.where(keep, wide[128:256], 0.0))
        two = split(jnp.where(keep, dot3(one, split(wide)), 0.0))
        window = split(dot_t(left, rows_of(ks, near)))
        nothing = jnp.zeros((64, 512), BF16)
        out_d = tuple(jnp.concatenate([x[32:64], x[320:352], nothing], axis=0) for x in ks)
        out_r = tuple(jnp.concatenate([x[64:96], x[288:320], nothing], axis=0) for x in ks)
        lh[0:128, :], ll[0:128, :] = split(dot_t(tile, rows_of(ks, near)))
        c, i = iota((48, 384), 0), iota((48, 384), 1)
        at = i + (first - 128)
        sums = jnp.where((i - 96 >= 4 * c) & (i - 96 < 4 * c + 4) & (at >= 0) & (at < limit), 0.25, 0.0)
        lh[128:176, :], ll[128:176, :] = split(dot2r(sums.astype(BF16), window))
        c, i = iota((48, WIN), 0), iota((48, WIN), 1)
        sums = jnp.where((i - 32 >= 4 * c) & (i - 32 < 4 * c + 4), 0.25, 0.0).astype(BF16)
        lh[176:224, :], ll[176:224, :] = sums, jnp.zeros_like(sums)
        lh[224:352, :], ll[224:352, :] = split(dot3(one, window))
        lh[352:480, :], ll[352:480, :] = split(dot3(two, window))
        oh[0:128, :], ol[0:128, :] = split(dot3(two, split(dot_t(left, out_d))))
        oh[128:256, :], ol[128:256, :] = split(dot3(one, split(dot_t(left, out_r))))
        c, i = iota((16, 384), 0), iota((16, 384), 1)
        c = jnp.where(c < 8, 4 * c - 64, 4 * c + 128)
        at = i + (first - 128)
        own = (i - 128 >= c) & (i - 128 < c + 4) & (at >= 0) & (at < limit)
        sums = jnp.where(own, 0.25, 0.0).astype(BF16)
        lh[480:496, :], ll[480:496, :] = split(dot2r(sums, window))
        oh[256:272, :], ol[256:272, :] = split(dot2r(sums, split(dot_t(left, out_d))))
        c, i = iota((16, WIN), 0), iota((16, WIN), 1)
        c = jnp.where(c < 8, 4 * c - 64, 4 * c + 128)
        sums = jnp.where((i - 64 >= c) & (i - 64 < c + 4), 0.25, 0.0).astype(BF16)
        lh[496:512, :], ll[496:512, :] = sums, jnp.zeros_like(sums)
        c, i = iota((16, 128), 0), iota((16, 128), 1)
        c = 4 * c
        sums = jnp.where((i >= c) & (i < c + 4) & (i < 64), 0.25, 0.0).astype(BF16)
        oh[272:288, :], ol[272:288, :] = sums, jnp.zeros_like(sums)
        for k in (0, 1, 6, 7):
            send(k)
        rc0[...] = hot((iota((EXT, 384), 0) >> 2) + 32 == iota((EXT, 384), 1))
        rc1[...] = hot((iota((384, 256), 0) >> 1) == iota((384, 256), 1))
        rc2[...] = hot((iota((256, 128), 0) >> 1) == iota((256, 128), 1))
        rc3[...] = hot((iota((128, 128), 0) >> 1) - 8 == (iota((128, 128), 1) & 31))
        pc0[...] = hot(iota((384, COLS), 0) == (iota((384, COLS), 1) >> 2) + 64)
        pc1[...] = hot(iota((256, 384), 0) == (iota((256, 384), 1) >> 1))
        pc2[...] = hot(iota((128, 256), 0) == (iota((128, 256), 1) >> 1))
        pc3[...] = hot(iota((128, 128), 0) == (iota((128, 128), 1) >> 1))
        for k in range(8, 16):
            send(k)
        for done in todo:
            done.wait()

    return kernel


def level_mask(level, shape, slab, gc, n_slab, n_gc, margin=8):
    height, width = 32 >> level, 256 >> level
    i = iota(shape, 0) - (margin >> level) + slab * height
    j = iota(shape, 1) - (64 >> level) + gc * width
    return (i >= 0) & (i < n_slab * height) & (j >= 0) & (j < n_gc * width)


def tile_mask(level, shape):
    i, j = iota(shape, 0) - (8 >> level), iota(shape, 1) - (64 >> level)
    return (i >= 0) & (i < 32 >> level) & (j >= 0) & (j < 256 >> level)


def beside(v):
    n, m = v.shape
    rows = pltpu.roll(v, 1, 0) + pltpu.roll(v, n - 1, 0)
    return rows + pltpu.roll(v, 1, 1) + pltpu.roll(v, m - 1, 1)


def operator(v, dg, cp):
    return dg * v - cp * beside(v)


def halo_kernel(n_slab, n_gc, n_grp):
    n_dev = n_slab * n_gc // n_grp

    def kernel(idx, damping, rho_in, diag, coupling, d_in, r_in, row_u, row_d, col_l, col_r, cor_ul, cor_ur, cor_dl, cor_dr,
               lh_in, ll_in, gh_in, gl_in, gsh_in, gsl_in, rc0_in, rc1_in, rc2_in, rc3_in,
               q_out, d2_out, r1_out, y3_out, y2_out, z_out, f0_out, f1_out, pay,
               d, r, lh, ll, gh, gl, gsh, gsl, rc0, rc1, rc2, rc3, q, d2, r1, y3, y2, z, f0, f1,
               dh, dl, rh, rl, sh, sl, th, tl, c1, sem):
        slab, gc = idx[0], idx[1]
        delta = damping[0]
        c = W / (1.0 + delta)
        ins, outs = [], []

        def copy(src, dst, todo):
            done = pltpu.make_async_copy(src, dst, sem.at[len(ins) + len(outs)])
            done.start()
            todo.append(done)

        for n, ref, main in ((DR, d, d_in), (RR, r, r_in)):
            copy(main, ref.at[:, pl.ds(128, COLS)], ins)
        for src, dst in ((lh_in, lh), (ll_in, ll), (gh_in.at[pl.ds(0, 6)], gh), (gl_in.at[pl.ds(0, 6)], gl), (gsh_in, gsh), (gsl_in, gsl), (rc0_in, rc0), (rc1_in, rc1), (rc2_in, rc2), (rc3_in, rc3)):
            copy(src, dst, ins)

        def put(hi_ref, lo_ref, r0, c0, x):
            hi, lo = split(x)
            hi_ref[r0 : r0 + x.shape[0], c0 : c0 + x.shape[1]] = hi
            lo_ref[r0 : r0 + x.shape[0], c0 : c0 + x.shape[1]] = lo

        zero = jnp.zeros((32, EXT), BF16)
        for ref in (rh, rl):
            ref[0:32, :] = zero
            ref[WIN - 32 : WIN, :] = zero
        for at, n, ref, hi, lo in ((0, DR, d, dh, dl), (1, RR, r, rh, rl)):
            cols = slice(128 * at, 128 * at + 128)
            rows = slice(DR * at, DR * at + n)
            base = (DR + BAND) * at
            ref[:, 0:128] = col_l[:, cols]
            ref[:, 128 + COLS :] = col_r[:, cols]
            for first, main, skip, left_c, right_c in (
                (64 - n, row_u, BAND, cor_ul, cor_ur),
                (192, row_d, 0, cor_dl, cor_dr),
            ):
                part = slice(base + skip, base + skip + n)
                put(hi, lo, first, 128, main[rows, :])
                put(hi, lo, first, 0, left_c[part, :])
                put(hi, lo, first, 128 + COLS, right_c[part, :])
            ins[at].wait()
            put(hi, lo, 64, 0, ref[...])
        for done in ins[2:]:
            done.wait()
        ds, rs = (dh[...], dl[...]), (rh[...], rl[...])

        def left(a, b):
            return (lh[a:b, :], ll[a:b, :])

        put(sh, sl, 0, 0, dot3(left(0, 176), ds))
        put(sh, sl, 176, 0, dot3(left(0, 128), rs))
        put(th, tl, 0, 0, dot3(left(224, 352), ds))
        rd = dot2r(lh[176:224, :], ds)
        rres = dot2r(lh[176:224, :], rs)
        y3[...] = dot3(left(352, 480), ds)
        y2[...] = dot3(left(224, 352), rs)
        z[0:16, :] = dot3(left(480, 496), ds)
        z[16:32, :] = dot2r(lh[496:512, :], ds)
        copy(y3, y3_out, outs)
        copy(y2, y2_out, outs)
        copy(z, z_out, outs)
        for g in range(4):
            v, i, o = VARIANT[g], slice(256 * g, 256 * g + 512), slice(256 * g, 256 * g + 256)
            c1[:, o] = dot3((sh[:, i], sl[:, i]), (gh[v], gl[v]))
            d2[:, o] = dot3((th[:, i], tl[:, i]), (gh[3 + v], gl[3 + v]))
        t = slice(128, 128 + COLS)
        p1 = c1[0:128, :]
        q[...] = p1 + delta * d[:, t]
        d2[...] = d2[...] + delta * (2.0 * p1 + delta * d[:, t])
        r1[...] = c1[176:304, :] + delta * r[:, t]
        copy(q, q_out, outs)
        copy(d2, d2_out, outs)
        copy(r1, r1_out, outs)
        qv, rv, aq, ar = q[...], r[:, t], d2[...], r1[...]
        s_dq = total(d[:, t] * qv)
        e_rr = total(rv * (3.0 * rv - 3.0 * c * ar) + c * c * (ar * ar)) * c
        e_qq = total(qv * (3.0 * qv - 3.0 * c * aq) + c * c * (aq * aq)) * c
        e_rq = total(rv * (3.0 * qv - 3.0 * c * aq) + c * c * (ar * aq)) * c
        sides = [
            dot3((sh[128:176, i], sl[128:176, i]), (gsh[k], gsl[k])) for k, i in ((0, slice(0, 256)), (1, slice(COLS, EXT)))
        ]
        fq = jnp.concatenate([sides[0], c1[128:176, :], sides[1]], axis=1) + delta * rd
        f = dot2(split(jnp.concatenate([fq, rres], axis=0)), rc0[...])
        f0[...] = f
        pair = (f[0:48], f[48:96])
        weight = 4.0
        for level, cols in ((0, rc1), (1, rc2), (2, rc3)):
            dg, cp = diag[level], coupling[level]
            sm = W / dg
            shape = pair[0].shape
            inside = level_mask(level, shape, slab, gc, n_slab, n_gc)
            mine = tile_mask(level, shape)
            bq, br = operator(pair[0], dg, cp), operator(pair[1], dg, cp)
            own_q, own_r = jnp.where(mine, pair[0], 0.0), jnp.where(mine, pair[1], 0.0)
            e_rr = e_rr + weight * total(own_r * (2.0 * sm * pair[1] - (sm * sm) * br))
            e_qq = e_qq + weight * total(own_q * (2.0 * sm * pair[0] - (sm * sm) * bq))
            e_rq = e_rq + weight * total(own_r * (2.0 * sm * pair[0] - (sm * sm) * bq))
            weight = 2.0 * weight
            rest_q = jnp.where(inside, pair[0] - sm * bq, 0.0)
            rest_r = jnp.where(inside, pair[1] - sm * br, 0.0)
            low = dot2(split(jnp.concatenate([rest_q, rest_r], axis=0)), cols[...])
            if level < 2:
                n, m = (24, 48) if level == 0 else (16, 24)
                half = jnp.where((iota((n, m), 1) >> 1) == iota((n, m), 0), 0.5, 0.0).astype(BF16)
                pair = (dot2r(half, split(low[0:m])), dot2r(half, split(low[m : 2 * m])))
                keep = level_mask(level + 1, pair[0].shape, slab, gc, n_slab, n_gc)
                pair = (jnp.where(keep, pair[0], 0.0), jnp.where(keep, pair[1], 0.0))
                if level == 0:
                    f1[0:n, :], f1[n : 2 * n, :] = pair
        copy(f0, f0_out, outs)
        copy(f1, f1_out, outs)
        i, lane = iota((16, 128), 0), iota((16, 128), 1)
        pick = (i >= 2) & (i < 10) & (((i - 2) >> 1) == (lane >> 5))
        gq = jnp.sum(jnp.where(pick, low[0:16], 0.0), axis=0, keepdims=True) * 0.5
        gr = jnp.sum(jnp.where(pick, low[16:32], 0.0), axis=0, keepdims=True) * 0.5
        lane = iota((1, 128), 1)
        sums = jnp.zeros((1, 128), F32)
        for k, x in enumerate((s_dq, e_rr, e_rq, e_qq)):
            sums = jnp.where(lane == k, x, sums)
        pay[:, 0:128] = jnp.broadcast_to(gq, (n_dev, 128))
        pay[:, 128:256] = jnp.broadcast_to(gr, (n_dev, 128))
        pay[:, 256:384] = jnp.broadcast_to(sums, (n_dev, 128))
        for done in outs:
            done.wait()

    return kernel


def outer_kernel(n_slab, n_gc):
    def kernel(idx, damping, diag, coupling, y3_in, y2_in, z_in, f0_in, oh_in, ol_in, gh_in, gl_in, gsh_in, gsl_in,
               rc0_in, rc1_in, rc2_in, band_u, band_d, cor_ul, cor_ur, cor_dl, cor_dr, p3_out, p2_out, f2_out,
               y3, y2, z, f0, oh, ol, gh, gl, gsh, gsl, rc0, rc1, rc2, p3, p2, f2, th, tl, ah, al, sem):
        slab, gc = idx[0], idx[1]
        delta = damping[0]
        ins, outs = [], []

        def copy(src, dst, todo):
            todo.append(pltpu.make_async_copy(src, dst, sem.at[len(ins) + len(outs)]))
            todo[-1].start()

        for src, dst in (
            (oh_in, oh), (ol_in, ol), (y3_in, y3), (y2_in, y2), (gh_in, gh), (gl_in, gl), (z_in, z), (f0_in, f0),
            (gsh_in, gsh), (gsl_in, gsl), (rc0_in, rc0), (rc1_in, rc1), (rc2_in, rc2),
        ):
            copy(src, dst, ins)
        ah[2 * BAND :, :], al[2 * BAND :, :] = (jnp.zeros((128 - 2 * BAND, EXT), BF16),) * 2
        for done in ins[:4]:
            done.wait()
        for at, y in ((0, y3), (1, y2)):
            rows = slice(BAND * at, BAND * at + BAND)
            base = (DR + BAND) * at
            n = (DR, RR)[at]
            for to, main, skip, left_c, right_c in ((0, band_u, 0, cor_ul, cor_ur), (BAND, band_d, n, cor_dl, cor_dr)):
                part = slice(base + skip, base + skip + BAND)
                for lane, x in ((0, left_c[part, :]), (128, main[rows, :]), (128 + COLS, right_c[part, :])):
                    hi, lo = split(x)
                    ah[to : to + BAND, lane : lane + x.shape[1]] = hi
                    al[to : to + BAND, lane : lane + x.shape[1]] = lo
            left = slice(128 * at, 128 * at + 128)
            outer = (ah[...], al[...])
            th[at, 0:ROWS], tl[at, 0:ROWS] = split(y[...] + dot3((oh[left], ol[left]), outer))
            if at == 0:
                part_q = dot3((oh[256:272], ol[256:272]), outer)
            else:
                far_r = dot2r(oh[272:288], outer)
        for done in ins[4:]:
            done.wait()
        e = split(z[0:16, :] + part_q)
        cols = [dot3((e[0][:, 0:256], e[1][:, 0:256]), (gsh[0], gsl[0]))]
        for g in range(4):
            v, i, o = VARIANT[g], slice(256 * g, 256 * g + 512), slice(256 * g, 256 * g + 256)
            cols.append(dot3((e[0][:, i], e[1][:, i]), (gh[v], gl[v])))
            for at, p, power in ((0, p3, 6), (1, p2, 3)):
                p[:, o] = dot3((th[at, :, i], tl[at, :, i]), (gh[power + v], gl[power + v]))
        cols.append(dot3((e[0][:, COLS:], e[1][:, COLS:]), (gsh[1], gsl[1])))
        copy(p3, p3_out, outs)
        copy(p2, p2_out, outs)
        far_q = jnp.concatenate(cols, axis=1) + delta * z[16:32, :]
        far = dot2(split(jnp.concatenate([far_q, far_r], axis=0)), rc0[...])
        pair = [
            jnp.concatenate([far[16 * k : 16 * k + 8], f0[48 * k : 48 * k + 48], far[16 * k + 8 : 16 * k + 16]], axis=0)
            for k in range(2)
        ]
        for level, matrix in ((0, rc1), (1, rc2)):
            dg, cp = diag[level], coupling[level]
            sm = W / dg
            m = 64 >> level
            inside = level_mask(level, pair[0].shape, slab, gc, n_slab, n_gc, 16)
            rest = [jnp.where(inside, x - sm * operator(x, dg, cp), 0.0) for x in pair]
            low = dot2(split(jnp.concatenate(rest, axis=0)), matrix[...])
            half = jnp.where((iota((m // 2, m), 1) >> 1) == iota((m // 2, m), 0), 0.5, 0.0).astype(BF16)
            pair = [dot2r(half, split(low[k * m : k * m + m])) for k in range(2)]
            keep = level_mask(level + 1, pair[0].shape, slab, gc, n_slab, n_gc, 16)
            pair = [jnp.where(keep, x, 0.0) for x in pair]
        f2[0:16, :], f2[16:32, :] = pair
        copy(f2, f2_out, outs)
        for done in outs:
            done.wait()

    return kernel


def final_kernel(n_slab, n_gc, n_grp):
    n_col = n_gc // n_grp

    def kernel(idx, damping, rho_in, diag, coupling, got, swap, d2_in, r1_in, p3_in, p2_in, q_in, r_in, d_in, sol_in,
               f0_in, f1_in, f2_in, pc0_in, pc1_in, pc2_in, pc3_in,
               o_sol, o_res, o_pre, o_dir, o_energy,
               d2, r1, p3, p2, q, r, d, sol, f0, f1, f2, pc0, pc1, pc2, pc3,
               vs, v_sol, v_res, v_pre, v_dir, sem):
        ins, outs = [], []

        def copy(src, dst, todo):
            done = pltpu.make_async_copy(src, dst, sem.at[len(ins) + len(outs)])
            done.start()
            todo.append(done)

        for src, dst in (
            (r_in, r), (q_in, q), (sol_in, sol), (d_in, d), (f0_in, f0), (f1_in, f1), (f2_in, f2), (pc1_in, pc1), (pc2_in, pc2),
            (pc3_in, pc3), (pc0_in, pc0), (d2_in, d2), (r1_in, r1), (p3_in, p3), (p2_in, p2),
        ):
            copy(src, dst, ins)
        slab, gc = idx[0], idx[1]
        delta, rho = damping[0], rho_in[0]
        c = W / (1.0 + delta)
        lane = iota((1, 128), 1)
        sums = jnp.sum(got[:, 256:384] + swap[:, 256:384], axis=0, keepdims=True)
        s_dq, e_rr, e_rq, e_qq = (
            jnp.sum(jnp.where(lane == k, sums, 0.0), axis=1, keepdims=True) for k in range(4)
        )
        alpha = rho / s_dq
        dg, cp = diag[3], coupling[3]
        first = (iota((n_gc, 128), 1) & 31) == 0
        last = (iota((n_gc, 128), 1) & 31) == 31
        top, bottom = iota((n_gc, 128), 1) < 32, iota((n_gc, 128), 1) >= 96
        left_end, right_end = iota((n_gc, 128), 0) == 0, iota((n_gc, 128), 0) == n_gc - 1
        mine = gc < n_col
        rhs = []
        for s in range(n_slab):
            at = s * n_col
            a, b = (x[at : at + n_col, 128:256] - alpha * x[at : at + n_col, 0:128] for x in (got, swap))
            rhs.append(jnp.concatenate([jnp.where(mine, a, b), jnp.where(mine, b, a)], axis=0))
        zero = jnp.zeros((n_gc, 128), F32)
        v = [W * x / dg for x in rhs]
        for _ in range(3):
            ups = [pltpu.roll(x, 32, 1) for x in v]
            downs = [pltpu.roll(x, 96, 1) for x in v]
            new = []
            for s in range(n_slab):
                x = v[s]
                low = jnp.where(left_end, 0.0, pltpu.roll(pltpu.roll(x, 97, 1), 1, 0))
                high = jnp.where(right_end, 0.0, pltpu.roll(pltpu.roll(x, 31, 1), n_gc - 1, 0))
                beside_x = jnp.where(first, low, pltpu.roll(x, 1, 1))
                beside_x = beside_x + jnp.where(last, high, pltpu.roll(x, 127, 1))
                beside_x = beside_x + jnp.where(top, ups[s - 1] if s > 0 else zero, ups[s])
                beside_x = beside_x + jnp.where(bottom, downs[s + 1] if s < n_slab - 1 else zero, downs[s])
                new.append(x + W * (rhs[s] - (dg * x - cp * beside_x)) / dg)
            v = new
        e3 = total(sum(a * b for a, b in zip(rhs, v)))
        energy = e_rr - alpha * (2.0 * e_rq) + (alpha * alpha) * e_qq + 32.0 * e3
        o_energy[...] = energy
        pitch = n_gc + 16
        vs[...] = jnp.zeros(vs.shape, F32)
        for s in range(n_slab):
            at = (s + 1) * pitch + 8
            vs[at : at + n_gc, :] = v[s]
        v3 = jnp.zeros((8, 128), F32)
        lanes, rows8 = iota((1, 128), 1), iota((8, 128), 0)
        for k, i in ((-1, 3), (0, 0), (0, 1), (0, 2), (0, 3), (1, 0)):
            at = (slab + 1 + k) * pitch + 8 + gc
            mid, lo, hi = (vs[pl.ds(at + x, 1), :] for x in (0, -1, 1))
            line = pltpu.roll(mid, (8 - 32 * i) % 128, 1)
            line = jnp.where(lanes == 7, pltpu.roll(lo, (8 - 32 * i - 32) % 128, 1), line)
            line = jnp.where(lanes == 40, pltpu.roll(hi, (8 - 32 * i + 32) % 128, 1), line)
            line = jnp.where((lanes >= 7) & (lanes <= 40), line, 0.0)
            v3 = jnp.where(rows8 == 4 * k + i + 1, line, v3)
        for done in ins[:4]:
            done.wait()
        v_res[...] = r[...] - alpha * q[...]
        copy(v_res, o_res, outs)
        v_sol[...] = sol[...] + alpha * d[...]
        copy(v_sol, o_sol, outs)
        for done in ins[4:15]:
            done.wait()
        own = pltpu.roll(f2[16:32, :] - alpha * f2[0:16, :], 14, 0)
        own = jnp.where(iota((16, 128), 0) < 12, own, 0.0)
        f = [f0[48:96, :] - alpha * f0[0:48, :], f1[24:48, :] - alpha * f1[0:24, :], own]
        low = v3
        for level, cols in ((2, pc3), (1, pc2), (0, pc1)):
            dg, cp = diag[level], coupling[level]
            sm = W / dg
            n, m = f[level].shape[0], low.shape[0]
            double = hot((iota((n, m), 0) >> 1) == iota((n, m), 1))
            wide = dot2r(double, split(dot2(split(low), cols[...])))
            inside = level_mask(level, f[level].shape, slab, gc, n_slab, n_gc)
            x = jnp.where(inside, sm * f[level] + wide, 0.0)
            low = jnp.where(inside, x + sm * (f[level] - operator(x, dg, cp)), 0.0)
        four = hot((iota((ROWS, 48), 0) >> 2) + 8 == iota((ROWS, 48), 1))
        spread = split(dot2r(four, split(low)))
        au = r1[...] - alpha * d2[...]
        a2r = p2[...] + (2.0 * delta) * r1[...] - (delta * delta) * r[...]
        a3d = p3[...] + delta * (3.0 * d2[...] - delta * (3.0 * q[...] - delta * d[...]))
        smooth = c * (3.0 * v_res[...] - (3.0 * c) * au + (c * c) * (a2r - alpha * a3d))
        pre = smooth + dot2(spread, pc0[...])
        v_pre[...] = pre
        copy(v_pre, o_pre, outs)
        v_dir[...] = pre + (energy / rho) * d[...]
        copy(v_dir, o_dir, outs)
        for done in outs:
            done.wait()

    return kernel


def call(kernel, specs, outs, out_specs, scratch, sems=0):
    where = {"s": pltpu.SMEM, "v": pltpu.VMEM, "h": pltpu.HBM}
    if INTERPRET:
        where["h"] = pl.ANY

    def out(x, shape, kind):
        if x == "h" and not INTERPRET:
            return pltpu.HBM(shape, kind)
        return jax.ShapeDtypeStruct(shape, kind)

    run = pl.pallas_call(
        kernel,
        out_shape=[out(x, s, t) for x, (s, t) in zip(out_specs, outs)],
        in_specs=[pl.BlockSpec(memory_space=where[x]) for x in specs],
        out_specs=[pl.BlockSpec(memory_space=where[x]) for x in out_specs],
        scratch_shapes=[pltpu.VMEM(s, t) for s, t in scratch] + ([pltpu.SemaphoreType.DMA((sems,))] if sems else []),
        compiler_params=pltpu.CompilerParams(vmem_limit_bytes=40 * 1024 * 1024),
        interpret=INTERPRET,
    )

    def apply(*args):
        if INTERPRET:
            return run(*args)
        return run(*(pltpu.with_memory_space_constraint(a, pltpu.HBM) if x == "h" else a for x, a in zip(specs, args)))

    return apply


def run_copies(sem, pairs):
    todo = []
    for k, (src, dst) in enumerate(pairs):
        todo.append(pltpu.make_async_copy(src, dst, sem.at[k]))
        todo[-1].start()
    for done in todo:
        done.wait()


def edges_kernel(d, r, row_u, row_d, cor_ul, cor_ur, cor_dl, cor_dr, col_l, col_r, band_u, band_d, sem):
    pairs = []
    for n, at, x in ((DR, 0, d), (RR, DR, r)):
        pairs.append((x.at[pl.ds(0, n), :], row_u.at[pl.ds(at, n), :]))
        pairs.append((x.at[pl.ds(ROWS - n, n), :], row_d.at[pl.ds(at, n), :]))
    for n, at, x in ((DR + BAND, 0, d), (RR + BAND, DR + BAND, r)):
        for first, lane, ref in (
            (0, 0, cor_ul),
            (0, COLS - 128, cor_ur),
            (ROWS - n, 0, cor_dl),
            (ROWS - n, COLS - 128, cor_dr),
        ):
            pairs.append((x.at[pl.ds(first, n), pl.ds(lane, 128)], ref.at[pl.ds(at, n), :]))
    for at, x in ((0, d), (128, r)):
        pairs.append((x.at[:, pl.ds(0, 128)], col_l.at[:, pl.ds(at, 128)]))
        pairs.append((x.at[:, pl.ds(COLS - 128, 128)], col_r.at[:, pl.ds(at, 128)]))
    for n, at, x in ((DR, 0, d), (RR, BAND, r)):
        pairs.append((x.at[pl.ds(n, BAND), :], band_u.at[pl.ds(at, BAND), :]))
        pairs.append((x.at[pl.ds(ROWS - n - BAND, BAND), :], band_d.at[pl.ds(at, BAND), :]))
    run_copies(sem, pairs)


def solution(mesh):
    n_grp, n_slab, n_col = mesh.shape["grp"], mesh.shape["slab"], mesh.shape["col"]
    n_gc = n_grp * n_col
    n_dev = n_slab * n_col

    def body(sol, r, d, row_taps, col_taps, damping, rho, diag, coupling):
        idx = jnp.stack([lax.axis_index("slab"), lax.axis_index(GC)]).astype(jnp.int32)
        row_u, row_d, cor_ul, cor_ur, cor_dl, cor_dr, col_l, col_r, band_u, band_d = call(
            edges_kernel,
            "hh",
            [((DR + RR, COLS), F32)] * 2
            + [((DR + RR + 2 * BAND, 128), F32)] * 4
            + [((ROWS, 256), F32)] * 2
            + [((2 * BAND, COLS), F32)] * 2,
            "v" * 10,
            [],
            20,
        )(d, r)

        def send(x, down, right):
            def at(i, j):
                return (j // n_col * n_slab + i) * n_col + j % n_col

            pairs = []
            for i in range(n_slab):
                for j in range(n_gc):
                    if 0 <= i + down < n_slab and 0 <= j + right < n_gc:
                        pairs.append((at(i, j), at(i + down, j + right)))
            return lax.ppermute(x, ("grp", "slab", "col"), pairs)

        from_u, from_d = send(row_d, 1, 0), send(row_u, -1, 0)
        from_ul, from_ur = send(cor_dr, 1, 1), send(cor_dl, 1, -1)
        from_dl, from_dr = send(cor_ur, -1, 1), send(cor_ul, -1, -1)
        from_l, from_r = send(col_r, 0, 1), send(col_l, 0, -1)
        from_bu, from_bd = send(band_d, 1, 0), send(band_u, -1, 0)
        par = (damping[None], rho[None], diag, coupling)
        mat_shapes = [((512, WIN), BF16)] * 2 + [((9, 512, 256), BF16)] * 2 + [((2, 256, 128), BF16)] * 2
        mat_shapes += [((288, 128), BF16)] * 2
        mat_shapes += [((EXT, 384), BF16), ((384, 256), BF16), ((256, 128), BF16), ((128, 128), BF16)]
        back_shapes = [((384, COLS), BF16), ((256, 384), BF16), ((128, 256), BF16), ((128, 128), BF16)]
        mats = call(
            matrices_kernel(n_slab, n_gc), "sss", mat_shapes + back_shapes, "h" * 16, mat_shapes + back_shapes, 16
        )(idx, row_taps, col_taps)
        lh, ll, gh, gl, gsh, gsl, oh, ol, rc0, rc1, rc2, rc3, pc0, pc1, pc2, pc3 = mats
        results = [((ROWS, COLS), F32)] * 3 + [((ROWS, EXT), F32)] * 2
        results += [((32, EXT), F32), ((96, 384), F32), ((48, 256), F32)]
        q, d2, r1, y3, y2, z, f0, f1, pay = call(
            halo_kernel(n_slab, n_gc, n_grp),
            "s" * 5 + "hh" + "v" * 8 + "h" * 10,
            results + [((n_dev, 384), F32)],
            "h" * 8 + "v",
            [((ROWS, EXT), F32)] * 2
            + [((512, WIN), BF16)] * 2
            + [((6, 512, 256), BF16)] * 2
            + [((2, 256, 128), BF16)] * 2
            + mat_shapes[8:]
            + results
            + [((WIN, EXT), BF16)] * 4
            + [((304, EXT), BF16)] * 2
            + [((128, EXT), BF16)] * 2
            + [((304, COLS), F32)],
            24,
        )(idx, *par, d, r, from_u, from_d, from_l, from_r, from_ul, from_ur, from_dl, from_dr, lh, ll, gh, gl, gsh, gsl, rc0, rc1, rc2, rc3)
        got = lax.all_to_all(pay, ("slab", "col"), 0, 0, tiled=True)
        swap = lax.ppermute(got, "grp", [(i, (i + 1) % n_grp) for i in range(n_grp)])
        tile = ((ROWS, COLS), F32)
        p3, p2, f2 = call(
            outer_kernel(n_slab, n_gc),
            "s" * 4 + "h" * 13 + "v" * 6,
            [tile] * 2 + [((32, 128), F32)],
            "hhh",
            [((ROWS, EXT), F32)] * 2
            + [((32, EXT), F32), ((96, 384), F32)]
            + [((288, 128), BF16)] * 2
            + [((9, 512, 256), BF16)] * 2
            + [((2, 256, 128), BF16)] * 2
            + mat_shapes[8:11]
            + [tile] * 2
            + [((32, 128), F32)]
            + [((2, ROWS, EXT), BF16)] * 2
            + [((128, EXT), BF16)] * 2,
            16,
        )(idx, damping[None], diag, coupling, y3, y2, z, f0, oh, ol, gh, gl, gsh, gsl, rc0, rc1, rc2,
          from_bu, from_bd, from_ul, from_ur, from_dl, from_dr)
        n_sol, n_res, pre, n_dir, energy = call(
            final_kernel(n_slab, n_gc, n_grp),
            "s" * 5 + "vv" + "h" * 15,
            [tile] * 4 + [((1, 1), F32)],
            "hhhhv",
            [tile] * 8
            + [((96, 384), F32), ((48, 256), F32), ((32, 128), F32)]
            + back_shapes
            + [(((n_slab + 2) * (n_gc + 16), 128), F32)]
            + [tile] * 4,
            20,
        )(idx, *par, got, swap, d2, r1, p3, p2, q, r, d, sol, f0, f1, f2, pc0, pc1, pc2, pc3)
        return n_sol, n_res, pre, n_dir, energy[0, 0]

    tile, rep = P("slab", GC), P()
    return jax.shard_map(
        body,
        mesh=mesh,
        in_specs=(tile,) * 3 + (rep,) * 6,
        out_specs=(tile,) * 4 + (rep,),
        check_vma=False,
    )
```

```python
import jax
import jax.numpy as jnp
from jax import lax
from jax.experimental import pallas as pl
from jax.experimental.pallas import tpu as pltpu
from jax.sharding import PartitionSpec as P


INTERPRET = False
W = 2.0 / 3.0
TAPS = 31
H = TAPS // 2
ROWS, COLS = 128, 1024
EXT = COLS + 256
WIN = ROWS + 128
DR, RR = 64, 32
IN0 = (0, 128, 384, 640, 768)
VARIANT = (0, 1, 1, 1, 2)
GC = ("grp", "col")
F32, BF16 = jnp.float32, jnp.bfloat16


def iota(shape, dim):
    return lax.broadcasted_iota(jnp.int32, shape, dim)


def split(x):
    high = x.astype(BF16)
    return high, (x - high.astype(F32)).astype(BF16)


def dot(a, b):
    return jnp.dot(a, b, preferred_element_type=F32)


def dot3(a, b):
    (ah, al), (bh, bl) = a, b
    return dot(ah, bh) + (dot(ah, bl) + dot(al, bh))


def dot2(a, b):
    return dot(a[0], b) + dot(a[1], b)


def dot2r(a, b):
    return dot(a, b[0]) + dot(a, b[1])


def hot(cond):
    return jnp.where(cond, 1.0, 0.0).astype(BF16)


def total(x):
    return jnp.sum(jnp.sum(x, axis=0, keepdims=True), axis=1, keepdims=True)


def dot_t(a, b):
    def nt(x, y):
        return lax.dot_general(x, y, (((1,), (1,)), ((), ())), preferred_element_type=F32)

    (ah, al), (bh, bl) = a, b
    return nt(ah, bh) + (nt(ah, bl) + nt(al, bh))


def toeplitz(taps):
    sum_taps = taps[0]
    for t in range(1, TAPS):
        sum_taps = sum_taps + taps[t]
    lane = iota((8, 384), 1)
    base = jnp.zeros((8, 384), F32)
    for t in range(TAPS):
        base = jnp.where(lane == 64 + H - t, taps[t], base)
    base = base / jnp.full((8, 384), sum_taps, F32)
    return pltpu.roll(jnp.broadcast_to(base[0:1], (256, 384)), 0, 1, stride=1, stride_axis=0)


def gram(kt, first, limit):
    ks = split(kt)
    left = ks
    if first is not None:
        m = iota((256, 384), 1) + (first - 128)
        left = split(jnp.where((m >= 0) & (m < limit), kt, 0.0))
    return left, ks


def block_powers(kt, first, limit):
    left, ks = gram(kt, first, limit)
    wide = dot_t(left, ks)
    g1 = dot_t(left, (ks[0][64:192], ks[1][64:192]))
    if first is not None:
        i = iota((256, 128), 0) + (first - 64)
        g1 = jnp.where((i >= 0) & (i < limit), g1, 0.0)
    g1s = split(g1)
    return g1s, split(dot3(split(wide), g1s))


def matrices_kernel(n_slab, n_gc):
    def kernel(idx, rt, ct, *refs):
        outs, scratch, sem = refs[:12], refs[12:24], refs[24]
        lh, ll, gh, gl, rc0, rc1, rc2, rc3, pc0, pc1, pc2, pc3 = scratch
        slab, gc = idx[0], idx[1]
        gh[...], gl[...] = jnp.zeros(gh.shape, BF16), jnp.zeros(gl.shape, BF16)
        kt = toeplitz(ct)
        inner = block_powers(kt, None, None)
        low = block_powers(kt, gc * COLS, n_gc * COLS)
        high = block_powers(kt, gc * COLS + COLS - 128, n_gc * COLS)
        has_l = jnp.where(gc > 0, 1.0, 0.0).astype(F32)
        has_r = jnp.where(gc < n_gc - 1, 1.0, 0.0).astype(F32)
        for power in range(2):
            for at, ref in enumerate((gh, gl)):
                mid = inner[power][at]
                wide = mid.astype(F32)
                outer_l, outer_r = (wide * has_l).astype(BF16), (wide * has_r).astype(BF16)
                for v, off, blocks in (
                    (0, 0, (outer_l, low[power][at])),
                    (1, 128, (mid, mid)),
                    (2, 256, (high[power][at], outer_r)),
                ):
                    for b in range(2):
                        start = off + 128 * b - 64
                        lo, hi = max(0, start), min(512, start + 256)
                        ref[3 * power + v, lo:hi, 128 * b : 128 * b + 128] = blocks[b][lo - start : hi - start]
        first, limit = slab * ROWS, n_slab * ROWS
        left, ks = gram(toeplitz(rt), first, limit)
        g1 = dot_t(left, ks)
        g1s = split(g1)
        lh[0:128, :], ll[0:128, :] = g1s[0][64:192, :], g1s[1][64:192, :]
        c, i = iota((48, WIN), 0), iota((48, WIN), 1)
        inside = (i + (first - 64) >= 0) & (i + (first - 64) < limit)
        rr = jnp.where((i - 32 >= 4 * c) & (i - 32 < 4 * c + 4) & inside, 0.25, 0.0).astype(BF16)
        lh[128:176, :], ll[128:176, :] = split(dot2r(rr, g1s))
        lh[176:224, :], ll[176:224, :] = rr, jnp.zeros_like(rr)
        k = iota((128, WIN), 1) + (first - 64)
        tile = split(jnp.where((k >= 0) & (k < limit), g1[64:192, :], 0.0))
        lh[224:352, :], ll[224:352, :] = split(dot3(tile, g1s))
        rc0[...] = hot((iota((EXT, 384), 0) >> 2) + 32 == iota((EXT, 384), 1))
        rc1[...] = hot((iota((384, 256), 0) >> 1) == iota((384, 256), 1))
        rc2[...] = hot((iota((256, 128), 0) >> 1) == iota((256, 128), 1))
        rc3[...] = hot((iota((128, 128), 0) >> 1) - 8 == (iota((128, 128), 1) & 31))
        pc0[...] = hot(iota((384, COLS), 0) == (iota((384, COLS), 1) >> 2) + 64)
        pc1[...] = hot(iota((256, 384), 0) == (iota((256, 384), 1) >> 1))
        pc2[...] = hot(iota((128, 256), 0) == (iota((128, 256), 1) >> 1))
        pc3[...] = hot(iota((128, 128), 0) == (iota((128, 128), 1) >> 1))
        run_copies(sem, list(zip(scratch, outs)))

    return kernel


def level_mask(level, shape, slab, gc, n_slab, n_gc):
    height, width = 32 >> level, 256 >> level
    i = iota(shape, 0) - (8 >> level) + slab * height
    j = iota(shape, 1) - (64 >> level) + gc * width
    return (i >= 0) & (i < n_slab * height) & (j >= 0) & (j < n_gc * width)


def tile_mask(level, shape):
    i, j = iota(shape, 0) - (8 >> level), iota(shape, 1) - (64 >> level)
    return (i >= 0) & (i < 32 >> level) & (j >= 0) & (j < 256 >> level)


def beside(v):
    n, m = v.shape
    rows = pltpu.roll(v, 1, 0) + pltpu.roll(v, n - 1, 0)
    return rows + pltpu.roll(v, 1, 1) + pltpu.roll(v, m - 1, 1)


def operator(v, dg, cp):
    return dg * v - cp * beside(v)


def halo_kernel(n_slab, n_gc, n_grp):
    n_dev = n_slab * n_gc // n_grp

    def kernel(idx, damping, rho_in, diag, coupling, d_in, r_in, row_u, row_d, col_l, col_r, cor_l, cor_r,
               lh_in, ll_in, gh_in, gl_in, rc0_in, rc1_in, rc2_in, rc3_in,
               q_out, d2_out, r1_out, f0_out, f1_out, f2_out, e_up, e_dn, pay,
               d, r, lh, ll, gh, gl, rc0, rc1, rc2, rc3, q, d2, r1, f0, f1, f2,
               dh, dl, rh, rl, sh, sl, th, tl, c1, sem):
        slab, gc = idx[0], idx[1]
        delta = damping[0]
        c = W / (1.0 + delta)
        ins, outs = [], []

        def copy(src, dst, todo):
            done = pltpu.make_async_copy(src, dst, sem.at[len(ins) + len(outs)])
            done.start()
            todo.append(done)

        for n, ref, main in ((DR, d, d_in), (RR, r, r_in)):
            copy(main, ref.at[:, pl.ds(128, COLS)], ins)
        for src, dst in ((lh_in, lh), (ll_in, ll), (gh_in, gh), (gl_in, gl), (rc0_in, rc0), (rc1_in, rc1), (rc2_in, rc2), (rc3_in, rc3)):
            copy(src, dst, ins)

        def put(hi_ref, lo_ref, r0, c0, x):
            hi, lo = split(x)
            hi_ref[r0 : r0 + x.shape[0], c0 : c0 + x.shape[1]] = hi
            lo_ref[r0 : r0 + x.shape[0], c0 : c0 + x.shape[1]] = lo

        zero = jnp.zeros((32, EXT), BF16)
        for ref in (rh, rl):
            ref[0:32, :] = zero
            ref[WIN - 32 : WIN, :] = zero
        for at, n, ref, hi, lo in ((0, DR, d, dh, dl), (1, RR, r, rh, rl)):
            cols = slice(128 * at, 128 * at + 128)
            rows = slice(DR * at, DR * at + n)
            ref[:, 0:128] = col_l[:, cols]
            ref[:, 128 + COLS :] = col_r[:, cols]
            for first, lane, main in ((64 - n, 0, row_u), (192, 128, row_d)):
                put(hi, lo, first, 128, main[rows, :])
                put(hi, lo, first, 0, cor_l[rows, lane : lane + 128])
                put(hi, lo, first, 128 + COLS, cor_r[rows, lane : lane + 128])
            ins[at].wait()
            put(hi, lo, 64, 0, ref[...])
        for done in ins[2:]:
            done.wait()
        ds, rs = (dh[...], dl[...]), (rh[...], rl[...])

        def left(a, b):
            return (lh[a:b, :], ll[a:b, :])

        put(sh, sl, 0, 0, dot3(left(0, 176), ds))
        put(sh, sl, 176, 0, dot3(left(0, 128), rs))
        put(th, tl, 0, 0, dot3(left(224, 352), ds))
        rd = dot2r(lh[176:224, :], ds)
        rres = dot2r(lh[176:224, :], rs)
        for g in range(5):
            a, v, o = IN0[g], VARIANT[g], slice(256 * g, 256 * g + 256)
            c1[:, o] = dot3((sh[:, a : a + 512], sl[:, a : a + 512]), (gh[v], gl[v]))
            d2[:, o] = dot3((th[:, a : a + 512], tl[:, a : a + 512]), (gh[3 + v], gl[3 + v]))
        t = slice(128, 128 + COLS)
        p1 = c1[0:128, :]
        q[...] = c1[0:128, t] + delta * d[:, t]
        d2[...] = d2[...] + delta * (2.0 * p1 + delta * d[...])
        r1[...] = c1[176:304, :] + delta * r[...]
        copy(q, q_out, outs)
        copy(d2, d2_out, outs)
        copy(r1, r1_out, outs)
        near = iota((32, 128), 1) < 64
        for ref, rows in ((e_dn, slice(96, 128)), (e_up, slice(0, 32))):
            for at, x in ((0, d2), (32, r1)):
                ref[at : at + 32, 0:COLS] = x[rows, t]
                ref[at : at + 32, COLS:] = jnp.where(near, x[rows, 128 + COLS :], x[rows, 0:128])
        qv, rv, aq, ar = q[...], r[:, t], d2[:, t], r1[:, t]
        s_dq = total(d[:, t] * qv)
        e_rr = total(rv * (3.0 * rv - 3.0 * c * ar) + c * c * (ar * ar)) * c
        e_qq = total(qv * (3.0 * qv - 3.0 * c * aq) + c * c * (aq * aq)) * c
        e_rq = total(rv * (3.0 * qv - 3.0 * c * aq) + c * c * (ar * aq)) * c
        fq = c1[128:176, :] + delta * rd
        f = dot2(split(jnp.concatenate([fq, rres], axis=0)), rc0[...])
        f0[...] = f
        pair = (f[0:48], f[48:96])
        weight = 4.0
        for level, cols in ((0, rc1), (1, rc2), (2, rc3)):
            dg, cp = diag[level], coupling[level]
            sm = W / dg
            shape = pair[0].shape
            inside = level_mask(level, shape, slab, gc, n_slab, n_gc)
            mine = tile_mask(level, shape)
            bq, br = operator(pair[0], dg, cp), operator(pair[1], dg, cp)
            own_q, own_r = jnp.where(mine, pair[0], 0.0), jnp.where(mine, pair[1], 0.0)
            e_rr = e_rr + weight * total(own_r * (2.0 * sm * pair[1] - (sm * sm) * br))
            e_qq = e_qq + weight * total(own_q * (2.0 * sm * pair[0] - (sm * sm) * bq))
            e_rq = e_rq + weight * total(own_r * (2.0 * sm * pair[0] - (sm * sm) * bq))
            weight = 2.0 * weight
            rest_q = jnp.where(inside, pair[0] - sm * bq, 0.0)
            rest_r = jnp.where(inside, pair[1] - sm * br, 0.0)
            low = dot2(split(jnp.concatenate([rest_q, rest_r], axis=0)), cols[...])
            if level < 2:
                n, m = (24, 48) if level == 0 else (16, 24)
                half = jnp.where((iota((n, m), 1) >> 1) == iota((n, m), 0), 0.5, 0.0).astype(BF16)
                pair = (dot2r(half, split(low[0:m])), dot2r(half, split(low[m : 2 * m])))
                keep = level_mask(level + 1, pair[0].shape, slab, gc, n_slab, n_gc)
                pair = (jnp.where(keep, pair[0], 0.0), jnp.where(keep, pair[1], 0.0))
                out = (f1, f2)[level]
                out[0:n, :], out[n : 2 * n, :] = pair
        for ref in (e_up, e_dn):
            ref[64:72, 0:128], ref[64:72, 128:256] = pair[0][2:10, :], pair[1][2:10, :]
            ref[64:72, 256:] = jnp.zeros((8, COLS - 128), F32)
        for src, dst in ((f0, f0_out), (f1, f1_out), (f2, f2_out)):
            copy(src, dst, outs)
        i, lane = iota((16, 128), 0), iota((16, 128), 1)
        pick = (i >= 2) & (i < 10) & (((i - 2) >> 1) == (lane >> 5))
        gq = jnp.sum(jnp.where(pick, low[0:16], 0.0), axis=0, keepdims=True) * 0.5
        gr = jnp.sum(jnp.where(pick, low[16:32], 0.0), axis=0, keepdims=True) * 0.5
        lane = iota((1, 128), 1)
        sums = jnp.zeros((1, 128), F32)
        for k, x in enumerate((s_dq, e_rr, e_rq, e_qq)):
            sums = jnp.where(lane == k, x, sums)
        pay[:, 0:128] = jnp.broadcast_to(gq, (n_dev, 128))
        pay[:, 128:256] = jnp.broadcast_to(gr, (n_dev, 128))
        pay[:, 256:384] = jnp.broadcast_to(sums, (n_dev, 128))
        for done in outs:
            done.wait()

    return kernel


def final_kernel(n_slab, n_gc, n_grp):
    n_col = n_gc // n_grp

    def kernel(idx, damping, rho_in, diag, coupling, got, swap, e_u, e_d, d2_in, r1_in, lh_in, ll_in, gh_in, gl_in, q_in, r_in, d_in, sol_in,
               f0_in, f1_in, f2_in, pc0_in, pc1_in, pc2_in, pc3_in,
               o_sol, o_res, o_pre, o_dir, o_energy,
               d2, r1, lh, ll, gh, gl, q, r, d, sol, f0, f1, f2, pc0, pc1, pc2, pc3,
               uh, ul, yh, yl, vs, kk, v_sol, v_res, v_pre, v_dir, sem):
        ins, outs = [], []

        def copy(src, dst, todo):
            done = pltpu.make_async_copy(src, dst, sem.at[len(ins) + len(outs)])
            done.start()
            todo.append(done)

        for src, dst in (
            (d2_in, d2), (r1_in, r1), (lh_in.at[pl.ds(0, 128), :], lh), (ll_in.at[pl.ds(0, 128), :], ll),
            (gh_in.at[pl.ds(0, 3)], gh), (gl_in.at[pl.ds(0, 3)], gl), (r_in, r), (q_in, q), (sol_in, sol), (d_in, d),
            (f0_in, f0), (f1_in, f1), (f2_in, f2), (pc1_in, pc1), (pc2_in, pc2), (pc3_in, pc3), (pc0_in, pc0),
        ):
            copy(src, dst, ins)
        slab, gc = idx[0], idx[1]
        delta, rho = damping[0], rho_in[0]
        c = W / (1.0 + delta)
        lane = iota((1, 128), 1)
        sums = jnp.sum(got[:, 256:384] + swap[:, 256:384], axis=0, keepdims=True)
        s_dq, e_rr, e_rq, e_qq = (
            jnp.sum(jnp.where(lane == k, sums, 0.0), axis=1, keepdims=True) for k in range(4)
        )
        alpha = rho / s_dq
        dg, cp = diag[3], coupling[3]
        first = (iota((n_gc, 128), 1) & 31) == 0
        last = (iota((n_gc, 128), 1) & 31) == 31
        top, bottom = iota((n_gc, 128), 1) < 32, iota((n_gc, 128), 1) >= 96
        left_end, right_end = iota((n_gc, 128), 0) == 0, iota((n_gc, 128), 0) == n_gc - 1
        mine = gc < n_col
        rhs = []
        for s in range(n_slab):
            at = s * n_col
            a, b = (x[at : at + n_col, 128:256] - alpha * x[at : at + n_col, 0:128] for x in (got, swap))
            rhs.append(jnp.concatenate([jnp.where(mine, a, b), jnp.where(mine, b, a)], axis=0))
        zero = jnp.zeros((n_gc, 128), F32)
        v = [W * x / dg for x in rhs]
        for _ in range(3):
            ups = [pltpu.roll(x, 32, 1) for x in v]
            downs = [pltpu.roll(x, 96, 1) for x in v]
            new = []
            for s in range(n_slab):
                x = v[s]
                low = jnp.where(left_end, 0.0, pltpu.roll(pltpu.roll(x, 97, 1), 1, 0))
                high = jnp.where(right_end, 0.0, pltpu.roll(pltpu.roll(x, 31, 1), n_gc - 1, 0))
                beside_x = jnp.where(first, low, pltpu.roll(x, 1, 1))
                beside_x = beside_x + jnp.where(last, high, pltpu.roll(x, 127, 1))
                beside_x = beside_x + jnp.where(top, ups[s - 1] if s > 0 else zero, ups[s])
                beside_x = beside_x + jnp.where(bottom, downs[s + 1] if s < n_slab - 1 else zero, downs[s])
                new.append(x + W * (rhs[s] - (dg * x - cp * beside_x)) / dg)
            v = new
        e3 = total(sum(a * b for a, b in zip(rhs, v)))
        energy = e_rr - alpha * (2.0 * e_rq) + (alpha * alpha) * e_qq + 32.0 * e3
        o_energy[...] = energy
        pitch = n_gc + 16
        vs[...] = jnp.zeros(vs.shape, F32)
        for s in range(n_slab):
            at = (s + 1) * pitch + 8
            vs[at : at + n_gc, :] = v[s]
        v3 = jnp.zeros((8, 128), F32)
        lanes, rows8 = iota((1, 128), 1), iota((8, 128), 0)
        for k, i in ((-1, 3), (0, 0), (0, 1), (0, 2), (0, 3), (1, 0)):
            at = (slab + 1 + k) * pitch + 8 + gc
            mid, lo, hi = (vs[pl.ds(at + x, 1), :] for x in (0, -1, 1))
            line = pltpu.roll(mid, (8 - 32 * i) % 128, 1)
            line = jnp.where(lanes == 7, pltpu.roll(lo, (8 - 32 * i - 32) % 128, 1), line)
            line = jnp.where(lanes == 40, pltpu.roll(hi, (8 - 32 * i + 32) % 128, 1), line)
            line = jnp.where((lanes >= 7) & (lanes <= 40), line, 0.0)
            v3 = jnp.where(rows8 == 4 * k + i + 1, line, v3)
        for done in ins[:10]:
            done.wait()
        v_res[...] = r[...] - alpha * q[...]
        copy(v_res, o_res, outs)
        for ref in (uh, ul):
            ref[0:32, :] = jnp.zeros((32, EXT), BF16)
            ref[WIN - 32 : WIN, :] = jnp.zeros((32, EXT), BF16)
        near = iota((32, 128), 1) < 64
        for at, x in ((32, e_u), (192, e_d)):
            edge = x[32:64, :] - alpha * x[0:32, :]
            side = edge[:, COLS:]
            for first, part in ((128, edge[:, 0:COLS]), (0, jnp.where(near, 0.0, side)), (128 + COLS, jnp.where(near, side, 0.0))):
                hi, lo = split(part)
                uh[at : at + 32, first : first + part.shape[1]] = hi
                ul[at : at + 32, first : first + part.shape[1]] = lo
        uh[64:192, :], ul[64:192, :] = split(r1[...] - alpha * d2[...])
        yh[...], yl[...] = split(dot3((lh[...], ll[...]), (uh[...], ul[...])))
        for g in range(5):
            a, v, o = IN0[g], VARIANT[g], slice(256 * g, 256 * g + 256)
            kk[:, o] = dot3((yh[:, a : a + 512], yl[:, a : a + 512]), (gh[v], gl[v]))
        for done in ins[10:19]:
            done.wait()
        v_sol[...] = sol[...] + alpha * d[...]
        copy(v_sol, o_sol, outs)
        up_q, up_r = e_u[64:72, 0:128], e_u[64:72, 128:256]
        dn_q, dn_r = e_d[64:72, 0:128], e_d[64:72, 128:256]
        edge_u, edge_d = up_r - alpha * up_q, dn_r - alpha * dn_q
        own = f2[16:32, :] - alpha * f2[0:16, :]
        row = iota((16, 128), 0)
        own = jnp.where(row == 0, edge_u[6:7, :], jnp.where(row == 1, edge_u[7:8, :], own))
        own = jnp.where(row == 10, edge_d[0:1, :], jnp.where(row == 11, edge_d[1:2, :], own))
        own = jnp.where(row < 12, own, 0.0)
        f = [f0[48:96, :] - alpha * f0[0:48, :], f1[24:48, :] - alpha * f1[0:24, :], own]
        low = v3
        for level, cols in ((2, pc3), (1, pc2), (0, pc1)):
            dg, cp = diag[level], coupling[level]
            sm = W / dg
            n, m = f[level].shape[0], low.shape[0]
            double = hot((iota((n, m), 0) >> 1) == iota((n, m), 1))
            wide = dot2r(double, split(dot2(split(low), cols[...])))
            inside = level_mask(level, f[level].shape, slab, gc, n_slab, n_gc)
            x = jnp.where(inside, sm * f[level] + wide, 0.0)
            low = jnp.where(inside, x + sm * (f[level] - operator(x, dg, cp)), 0.0)
        four = hot((iota((ROWS, 48), 0) >> 2) + 8 == iota((ROWS, 48), 1))
        t = slice(128, 128 + COLS)
        spread = split(dot2r(four, split(low)))
        au = r1[:, t] - alpha * d2[:, t]
        smooth = c * (3.0 * v_res[...] - (3.0 * c) * au + (c * c) * (kk[:, t] + delta * au))
        pre = smooth + dot2(spread, pc0[...])
        v_pre[...] = pre
        copy(v_pre, o_pre, outs)
        v_dir[...] = pre + (energy / rho) * d[...]
        copy(v_dir, o_dir, outs)
        for done in outs:
            done.wait()

    return kernel


def call(kernel, specs, outs, out_specs, scratch, sems=0):
    where = {"s": pltpu.SMEM, "v": pltpu.VMEM, "h": pltpu.HBM}
    if INTERPRET:
        where["h"] = pl.ANY

    def out(x, shape, kind):
        if x == "h" and not INTERPRET:
            return pltpu.HBM(shape, kind)
        return jax.ShapeDtypeStruct(shape, kind)

    run = pl.pallas_call(
        kernel,
        out_shape=[out(x, s, t) for x, (s, t) in zip(out_specs, outs)],
        in_specs=[pl.BlockSpec(memory_space=where[x]) for x in specs],
        out_specs=[pl.BlockSpec(memory_space=where[x]) for x in out_specs],
        scratch_shapes=[pltpu.VMEM(s, t) for s, t in scratch] + ([pltpu.SemaphoreType.DMA((sems,))] if sems else []),
        compiler_params=pltpu.CompilerParams(vmem_limit_bytes=40 * 1024 * 1024),
        interpret=INTERPRET,
    )

    def apply(*args):
        if INTERPRET:
            return run(*args)
        return run(*(pltpu.with_memory_space_constraint(a, pltpu.HBM) if x == "h" else a for x, a in zip(specs, args)))

    return apply


def run_copies(sem, pairs):
    todo = []
    for k, (src, dst) in enumerate(pairs):
        todo.append(pltpu.make_async_copy(src, dst, sem.at[k]))
        todo[-1].start()
    for done in todo:
        done.wait()


def edges_kernel(d, r, row_u, row_d, col_l, col_r, sem):
    pairs = []
    for n, at, x in ((DR, 0, d), (RR, DR, r)):
        pairs.append((x.at[pl.ds(0, n), :], row_u.at[pl.ds(at, n), :]))
        pairs.append((x.at[pl.ds(ROWS - n, n), :], row_d.at[pl.ds(at, n), :]))
    for at, x in ((0, d), (128, r)):
        pairs.append((x.at[:, pl.ds(0, 128)], col_l.at[:, pl.ds(at, 128)]))
        pairs.append((x.at[:, pl.ds(COLS - 128, 128)], col_r.at[:, pl.ds(at, 128)]))
    run_copies(sem, pairs)


def corners_kernel(from_u, from_d, cor_l, cor_r):
    for lane, x in ((0, from_u), (128, from_d)):
        cor_l[:, lane : lane + 128] = x[:, 0:128]
        cor_r[:, lane : lane + 128] = x[:, COLS - 128 :]


def solution(mesh):
    n_grp, n_slab, n_col = mesh.shape["grp"], mesh.shape["slab"], mesh.shape["col"]
    n_gc = n_grp * n_col
    n_dev = n_slab * n_col

    def forward(n):
        return [(i, i + 1) for i in range(n - 1)]

    def backward(n):
        return [(i + 1, i) for i in range(n - 1)]

    def body(sol, r, d, row_taps, col_taps, damping, rho, diag, coupling):
        idx = jnp.stack([lax.axis_index("slab"), lax.axis_index(GC)]).astype(jnp.int32)
        row_u, row_d, col_l, col_r = call(
            edges_kernel, "hh", [((DR + RR, COLS), F32)] * 2 + [((ROWS, 256), F32)] * 2, "vvvv", [], 8
        )(d, r)
        from_u = lax.ppermute(row_d, "slab", forward(n_slab))
        from_d = lax.ppermute(row_u, "slab", backward(n_slab))
        from_l = lax.ppermute(col_r, GC, forward(n_gc))
        from_r = lax.ppermute(col_l, GC, backward(n_gc))
        par = (damping[None], rho[None], diag, coupling)
        mat_shapes = [((352, WIN), BF16)] * 2 + [((6, 512, 256), BF16)] * 2
        mat_shapes += [((EXT, 384), BF16), ((384, 256), BF16), ((256, 128), BF16), ((128, 128), BF16)]
        back_shapes = [((384, COLS), BF16), ((256, 384), BF16), ((128, 256), BF16), ((128, 128), BF16)]
        mats = call(
            matrices_kernel(n_slab, n_gc), "sss", mat_shapes + back_shapes, "h" * 12, mat_shapes + back_shapes, 12
        )(idx, row_taps, col_taps)
        lh, ll, gh, gl, rc0, rc1, rc2, rc3, pc0, pc1, pc2, pc3 = mats
        send_l, send_r = call(corners_kernel, "vv", [((DR + RR, 256), F32)] * 2, "vv", [])(from_u, from_d)
        cor_l = lax.ppermute(send_r, GC, forward(n_gc))
        cor_r = lax.ppermute(send_l, GC, backward(n_gc))
        results = [((ROWS, COLS), F32), ((ROWS, EXT), F32), ((ROWS, EXT), F32)]
        results += [((96, 384), F32), ((48, 256), F32), ((32, 128), F32)]
        q, d2, r1, f0, f1, f2, e_up, e_dn, pay = call(
            halo_kernel(n_slab, n_gc, n_grp),
            "s" * 5 + "hh" + "v" * 6 + "h" * 8,
            results + [((72, COLS + 128), F32)] * 2 + [((n_dev, 384), F32)],
            "h" * 6 + "vvv",
            [((ROWS, EXT), F32)] * 2
            + mat_shapes
            + results
            + [((WIN, EXT), BF16)] * 4
            + [((304, EXT), BF16)] * 2
            + [((128, EXT), BF16)] * 2
            + [((304, EXT), F32)],
            40,
        )(idx, *par, d, r, from_u, from_d, from_l, from_r, cor_l, cor_r, lh, ll, gh, gl, rc0, rc1, rc2, rc3)
        edge_u = lax.ppermute(e_dn, "slab", forward(n_slab))
        edge_d = lax.ppermute(e_up, "slab", backward(n_slab))
        got = lax.all_to_all(pay, ("slab", "col"), 0, 0, tiled=True)
        swap = lax.ppermute(got, "grp", [(i, (i + 1) % n_grp) for i in range(n_grp)])
        tile = ((ROWS, COLS), F32)
        n_sol, n_res, pre, n_dir, energy = call(
            final_kernel(n_slab, n_gc, n_grp),
            "s" * 5 + "vvvv" + "h" * 17,
            [tile] * 4 + [((1, 1), F32)],
            "hhhhv",
            [((ROWS, EXT), F32)] * 2
            + [((128, WIN), BF16)] * 2
            + [((3, 512, 256), BF16)] * 2
            + [tile] * 4
            + [((96, 384), F32), ((48, 256), F32), ((32, 128), F32)]
            + back_shapes
            + [((WIN, EXT), BF16)] * 2
            + [((ROWS, EXT), BF16)] * 2
            + [(((n_slab + 2) * (n_gc + 16), 128), F32), ((ROWS, EXT), F32)]
            + [tile] * 4,
            24,
        )(idx, *par, got, swap, edge_u, edge_d, d2, r1, lh, ll, gh, gl, q, r, d, sol, f0, f1, f2, pc0, pc1, pc2, pc3)
        return n_sol, n_res, pre, n_dir, energy[0, 0]

    tile, rep = P("slab", GC), P()
    return jax.shard_map(
        body,
        mesh=mesh,
        in_specs=(tile,) * 3 + (rep,) * 6,
        out_specs=(tile,) * 4 + (rep,),
        check_vma=False,
    )
```

```python
import jax
import jax.numpy as jnp
from jax import lax
from jax.experimental import pallas as pl
from jax.experimental.pallas import tpu as pltpu
from jax.sharding import PartitionSpec as P


INTERPRET = False
W = 2.0 / 3.0
TAPS = 31
H = TAPS // 2
ROWS, COLS = 128, 1024
EXT = COLS + 256
WIN = ROWS + 128
DR, RR = 64, 32
IN0 = (0, 128, 384, 640, 768)
VARIANT = (0, 1, 1, 1, 2)
GC = ("grp", "col")
F32, BF16 = jnp.float32, jnp.bfloat16


def iota(shape, dim):
    return lax.broadcasted_iota(jnp.int32, shape, dim)


def split(x):
    high = x.astype(BF16)
    return high, (x - high.astype(F32)).astype(BF16)


def dot(a, b):
    return jnp.dot(a, b, preferred_element_type=F32)


def dot3(a, b):
    (ah, al), (bh, bl) = a, b
    return dot(ah, bh) + (dot(ah, bl) + dot(al, bh))


def dot2(a, b):
    return dot(a[0], b) + dot(a[1], b)


def dot2r(a, b):
    return dot(a, b[0]) + dot(a, b[1])


def hot(cond):
    return jnp.where(cond, 1.0, 0.0).astype(BF16)


def total(x):
    return jnp.sum(jnp.sum(x, axis=0, keepdims=True), axis=1, keepdims=True)


def dot_t(a, b):
    def nt(x, y):
        return lax.dot_general(x, y, (((1,), (1,)), ((), ())), preferred_element_type=F32)

    (ah, al), (bh, bl) = a, b
    return nt(ah, bh) + (nt(ah, bl) + nt(al, bh))


def toeplitz(taps):
    sum_taps = taps[0]
    for t in range(1, TAPS):
        sum_taps = sum_taps + taps[t]
    lane = iota((8, 384), 1)
    base = jnp.zeros((8, 384), F32)
    for t in range(TAPS):
        base = jnp.where(lane == 64 + H - t, taps[t], base)
    base = base / jnp.full((8, 384), sum_taps, F32)
    return pltpu.roll(jnp.broadcast_to(base[0:1], (256, 384)), 0, 1, stride=1, stride_axis=0)


def gram(kt, first, limit):
    ks = split(kt)
    left = ks
    if first is not None:
        m = iota((256, 384), 1) + (first - 128)
        left = split(jnp.where((m >= 0) & (m < limit), kt, 0.0))
    return left, ks


def block_powers(kt, first, limit):
    left, ks = gram(kt, first, limit)
    wide = dot_t(left, ks)
    g1 = dot_t(left, (ks[0][64:192], ks[1][64:192]))
    if first is not None:
        i = iota((256, 128), 0) + (first - 64)
        g1 = jnp.where((i >= 0) & (i < limit), g1, 0.0)
    g1s = split(g1)
    return g1s, split(dot3(split(wide), g1s))


def matrices_kernel(n_slab, n_gc):
    def kernel(idx, rt, ct, *refs):
        outs, scratch, sem = refs[:12], refs[12:24], refs[24]
        lh, ll, gh, gl, rc0, rc1, rc2, rc3, pc0, pc1, pc2, pc3 = scratch
        slab, gc = idx[0], idx[1]
        gh[...], gl[...] = jnp.zeros(gh.shape, BF16), jnp.zeros(gl.shape, BF16)
        kt = toeplitz(ct)
        inner = block_powers(kt, None, None)
        low = block_powers(kt, gc * COLS, n_gc * COLS)
        high = block_powers(kt, gc * COLS + COLS - 128, n_gc * COLS)
        has_l = jnp.where(gc > 0, 1.0, 0.0).astype(F32)
        has_r = jnp.where(gc < n_gc - 1, 1.0, 0.0).astype(F32)
        for power in range(2):
            for at, ref in enumerate((gh, gl)):
                mid = inner[power][at]
                wide = mid.astype(F32)
                outer_l, outer_r = (wide * has_l).astype(BF16), (wide * has_r).astype(BF16)
                for v, off, blocks in (
                    (0, 0, (outer_l, low[power][at])),
                    (1, 128, (mid, mid)),
                    (2, 256, (high[power][at], outer_r)),
                ):
                    for b in range(2):
                        start = off + 128 * b - 64
                        lo, hi = max(0, start), min(512, start + 256)
                        ref[3 * power + v, lo:hi, 128 * b : 128 * b + 128] = blocks[b][lo - start : hi - start]
        first, limit = slab * ROWS, n_slab * ROWS
        left, ks = gram(toeplitz(rt), first, limit)
        g1 = dot_t(left, ks)
        g1s = split(g1)
        lh[0:128, :], ll[0:128, :] = g1s[0][64:192, :], g1s[1][64:192, :]
        c, i = iota((48, WIN), 0), iota((48, WIN), 1)
        inside = (i + (first - 64) >= 0) & (i + (first - 64) < limit)
        rr = jnp.where((i - 32 >= 4 * c) & (i - 32 < 4 * c + 4) & inside, 0.25, 0.0).astype(BF16)
        lh[128:176, :], ll[128:176, :] = split(dot2r(rr, g1s))
        lh[176:224, :], ll[176:224, :] = rr, jnp.zeros_like(rr)
        k = iota((128, WIN), 1) + (first - 64)
        tile = split(jnp.where((k >= 0) & (k < limit), g1[64:192, :], 0.0))
        lh[224:352, :], ll[224:352, :] = split(dot3(tile, g1s))
        rc0[...] = hot((iota((EXT, 384), 0) >> 2) + 32 == iota((EXT, 384), 1))
        rc1[...] = hot((iota((384, 256), 0) >> 1) == iota((384, 256), 1))
        rc2[...] = hot((iota((256, 128), 0) >> 1) == iota((256, 128), 1))
        rc3[...] = hot((iota((128, 128), 0) >> 1) - 8 == (iota((128, 128), 1) & 31))
        pc0[...] = hot(iota((384, COLS), 0) == (iota((384, COLS), 1) >> 2) + 64)
        pc1[...] = hot(iota((256, 384), 0) == (iota((256, 384), 1) >> 1))
        pc2[...] = hot(iota((128, 256), 0) == (iota((128, 256), 1) >> 1))
        pc3[...] = hot(iota((128, 128), 0) == (iota((128, 128), 1) >> 1))
        run_copies(sem, list(zip(scratch, outs)))

    return kernel


def level_mask(level, shape, slab, gc, n_slab, n_gc):
    height, width = 32 >> level, 256 >> level
    i = iota(shape, 0) - (8 >> level) + slab * height
    j = iota(shape, 1) - (64 >> level) + gc * width
    return (i >= 0) & (i < n_slab * height) & (j >= 0) & (j < n_gc * width)


def tile_mask(level, shape):
    i, j = iota(shape, 0) - (8 >> level), iota(shape, 1) - (64 >> level)
    return (i >= 0) & (i < 32 >> level) & (j >= 0) & (j < 256 >> level)


def beside(v):
    n, m = v.shape
    rows = pltpu.roll(v, 1, 0) + pltpu.roll(v, n - 1, 0)
    return rows + pltpu.roll(v, 1, 1) + pltpu.roll(v, m - 1, 1)


def operator(v, dg, cp):
    return dg * v - cp * beside(v)


def halo_kernel(n_slab, n_gc, n_grp):
    n_dev = n_slab * n_gc // n_grp

    def kernel(idx, damping, rho_in, diag, coupling, d_in, r_in, row_u, row_d, col_l, col_r, cor_l, cor_r,
               lh_in, ll_in, gh_in, gl_in, rc0_in, rc1_in, rc2_in, rc3_in,
               q_out, d2_out, r1_out, f0_out, f1_out, f2_out, e_up, e_dn, pay,
               d, r, lh, ll, gh, gl, rc0, rc1, rc2, rc3, q, d2, r1, f0, f1, f2,
               dh, dl, rh, rl, sh, sl, th, tl, c1, sem):
        slab, gc = idx[0], idx[1]
        delta = damping[0]
        c = W / (1.0 + delta)
        ins, outs = [], []

        def copy(src, dst, todo):
            done = pltpu.make_async_copy(src, dst, sem.at[len(ins) + len(outs)])
            done.start()
            todo.append(done)

        for ref, main in ((d, d_in), (r, r_in)):
            copy(main, ref.at[:, pl.ds(128, COLS)], ins)
        for src, dst in ((lh_in, lh), (ll_in, ll), (gh_in, gh), (gl_in, gl), (rc0_in, rc0), (rc1_in, rc1), (rc2_in, rc2), (rc3_in, rc3)):
            copy(src, dst, ins)

        def put(hi_ref, lo_ref, r0, c0, x):
            hi, lo = split(x)
            hi_ref[r0 : r0 + x.shape[0], c0 : c0 + x.shape[1]] = hi
            lo_ref[r0 : r0 + x.shape[0], c0 : c0 + x.shape[1]] = lo

        zero = jnp.zeros((32, EXT), BF16)
        for ref in (rh, rl):
            ref[0:32, :] = zero
            ref[WIN - 32 : WIN, :] = zero
        for at, n, ref, hi, lo in ((0, DR, d, dh, dl), (1, RR, r, rh, rl)):
            cols = slice(128 * at, 128 * at + 128)
            rows = slice(DR * at, DR * at + n)
            ref[:, 0:128] = col_l[:, cols]
            ref[:, 128 + COLS :] = col_r[:, cols]
            for first, lane, main in ((64 - n, 0, row_u), (192, 128, row_d)):
                put(hi, lo, first, 128, main[rows, :])
                put(hi, lo, first, 0, cor_l[rows, lane : lane + 128])
                put(hi, lo, first, 128 + COLS, cor_r[rows, lane : lane + 128])
            ins[at].wait()
            put(hi, lo, 64, 0, ref[...])
        for done in ins[2:4]:
            done.wait()
        ds, rs = (dh[...], dl[...]), (rh[...], rl[...])

        def left(a, b):
            return (lh[a:b, :], ll[a:b, :])

        put(sh, sl, 0, 0, dot3(left(0, 176), ds))
        put(sh, sl, 176, 0, dot3(left(0, 128), rs))
        put(th, tl, 0, 0, dot3(left(224, 352), ds))
        rd = dot2r(lh[176:224, :], ds)
        rres = dot2r(lh[176:224, :], rs)
        for done in ins[4:]:
            done.wait()
        for g in range(5):
            a, v, o = IN0[g], VARIANT[g], slice(256 * g, 256 * g + 256)
            c1[:, o] = dot3((sh[:, a : a + 512], sl[:, a : a + 512]), (gh[v], gl[v]))
        sums_of = []

        def coarse():
            fq = c1[128:176, :] + delta * rd
            f = dot2(split(jnp.concatenate([fq, rres], axis=0)), rc0[...])
            f0[...] = f
            yield None
            pair = (f[0:48], f[48:96])
            weight = 4.0
            for level, cols in ((0, rc1), (1, rc2), (2, rc3)):
                dg, cp = diag[level], coupling[level]
                sm = W / dg
                shape = pair[0].shape
                inside = level_mask(level, shape, slab, gc, n_slab, n_gc)
                mine = tile_mask(level, shape)
                bq, br = operator(pair[0], dg, cp), operator(pair[1], dg, cp)
                rest_q = jnp.where(inside, pair[0] - sm * bq, 0.0)
                rest_r = jnp.where(inside, pair[1] - sm * br, 0.0)
                low = dot2(split(jnp.concatenate([rest_q, rest_r], axis=0)), cols[...])
                own_q, own_r = jnp.where(mine, pair[0], 0.0), jnp.where(mine, pair[1], 0.0)
                sums_of.append(
                    (
                        weight * total(own_r * (2.0 * sm * pair[1] - (sm * sm) * br)),
                        weight * total(own_q * (2.0 * sm * pair[0] - (sm * sm) * bq)),
                        weight * total(own_r * (2.0 * sm * pair[0] - (sm * sm) * bq)),
                    )
                )
                weight = 2.0 * weight
                if level < 2:
                    yield None
                    n, m = (24, 48) if level == 0 else (16, 24)
                    half = jnp.where((iota((n, m), 1) >> 1) == iota((n, m), 0), 0.5, 0.0).astype(BF16)
                    pair = (dot2r(half, split(low[0:m])), dot2r(half, split(low[m : 2 * m])))
                    keep = level_mask(level + 1, pair[0].shape, slab, gc, n_slab, n_gc)
                    pair = (jnp.where(keep, pair[0], 0.0), jnp.where(keep, pair[1], 0.0))
                    out = (f1, f2)[level]
                    out[0:n, :], out[n : 2 * n, :] = pair
                    yield None
            yield pair, low

        steps = coarse()
        last = next(steps)
        for g in range(5):
            a, v, o = IN0[g], VARIANT[g], slice(256 * g, 256 * g + 256)
            d2[:, o] = dot3((th[:, a : a + 512], tl[:, a : a + 512]), (gh[3 + v], gl[3 + v]))
            last = next(steps)
        pair, low = last
        t = slice(128, 128 + COLS)
        p1 = c1[0:128, :]
        q[...] = c1[0:128, t] + delta * d[:, t]
        d2[...] = d2[...] + delta * (2.0 * p1 + delta * d[...])
        r1[...] = c1[176:304, :] + delta * r[...]
        copy(q, q_out, outs)
        copy(d2, d2_out, outs)
        copy(r1, r1_out, outs)
        near = iota((32, 128), 1) < 64
        for ref, rows in ((e_dn, slice(96, 128)), (e_up, slice(0, 32))):
            for at, x in ((0, d2), (32, r1)):
                ref[at : at + 32, 0:COLS] = x[rows, t]
                ref[at : at + 32, COLS:] = jnp.where(near, x[rows, 128 + COLS :], x[rows, 0:128])
        qv, rv, aq, ar = q[...], r[:, t], d2[:, t], r1[:, t]
        s_dq = total(d[:, t] * qv)
        e_rr = total(rv * (3.0 * rv - 3.0 * c * ar) + c * c * (ar * ar)) * c
        e_qq = total(qv * (3.0 * qv - 3.0 * c * aq) + c * c * (aq * aq)) * c
        e_rq = total(rv * (3.0 * qv - 3.0 * c * aq) + c * c * (ar * aq)) * c
        for x, y, z in sums_of:
            e_rr, e_qq, e_rq = e_rr + x, e_qq + y, e_rq + z
        for ref in (e_up, e_dn):
            ref[64:72, 0:128], ref[64:72, 128:256] = pair[0][2:10, :], pair[1][2:10, :]
            ref[64:72, 256:] = jnp.zeros((8, COLS - 128), F32)
        for src, dst in ((f0, f0_out), (f1, f1_out), (f2, f2_out)):
            copy(src, dst, outs)
        i, lane = iota((16, 128), 0), iota((16, 128), 1)
        pick = (i >= 2) & (i < 10) & (((i - 2) >> 1) == (lane >> 5))
        gq = jnp.sum(jnp.where(pick, low[0:16], 0.0), axis=0, keepdims=True) * 0.5
        gr = jnp.sum(jnp.where(pick, low[16:32], 0.0), axis=0, keepdims=True) * 0.5
        lane = iota((1, 128), 1)
        sums = jnp.zeros((1, 128), F32)
        for k, x in enumerate((s_dq, e_rr, e_rq, e_qq)):
            sums = jnp.where(lane == k, x, sums)
        pay[:, 0:128] = jnp.broadcast_to(gq, (n_dev, 128))
        pay[:, 128:256] = jnp.broadcast_to(gr, (n_dev, 128))
        pay[:, 256:384] = jnp.broadcast_to(sums, (n_dev, 128))
        for done in outs:
            done.wait()

    return kernel


def final_kernel(n_slab, n_gc, n_grp):
    n_col = n_gc // n_grp

    def kernel(idx, damping, rho_in, diag, coupling, got, swap, e_u, e_d, d2_in, r1_in, lh_in, ll_in, gh_in, gl_in, q_in, r_in, d_in, sol_in,
               f0_in, f1_in, f2_in, pc0_in, pc1_in, pc2_in, pc3_in,
               o_sol, o_res, o_pre, o_dir, o_energy,
               d2, r1, lh, ll, gh, gl, q, r, d, sol, f0, f1, f2, pc0, pc1, pc2, pc3,
               uh, ul, yh, yl, vs, kk, v_sol, v_res, v_pre, v_dir, sem):
        ins, outs = [], []

        def copy(src, dst, todo):
            done = pltpu.make_async_copy(src, dst, sem.at[len(ins) + len(outs)])
            done.start()
            todo.append(done)

        for src, dst in (
            (d2_in, d2), (r1_in, r1), (lh_in.at[pl.ds(0, 128), :], lh), (ll_in.at[pl.ds(0, 128), :], ll),
            (gh_in.at[pl.ds(0, 3)], gh), (gl_in.at[pl.ds(0, 3)], gl), (r_in, r), (q_in, q), (sol_in, sol), (d_in, d),
            (f0_in, f0), (f1_in, f1), (f2_in, f2), (pc1_in, pc1), (pc2_in, pc2), (pc3_in, pc3), (pc0_in, pc0),
        ):
            copy(src, dst, ins)
        slab, gc = idx[0], idx[1]
        delta, rho = damping[0], rho_in[0]
        c = W / (1.0 + delta)
        lane = iota((1, 128), 1)
        sums = jnp.sum(got[:, 256:384] + swap[:, 256:384], axis=0, keepdims=True)
        s_dq, e_rr, e_rq, e_qq = (
            jnp.sum(jnp.where(lane == k, sums, 0.0), axis=1, keepdims=True) for k in range(4)
        )
        alpha = rho / s_dq
        dg, cp = diag[3], coupling[3]
        first = (iota((n_gc, 128), 1) & 31) == 0
        last = (iota((n_gc, 128), 1) & 31) == 31
        top, bottom = iota((n_gc, 128), 1) < 32, iota((n_gc, 128), 1) >= 96
        left_end, right_end = iota((n_gc, 128), 0) == 0, iota((n_gc, 128), 0) == n_gc - 1
        mine = gc < n_col
        rhs = []
        for s in range(n_slab):
            at = s * n_col
            a, b = (x[at : at + n_col, 128:256] - alpha * x[at : at + n_col, 0:128] for x in (got, swap))
            rhs.append(jnp.concatenate([jnp.where(mine, a, b), jnp.where(mine, b, a)], axis=0))
        zero = jnp.zeros((n_gc, 128), F32)
        v = [W * x / dg for x in rhs]
        for _ in range(3):
            ups = [pltpu.roll(x, 32, 1) for x in v]
            downs = [pltpu.roll(x, 96, 1) for x in v]
            new = []
            for s in range(n_slab):
                x = v[s]
                low = jnp.where(left_end, 0.0, pltpu.roll(pltpu.roll(x, 97, 1), 1, 0))
                high = jnp.where(right_end, 0.0, pltpu.roll(pltpu.roll(x, 31, 1), n_gc - 1, 0))
                beside_x = jnp.where(first, low, pltpu.roll(x, 1, 1))
                beside_x = beside_x + jnp.where(last, high, pltpu.roll(x, 127, 1))
                beside_x = beside_x + jnp.where(top, ups[s - 1] if s > 0 else zero, ups[s])
                beside_x = beside_x + jnp.where(bottom, downs[s + 1] if s < n_slab - 1 else zero, downs[s])
                new.append(x + W * (rhs[s] - (dg * x - cp * beside_x)) / dg)
            v = new
        e3 = total(sum(a * b for a, b in zip(rhs, v)))
        energy = e_rr - alpha * (2.0 * e_rq) + (alpha * alpha) * e_qq + 32.0 * e3
        o_energy[...] = energy
        pitch = n_gc + 16
        vs[...] = jnp.zeros(vs.shape, F32)
        for s in range(n_slab):
            at = (s + 1) * pitch + 8
            vs[at : at + n_gc, :] = v[s]
        v3 = jnp.zeros((8, 128), F32)
        lanes, rows8 = iota((1, 128), 1), iota((8, 128), 0)
        for k, i in ((-1, 3), (0, 0), (0, 1), (0, 2), (0, 3), (1, 0)):
            at = (slab + 1 + k) * pitch + 8 + gc
            mid, lo, hi = (vs[pl.ds(at + x, 1), :] for x in (0, -1, 1))
            line = pltpu.roll(mid, (8 - 32 * i) % 128, 1)
            line = jnp.where(lanes == 7, pltpu.roll(lo, (8 - 32 * i - 32) % 128, 1), line)
            line = jnp.where(lanes == 40, pltpu.roll(hi, (8 - 32 * i + 32) % 128, 1), line)
            line = jnp.where((lanes >= 7) & (lanes <= 40), line, 0.0)
            v3 = jnp.where(rows8 == 4 * k + i + 1, line, v3)
        for ref in (uh, ul):
            ref[0:32, :] = jnp.zeros((32, EXT), BF16)
            ref[WIN - 32 : WIN, :] = jnp.zeros((32, EXT), BF16)
        for done in ins[:4]:
            done.wait()
        near = iota((32, 128), 1) < 64
        for at, x in ((32, e_u), (192, e_d)):
            edge = x[32:64, :] - alpha * x[0:32, :]
            side = edge[:, COLS:]
            for first, part in ((128, edge[:, 0:COLS]), (0, jnp.where(near, 0.0, side)), (128 + COLS, jnp.where(near, side, 0.0))):
                hi, lo = split(part)
                uh[at : at + 32, first : first + part.shape[1]] = hi
                ul[at : at + 32, first : first + part.shape[1]] = lo
        uh[64:192, :], ul[64:192, :] = split(r1[...] - alpha * d2[...])
        yh[...], yl[...] = split(dot3((lh[...], ll[...]), (uh[...], ul[...])))
        for done in ins[4:19]:
            done.wait()
        v_res[...] = r[...] - alpha * q[...]
        copy(v_res, o_res, outs)
        v_sol[...] = sol[...] + alpha * d[...]
        copy(v_sol, o_sol, outs)
        up_q, up_r = e_u[64:72, 0:128], e_u[64:72, 128:256]
        dn_q, dn_r = e_d[64:72, 0:128], e_d[64:72, 128:256]
        edge_u, edge_d = up_r - alpha * up_q, dn_r - alpha * dn_q
        own = f2[16:32, :] - alpha * f2[0:16, :]
        row = iota((16, 128), 0)
        own = jnp.where(row == 0, edge_u[6:7, :], jnp.where(row == 1, edge_u[7:8, :], own))
        own = jnp.where(row == 10, edge_d[0:1, :], jnp.where(row == 11, edge_d[1:2, :], own))
        own = jnp.where(row < 12, own, 0.0)
        f = [f0[48:96, :] - alpha * f0[0:48, :], f1[24:48, :] - alpha * f1[0:24, :], own]

        def upwards():
            low = v3
            for level, cols in ((2, pc3), (1, pc2), (0, pc1)):
                dg, cp = diag[level], coupling[level]
                sm = W / dg
                n, m = f[level].shape[0], low.shape[0]
                double = hot((iota((n, m), 0) >> 1) == iota((n, m), 1))
                wide = dot2r(double, split(dot2(split(low), cols[...])))
                inside = level_mask(level, f[level].shape, slab, gc, n_slab, n_gc)
                x = jnp.where(inside, sm * f[level] + wide, 0.0)
                low = jnp.where(inside, x + sm * (f[level] - operator(x, dg, cp)), 0.0)
                if level > 0:
                    yield None
            four = hot((iota((ROWS, 48), 0) >> 2) + 8 == iota((ROWS, 48), 1))
            yield split(dot2r(four, split(low)))

        steps = upwards()
        for g in range(5):
            a, v, o = IN0[g], VARIANT[g], slice(256 * g, 256 * g + 256)
            kk[:, o] = dot3((yh[:, a : a + 512], yl[:, a : a + 512]), (gh[v], gl[v]))
            if g in (0, 2, 4):
                spread = next(steps)
        t = slice(128, 128 + COLS)
        au = r1[:, t] - alpha * d2[:, t]
        smooth = c * (3.0 * v_res[...] - (3.0 * c) * au + (c * c) * (kk[:, t] + delta * au))
        pre = smooth + dot2(spread, pc0[...])
        v_pre[...] = pre
        copy(v_pre, o_pre, outs)
        v_dir[...] = pre + (energy / rho) * d[...]
        copy(v_dir, o_dir, outs)
        for done in outs:
            done.wait()

    return kernel


def call(kernel, specs, outs, out_specs, scratch, sems=0):
    where = {"s": pltpu.SMEM, "v": pltpu.VMEM, "h": pltpu.HBM}
    if INTERPRET:
        where["h"] = pl.ANY

    def out(x, shape, kind):
        if x == "h" and not INTERPRET:
            return pltpu.HBM(shape, kind)
        return jax.ShapeDtypeStruct(shape, kind)

    run = pl.pallas_call(
        kernel,
        out_shape=[out(x, s, t) for x, (s, t) in zip(out_specs, outs)],
        in_specs=[pl.BlockSpec(memory_space=where[x]) for x in specs],
        out_specs=[pl.BlockSpec(memory_space=where[x]) for x in out_specs],
        scratch_shapes=[pltpu.VMEM(s, t) for s, t in scratch] + ([pltpu.SemaphoreType.DMA((sems,))] if sems else []),
        compiler_params=pltpu.CompilerParams(vmem_limit_bytes=40 * 1024 * 1024),
        interpret=INTERPRET,
    )

    def apply(*args):
        if INTERPRET:
            return run(*args)
        return run(*(pltpu.with_memory_space_constraint(a, pltpu.HBM) if x == "h" else a for x, a in zip(specs, args)))

    return apply


def run_copies(sem, pairs):
    todo = []
    for k, (src, dst) in enumerate(pairs):
        todo.append(pltpu.make_async_copy(src, dst, sem.at[k]))
        todo[-1].start()
    for done in todo:
        done.wait()


def edges_kernel(d, r, row_u, row_d, col_l, col_r, sem):
    pairs = []
    for n, at, x in ((DR, 0, d), (RR, DR, r)):
        pairs.append((x.at[pl.ds(0, n), :], row_u.at[pl.ds(at, n), :]))
        pairs.append((x.at[pl.ds(ROWS - n, n), :], row_d.at[pl.ds(at, n), :]))
    for at, x in ((0, d), (128, r)):
        pairs.append((x.at[:, pl.ds(0, 128)], col_l.at[:, pl.ds(at, 128)]))
        pairs.append((x.at[:, pl.ds(COLS - 128, 128)], col_r.at[:, pl.ds(at, 128)]))
    run_copies(sem, pairs)


def corners_kernel(from_u, from_d, cor_l, cor_r):
    for lane, x in ((0, from_u), (128, from_d)):
        cor_l[:, lane : lane + 128] = x[:, 0:128]
        cor_r[:, lane : lane + 128] = x[:, COLS - 128 :]


def solution(mesh):
    n_grp, n_slab, n_col = mesh.shape["grp"], mesh.shape["slab"], mesh.shape["col"]
    n_gc = n_grp * n_col
    n_dev = n_slab * n_col

    def forward(n):
        return [(i, i + 1) for i in range(n - 1)]

    def backward(n):
        return [(i + 1, i) for i in range(n - 1)]

    def body(sol, r, d, row_taps, col_taps, damping, rho, diag, coupling):
        idx = jnp.stack([lax.axis_index("slab"), lax.axis_index(GC)]).astype(jnp.int32)
        row_u, row_d, col_l, col_r = call(
            edges_kernel, "hh", [((DR + RR, COLS), F32)] * 2 + [((ROWS, 256), F32)] * 2, "vvvv", [], 8
        )(d, r)
        from_u = lax.ppermute(row_d, "slab", forward(n_slab))
        from_d = lax.ppermute(row_u, "slab", backward(n_slab))
        from_l = lax.ppermute(col_r, GC, forward(n_gc))
        from_r = lax.ppermute(col_l, GC, backward(n_gc))
        par = (damping[None], rho[None], diag, coupling)
        mat_shapes = [((352, WIN), BF16)] * 2 + [((6, 512, 256), BF16)] * 2
        mat_shapes += [((EXT, 384), BF16), ((384, 256), BF16), ((256, 128), BF16), ((128, 128), BF16)]
        back_shapes = [((384, COLS), BF16), ((256, 384), BF16), ((128, 256), BF16), ((128, 128), BF16)]
        mats = call(
            matrices_kernel(n_slab, n_gc), "sss", mat_shapes + back_shapes, "h" * 12, mat_shapes + back_shapes, 12
        )(idx, row_taps, col_taps)
        lh, ll, gh, gl, rc0, rc1, rc2, rc3, pc0, pc1, pc2, pc3 = mats
        send_l, send_r = call(corners_kernel, "vv", [((DR + RR, 256), F32)] * 2, "vv", [])(from_u, from_d)
        cor_l = lax.ppermute(send_r, GC, forward(n_gc))
        cor_r = lax.ppermute(send_l, GC, backward(n_gc))
        results = [((ROWS, COLS), F32), ((ROWS, EXT), F32), ((ROWS, EXT), F32)]
        results += [((96, 384), F32), ((48, 256), F32), ((32, 128), F32)]
        q, d2, r1, f0, f1, f2, e_up, e_dn, pay = call(
            halo_kernel(n_slab, n_gc, n_grp),
            "s" * 5 + "hh" + "v" * 6 + "h" * 8,
            results + [((72, COLS + 128), F32)] * 2 + [((n_dev, 384), F32)],
            "h" * 6 + "vvv",
            [((ROWS, EXT), F32)] * 2
            + mat_shapes
            + results
            + [((WIN, EXT), BF16)] * 4
            + [((304, EXT), BF16)] * 2
            + [((128, EXT), BF16)] * 2
            + [((304, EXT), F32)],
            40,
        )(idx, *par, d, r, from_u, from_d, from_l, from_r, cor_l, cor_r, lh, ll, gh, gl, rc0, rc1, rc2, rc3)
        edge_u = lax.ppermute(e_dn, "slab", forward(n_slab))
        edge_d = lax.ppermute(e_up, "slab", backward(n_slab))
        got = lax.all_to_all(pay, ("slab", "col"), 0, 0, tiled=True)
        swap = lax.ppermute(got, "grp", [(i, (i + 1) % n_grp) for i in range(n_grp)])
        tile = ((ROWS, COLS), F32)
        n_sol, n_res, pre, n_dir, energy = call(
            final_kernel(n_slab, n_gc, n_grp),
            "s" * 5 + "vvvv" + "h" * 17,
            [tile] * 4 + [((1, 1), F32)],
            "hhhhv",
            [((ROWS, EXT), F32)] * 2
            + [((128, WIN), BF16)] * 2
            + [((3, 512, 256), BF16)] * 2
            + [tile] * 4
            + [((96, 384), F32), ((48, 256), F32), ((32, 128), F32)]
            + back_shapes
            + [((WIN, EXT), BF16)] * 2
            + [((ROWS, EXT), BF16)] * 2
            + [(((n_slab + 2) * (n_gc + 16), 128), F32), ((ROWS, EXT), F32)]
            + [tile] * 4,
            24,
        )(idx, *par, got, swap, edge_u, edge_d, d2, r1, lh, ll, gh, gl, q, r, d, sol, f0, f1, f2, pc0, pc1, pc2, pc3)
        return n_sol, n_res, pre, n_dir, energy[0, 0]

    tile, rep = P("slab", GC), P()
    return jax.shard_map(
        body,
        mesh=mesh,
        in_specs=(tile,) * 3 + (rep,) * 6,
        out_specs=(tile,) * 4 + (rep,),
        check_vma=False,
    )
```

```python
import jax
import jax.numpy as jnp
from jax import lax
from jax.experimental import pallas as pl
from jax.experimental.pallas import tpu as pltpu
from jax.sharding import PartitionSpec as P


INTERPRET = False
W = 2.0 / 3.0
TAPS = 31
H = TAPS // 2
ROWS, COLS = 128, 1024
EXT = COLS + 256
WIN = ROWS + 128
DR, RR = 64, 32
IN0 = (0, 128, 384, 640, 768)
VARIANT = (0, 1, 1, 1, 2)
GC = ("grp", "col")
F32, BF16 = jnp.float32, jnp.bfloat16


def iota(shape, dim):
    return lax.broadcasted_iota(jnp.int32, shape, dim)


def split(x):
    high = x.astype(BF16)
    return high, (x - high.astype(F32)).astype(BF16)


def dot(a, b):
    return jnp.dot(a, b, preferred_element_type=F32)


def dot3(a, b):
    (ah, al), (bh, bl) = a, b
    return dot(ah, bh) + (dot(ah, bl) + dot(al, bh))


def dot2(a, b):
    return dot(a[0], b) + dot(a[1], b)


def dot2r(a, b):
    return dot(a, b[0]) + dot(a, b[1])


def hot(cond):
    return jnp.where(cond, 1.0, 0.0).astype(BF16)


def total(x):
    return jnp.sum(jnp.sum(x, axis=0, keepdims=True), axis=1, keepdims=True)


def dot_t(a, b):
    def nt(x, y):
        return lax.dot_general(x, y, (((1,), (1,)), ((), ())), preferred_element_type=F32)

    (ah, al), (bh, bl) = a, b
    return nt(ah, bh) + (nt(ah, bl) + nt(al, bh))


def toeplitz(taps):
    sum_taps = taps[0]
    for t in range(1, TAPS):
        sum_taps = sum_taps + taps[t]
    lane = iota((8, 384), 1)
    base = jnp.zeros((8, 384), F32)
    for t in range(TAPS):
        base = jnp.where(lane == 64 + H - t, taps[t], base)
    base = base / jnp.full((8, 384), sum_taps, F32)
    return pltpu.roll(jnp.broadcast_to(base[0:1], (256, 384)), 0, 1, stride=1, stride_axis=0)


def gram(kt, first, limit):
    ks = split(kt)
    left = ks
    if first is not None:
        m = iota((256, 384), 1) + (first - 128)
        left = split(jnp.where((m >= 0) & (m < limit), kt, 0.0))
    return left, ks


def block_powers(kt, first, limit):
    left, ks = gram(kt, first, limit)
    wide = dot_t(left, ks)
    g1 = dot_t(left, (ks[0][64:192], ks[1][64:192]))
    if first is not None:
        i = iota((256, 128), 0) + (first - 64)
        g1 = jnp.where((i >= 0) & (i < limit), g1, 0.0)
    g1s = split(g1)
    return g1s, split(dot3(split(wide), g1s))


def matrices_kernel(n_slab, n_gc):
    def kernel(idx, rt_in, ct_in, *refs):
        outs, scratch, sem, rt, ct = refs[:12], refs[12:24], refs[24], refs[25], refs[26]
        todo = []

        def copy(src, dst):
            todo.append(pltpu.make_async_copy(src, dst, sem.at[len(todo)]))
            todo[-1].start()

        copy(ct_in, ct)
        copy(rt_in, rt)
        lh, ll, gh, gl, rc0, rc1, rc2, rc3, pc0, pc1, pc2, pc3 = scratch
        slab, gc = idx[0], idx[1]
        gh[...], gl[...] = jnp.zeros(gh.shape, BF16), jnp.zeros(gl.shape, BF16)
        todo[0].wait()
        kt = toeplitz(ct)
        inner = block_powers(kt, None, None)
        end = block_powers(kt, jnp.where(gc == 0, 0, gc * COLS + COLS - 128), n_gc * COLS)
        at_l, at_r = gc == 0, gc == n_gc - 1
        has_l = jnp.where(gc > 0, 1.0, 0.0).astype(F32)
        has_r = jnp.where(gc < n_gc - 1, 1.0, 0.0).astype(F32)
        for power in range(2):
            for at, ref in enumerate((gh, gl)):
                mid = inner[power][at]
                wide, other = mid.astype(F32), end[power][at].astype(F32)
                low = jnp.where(at_l, other, wide).astype(BF16)
                high = jnp.where(at_r, other, wide).astype(BF16)
                outer_l, outer_r = (wide * has_l).astype(BF16), (wide * has_r).astype(BF16)
                for v, off, blocks in (
                    (0, 0, (outer_l, low)),
                    (1, 128, (mid, mid)),
                    (2, 256, (high, outer_r)),
                ):
                    for b in range(2):
                        start = off + 128 * b - 64
                        lo, hi = max(0, start), min(512, start + 256)
                        ref[3 * power + v, lo:hi, 128 * b : 128 * b + 128] = blocks[b][lo - start : hi - start]
        for k in (2, 3):
            copy(scratch[k], outs[k])
        first, limit = slab * ROWS, n_slab * ROWS
        todo[1].wait()
        left, ks = gram(toeplitz(rt), first, limit)
        g1 = dot_t(left, ks)
        g1s = split(g1)
        lh[0:128, :], ll[0:128, :] = g1s[0][64:192, :], g1s[1][64:192, :]
        c, i = iota((48, WIN), 0), iota((48, WIN), 1)
        inside = (i + (first - 64) >= 0) & (i + (first - 64) < limit)
        rr = jnp.where((i - 32 >= 4 * c) & (i - 32 < 4 * c + 4) & inside, 0.25, 0.0).astype(BF16)
        lh[128:176, :], ll[128:176, :] = split(dot2r(rr, g1s))
        lh[176:224, :], ll[176:224, :] = rr, jnp.zeros_like(rr)
        k = iota((128, WIN), 1) + (first - 64)
        tile = split(jnp.where((k >= 0) & (k < limit), g1[64:192, :], 0.0))
        lh[224:352, :], ll[224:352, :] = split(dot3(tile, g1s))
        for k in (0, 1):
            copy(scratch[k], outs[k])
        rc0[...] = hot((iota((EXT, 384), 0) >> 2) + 32 == iota((EXT, 384), 1))
        rc1[...] = hot((iota((384, 256), 0) >> 1) == iota((384, 256), 1))
        rc2[...] = hot((iota((256, 128), 0) >> 1) == iota((256, 128), 1))
        rc3[...] = hot((iota((128, 128), 0) >> 1) - 8 == (iota((128, 128), 1) & 31))
        pc0[...] = hot(iota((384, COLS), 0) == (iota((384, COLS), 1) >> 2) + 64)
        pc1[...] = hot(iota((256, 384), 0) == (iota((256, 384), 1) >> 1))
        pc2[...] = hot(iota((128, 256), 0) == (iota((128, 256), 1) >> 1))
        pc3[...] = hot(iota((128, 128), 0) == (iota((128, 128), 1) >> 1))
        for k in range(4, 12):
            copy(scratch[k], outs[k])
        for done in todo[2:]:
            done.wait()

    return kernel


def level_mask(level, shape, slab, gc, n_slab, n_gc):
    height, width = 32 >> level, 256 >> level
    i = iota(shape, 0) - (8 >> level) + slab * height
    j = iota(shape, 1) - (64 >> level) + gc * width
    return (i >= 0) & (i < n_slab * height) & (j >= 0) & (j < n_gc * width)


def tile_mask(level, shape):
    i, j = iota(shape, 0) - (8 >> level), iota(shape, 1) - (64 >> level)
    return (i >= 0) & (i < 32 >> level) & (j >= 0) & (j < 256 >> level)


def beside(v):
    n, m = v.shape
    rows = pltpu.roll(v, 1, 0) + pltpu.roll(v, n - 1, 0)
    return rows + pltpu.roll(v, 1, 1) + pltpu.roll(v, m - 1, 1)


def operator(v, dg, cp):
    return dg * v - cp * beside(v)


def halo_kernel(n_slab, n_gc, n_grp):
    n_dev = n_slab * n_gc // n_grp

    def kernel(idx, damping, rho_in, diag, coupling, d_in, r_in, row_u, row_d, col_l, col_r, cor_l, cor_r,
               lh_in, ll_in, gh_in, gl_in, rc0_in, rc1_in, rc2_in, rc3_in,
               q_out, d2_out, r1_out, f0_out, f1_out, f2_out, e_up, e_dn, pay,
               d, r, lh, ll, gh, gl, rc0, rc1, rc2, rc3, q, d2, r1, f0, f1, f2,
               dh, dl, rh, rl, sh, sl, th, tl, c1, sem):
        slab, gc = idx[0], idx[1]
        delta = damping[0]
        c = W / (1.0 + delta)
        ins, outs = [], []

        def copy(src, dst, todo):
            done = pltpu.make_async_copy(src, dst, sem.at[len(ins) + len(outs)])
            done.start()
            todo.append(done)

        for ref, main in ((d, d_in), (r, r_in)):
            copy(main, ref.at[:, pl.ds(128, COLS)], ins)
        for src, dst in ((lh_in, lh), (ll_in, ll), (gh_in, gh), (gl_in, gl), (rc0_in, rc0), (rc1_in, rc1), (rc2_in, rc2), (rc3_in, rc3)):
            copy(src, dst, ins)

        def put(hi_ref, lo_ref, r0, c0, x):
            hi, lo = split(x)
            hi_ref[r0 : r0 + x.shape[0], c0 : c0 + x.shape[1]] = hi
            lo_ref[r0 : r0 + x.shape[0], c0 : c0 + x.shape[1]] = lo

        zero = jnp.zeros((32, EXT), BF16)
        for ref in (rh, rl):
            ref[0:32, :] = zero
            ref[WIN - 32 : WIN, :] = zero
        for at, n, ref, hi, lo in ((0, DR, d, dh, dl), (1, RR, r, rh, rl)):
            cols = slice(128 * at, 128 * at + 128)
            rows = slice(DR * at, DR * at + n)
            ref[:, 0:128] = col_l[:, cols]
            ref[:, 128 + COLS :] = col_r[:, cols]
            for first, lane, main in ((64 - n, 0, row_u), (192, 128, row_d)):
                put(hi, lo, first, 128, main[rows, :])
                put(hi, lo, first, 0, cor_l[rows, lane : lane + 128])
                put(hi, lo, first, 128 + COLS, cor_r[rows, lane : lane + 128])
            ins[at].wait()
            put(hi, lo, 64, 0, ref[...])
        for done in ins[2:4]:
            done.wait()
        ds, rs = (dh[...], dl[...]), (rh[...], rl[...])

        def left(a, b):
            return (lh[a:b, :], ll[a:b, :])

        put(sh, sl, 0, 0, dot3(left(0, 176), ds))
        put(sh, sl, 176, 0, dot3(left(0, 128), rs))
        put(th, tl, 0, 0, dot3(left(224, 352), ds))
        rd = dot2r(lh[176:224, :], ds)
        rres = dot2r(lh[176:224, :], rs)
        for done in ins[4:]:
            done.wait()
        for g in range(5):
            a, v, o = IN0[g], VARIANT[g], slice(256 * g, 256 * g + 256)
            c1[:, o] = dot3((sh[:, a : a + 512], sl[:, a : a + 512]), (gh[v], gl[v]))
        sums_of = []

        def coarse():
            fq = c1[128:176, :] + delta * rd
            f = dot2(split(jnp.concatenate([fq, rres], axis=0)), rc0[...])
            f0[...] = f
            yield None
            pair = (f[0:48], f[48:96])
            weight = 4.0
            for level, cols in ((0, rc1), (1, rc2), (2, rc3)):
                dg, cp = diag[level], coupling[level]
                sm = W / dg
                shape = pair[0].shape
                inside = level_mask(level, shape, slab, gc, n_slab, n_gc)
                mine = tile_mask(level, shape)
                bq, br = operator(pair[0], dg, cp), operator(pair[1], dg, cp)
                rest_q = jnp.where(inside, pair[0] - sm * bq, 0.0)
                rest_r = jnp.where(inside, pair[1] - sm * br, 0.0)
                low = dot2(split(jnp.concatenate([rest_q, rest_r], axis=0)), cols[...])
                own_q, own_r = jnp.where(mine, pair[0], 0.0), jnp.where(mine, pair[1], 0.0)
                sums_of.append(
                    (
                        weight * total(own_r * (2.0 * sm * pair[1] - (sm * sm) * br)),
                        weight * total(own_q * (2.0 * sm * pair[0] - (sm * sm) * bq)),
                        weight * total(own_r * (2.0 * sm * pair[0] - (sm * sm) * bq)),
                    )
                )
                weight = 2.0 * weight
                if level < 2:
                    yield None
                    n, m = (24, 48) if level == 0 else (16, 24)
                    half = jnp.where((iota((n, m), 1) >> 1) == iota((n, m), 0), 0.5, 0.0).astype(BF16)
                    pair = (dot2r(half, split(low[0:m])), dot2r(half, split(low[m : 2 * m])))
                    keep = level_mask(level + 1, pair[0].shape, slab, gc, n_slab, n_gc)
                    pair = (jnp.where(keep, pair[0], 0.0), jnp.where(keep, pair[1], 0.0))
                    out = (f1, f2)[level]
                    out[0:n, :], out[n : 2 * n, :] = pair
                    yield None
            yield pair, low

        steps = coarse()
        last = next(steps)
        for g in range(5):
            a, v, o = IN0[g], VARIANT[g], slice(256 * g, 256 * g + 256)
            d2[:, o] = dot3((th[:, a : a + 512], tl[:, a : a + 512]), (gh[3 + v], gl[3 + v]))
            last = next(steps)
        pair, low = last
        t = slice(128, 128 + COLS)
        p1 = c1[0:128, :]
        q[...] = c1[0:128, t] + delta * d[:, t]
        d2[...] = d2[...] + delta * (2.0 * p1 + delta * d[...])
        r1[...] = c1[176:304, :] + delta * r[...]
        copy(q, q_out, outs)
        copy(d2, d2_out, outs)
        copy(r1, r1_out, outs)
        near = iota((32, 128), 1) < 64
        for ref, rows in ((e_dn, slice(96, 128)), (e_up, slice(0, 32))):
            for at, x in ((0, d2), (32, r1)):
                ref[at : at + 32, 0:COLS] = x[rows, t]
                ref[at : at + 32, COLS:] = jnp.where(near, x[rows, 128 + COLS :], x[rows, 0:128])
        qv, rv, aq, ar = q[...], r[:, t], d2[:, t], r1[:, t]
        s_dq = total(d[:, t] * qv)
        e_rr = total(rv * (3.0 * rv - 3.0 * c * ar) + c * c * (ar * ar)) * c
        e_qq = total(qv * (3.0 * qv - 3.0 * c * aq) + c * c * (aq * aq)) * c
        e_rq = total(rv * (3.0 * qv - 3.0 * c * aq) + c * c * (ar * aq)) * c
        for x, y, z in sums_of:
            e_rr, e_qq, e_rq = e_rr + x, e_qq + y, e_rq + z
        for ref, to, first in ((e_up, 30, 2), (e_dn, 0, 8)):
            for at, x in ((0, pair[0]), (32, pair[1])):
                ref[at + to : at + to + 2, 0:128] = x[first : first + 2, :]
        for src, dst in ((f0, f0_out), (f1, f1_out), (f2, f2_out)):
            copy(src, dst, outs)
        i, lane = iota((16, 128), 0), iota((16, 128), 1)
        pick = (i >= 2) & (i < 10) & (((i - 2) >> 1) == (lane >> 5))
        gq = jnp.sum(jnp.where(pick, low[0:16], 0.0), axis=0, keepdims=True) * 0.5
        gr = jnp.sum(jnp.where(pick, low[16:32], 0.0), axis=0, keepdims=True) * 0.5
        lane = iota((1, 128), 1)
        sums = jnp.zeros((1, 128), F32)
        for k, x in enumerate((s_dq, e_rr, e_rq, e_qq)):
            sums = jnp.where(lane == k, x, sums)
        pay[:, 0:128] = jnp.broadcast_to(gq, (n_dev, 128))
        pay[:, 128:256] = jnp.broadcast_to(gr, (n_dev, 128))
        pay[:, 256:384] = jnp.broadcast_to(sums, (n_dev, 128))
        for done in outs:
            done.wait()

    return kernel


def final_kernel(n_slab, n_gc, n_grp):
    n_col = n_gc // n_grp

    def kernel(idx, damping, rho_in, diag, coupling, got, swap, e_u, e_d, d2_in, r1_in, lh_in, ll_in, gh_in, gl_in, q_in, r_in, d_in, sol_in,
               f0_in, f1_in, f2_in, pc0_in, pc1_in, pc2_in, pc3_in,
               o_sol, o_res, o_pre, o_dir, o_energy,
               d2, r1, lh, ll, gh, gl, q, r, d, sol, f0, f1, f2, pc0, pc1, pc2, pc3,
               uh, ul, yh, yl, vs, kk, v_sol, v_res, v_pre, v_dir, sem):
        ins, outs = [], []

        def copy(src, dst, todo):
            done = pltpu.make_async_copy(src, dst, sem.at[len(ins) + len(outs)])
            done.start()
            todo.append(done)

        for src, dst in (
            (d2_in, d2), (r1_in, r1), (lh_in.at[pl.ds(0, 128), :], lh), (ll_in.at[pl.ds(0, 128), :], ll),
            (gh_in.at[pl.ds(0, 3)], gh), (gl_in.at[pl.ds(0, 3)], gl), (r_in, r), (q_in, q), (sol_in, sol), (d_in, d),
            (f0_in, f0), (f1_in, f1), (f2_in, f2), (pc1_in, pc1), (pc2_in, pc2), (pc3_in, pc3), (pc0_in, pc0),
        ):
            copy(src, dst, ins)
        slab, gc = idx[0], idx[1]
        delta, rho = damping[0], rho_in[0]
        c = W / (1.0 + delta)
        lane = iota((1, 128), 1)
        sums = jnp.sum(got[:, 256:384] + swap[:, 256:384], axis=0, keepdims=True)
        s_dq, e_rr, e_rq, e_qq = (
            jnp.sum(jnp.where(lane == k, sums, 0.0), axis=1, keepdims=True) for k in range(4)
        )
        alpha = rho / s_dq
        dg, cp = diag[3], coupling[3]
        first = (iota((n_gc, 128), 1) & 31) == 0
        last = (iota((n_gc, 128), 1) & 31) == 31
        top, bottom = iota((n_gc, 128), 1) < 32, iota((n_gc, 128), 1) >= 96
        left_end, right_end = iota((n_gc, 128), 0) == 0, iota((n_gc, 128), 0) == n_gc - 1
        mine = gc < n_col
        rhs = []
        for s in range(n_slab):
            at = s * n_col
            a, b = (x[at : at + n_col, 128:256] - alpha * x[at : at + n_col, 0:128] for x in (got, swap))
            rhs.append(jnp.concatenate([jnp.where(mine, a, b), jnp.where(mine, b, a)], axis=0))
        zero = jnp.zeros((n_gc, 128), F32)
        v = [W * x / dg for x in rhs]
        for _ in range(3):
            ups = [pltpu.roll(x, 32, 1) for x in v]
            downs = [pltpu.roll(x, 96, 1) for x in v]
            new = []
            for s in range(n_slab):
                x = v[s]
                low = jnp.where(left_end, 0.0, pltpu.roll(pltpu.roll(x, 97, 1), 1, 0))
                high = jnp.where(right_end, 0.0, pltpu.roll(pltpu.roll(x, 31, 1), n_gc - 1, 0))
                beside_x = jnp.where(first, low, pltpu.roll(x, 1, 1))
                beside_x = beside_x + jnp.where(last, high, pltpu.roll(x, 127, 1))
                beside_x = beside_x + jnp.where(top, ups[s - 1] if s > 0 else zero, ups[s])
                beside_x = beside_x + jnp.where(bottom, downs[s + 1] if s < n_slab - 1 else zero, downs[s])
                new.append(x + W * (rhs[s] - (dg * x - cp * beside_x)) / dg)
            v = new
        e3 = total(sum(a * b for a, b in zip(rhs, v)))
        energy = e_rr - alpha * (2.0 * e_rq) + (alpha * alpha) * e_qq + 32.0 * e3
        o_energy[...] = energy
        pitch = n_gc + 16
        vs[...] = jnp.zeros(vs.shape, F32)
        for s in range(n_slab):
            at = (s + 1) * pitch + 8
            vs[at : at + n_gc, :] = v[s]
        v3 = jnp.zeros((8, 128), F32)
        lanes, rows8 = iota((1, 128), 1), iota((8, 128), 0)
        for k, i in ((-1, 3), (0, 0), (0, 1), (0, 2), (0, 3), (1, 0)):
            at = (slab + 1 + k) * pitch + 8 + gc
            mid, lo, hi = (vs[pl.ds(at + x, 1), :] for x in (0, -1, 1))
            line = pltpu.roll(mid, (8 - 32 * i) % 128, 1)
            line = jnp.where(lanes == 7, pltpu.roll(lo, (8 - 32 * i - 32) % 128, 1), line)
            line = jnp.where(lanes == 40, pltpu.roll(hi, (8 - 32 * i + 32) % 128, 1), line)
            line = jnp.where((lanes >= 7) & (lanes <= 40), line, 0.0)
            v3 = jnp.where(rows8 == 4 * k + i + 1, line, v3)
        for ref in (uh, ul):
            ref[0:32, :] = jnp.zeros((32, EXT), BF16)
            ref[WIN - 32 : WIN, :] = jnp.zeros((32, EXT), BF16)
        for done in ins[:4]:
            done.wait()
        near = iota((32, 128), 1) < 64
        for at, x, spare in ((32, e_u, 0), (192, e_d, 30)):
            edge = x[32:64, :] - alpha * x[0:32, :]
            place = iota((32, COLS + 128), 0)
            edge = jnp.where((place == spare) | (place == spare + 1), 0.0, edge)
            side = edge[:, COLS:]
            for first, part in ((128, edge[:, 0:COLS]), (0, jnp.where(near, 0.0, side)), (128 + COLS, jnp.where(near, side, 0.0))):
                hi, lo = split(part)
                uh[at : at + 32, first : first + part.shape[1]] = hi
                ul[at : at + 32, first : first + part.shape[1]] = lo
        uh[64:192, :], ul[64:192, :] = split(r1[...] - alpha * d2[...])
        yh[...], yl[...] = split(dot3((lh[...], ll[...]), (uh[...], ul[...])))
        for done in ins[4:19]:
            done.wait()
        v_res[...] = r[...] - alpha * q[...]
        copy(v_res, o_res, outs)
        v_sol[...] = sol[...] + alpha * d[...]
        copy(v_sol, o_sol, outs)
        edge_u = e_u[32:34, 0:128] - alpha * e_u[0:2, 0:128]
        edge_d = e_d[62:64, 0:128] - alpha * e_d[30:32, 0:128]
        own = f2[16:32, :] - alpha * f2[0:16, :]
        row = iota((16, 128), 0)
        own = jnp.where(row == 0, edge_u[0:1, :], jnp.where(row == 1, edge_u[1:2, :], own))
        own = jnp.where(row == 10, edge_d[0:1, :], jnp.where(row == 11, edge_d[1:2, :], own))
        own = jnp.where(row < 12, own, 0.0)
        f = [f0[48:96, :] - alpha * f0[0:48, :], f1[24:48, :] - alpha * f1[0:24, :], own]

        def upwards():
            low = v3
            for level, cols in ((2, pc3), (1, pc2), (0, pc1)):
                dg, cp = diag[level], coupling[level]
                sm = W / dg
                n, m = f[level].shape[0], low.shape[0]
                double = hot((iota((n, m), 0) >> 1) == iota((n, m), 1))
                wide = dot2r(double, split(dot2(split(low), cols[...])))
                inside = level_mask(level, f[level].shape, slab, gc, n_slab, n_gc)
                x = jnp.where(inside, sm * f[level] + wide, 0.0)
                low = jnp.where(inside, x + sm * (f[level] - operator(x, dg, cp)), 0.0)
                if level > 0:
                    yield None
            four = hot((iota((ROWS, 48), 0) >> 2) + 8 == iota((ROWS, 48), 1))
            yield split(dot2r(four, split(low)))

        steps = upwards()
        for g in range(5):
            a, v, o = IN0[g], VARIANT[g], slice(256 * g, 256 * g + 256)
            kk[:, o] = dot3((yh[:, a : a + 512], yl[:, a : a + 512]), (gh[v], gl[v]))
            if g in (0, 2, 4):
                spread = next(steps)
        t = slice(128, 128 + COLS)
        au = r1[:, t] - alpha * d2[:, t]
        smooth = c * (3.0 * v_res[...] - (3.0 * c) * au + (c * c) * (kk[:, t] + delta * au))
        pre = smooth + dot2(spread, pc0[...])
        v_pre[...] = pre
        copy(v_pre, o_pre, outs)
        v_dir[...] = pre + (energy / rho) * d[...]
        copy(v_dir, o_dir, outs)
        for done in outs:
            done.wait()

    return kernel


def call(kernel, specs, outs, out_specs, scratch, sems=0, more=()):
    where = {"s": pltpu.SMEM, "v": pltpu.VMEM, "h": pltpu.HBM}
    if INTERPRET:
        where["h"] = pl.ANY

    def out(x, shape, kind):
        if x == "h" and not INTERPRET:
            return pltpu.HBM(shape, kind)
        return jax.ShapeDtypeStruct(shape, kind)

    run = pl.pallas_call(
        kernel,
        out_shape=[out(x, s, t) for x, (s, t) in zip(out_specs, outs)],
        in_specs=[pl.BlockSpec(memory_space=where[x]) for x in specs],
        out_specs=[pl.BlockSpec(memory_space=where[x]) for x in out_specs],
        scratch_shapes=[pltpu.VMEM(s, t) for s, t in scratch] + ([pltpu.SemaphoreType.DMA((sems,))] if sems else []) + list(more),
        compiler_params=pltpu.CompilerParams(vmem_limit_bytes=40 * 1024 * 1024),
        interpret=INTERPRET,
    )

    def apply(*args):
        if INTERPRET:
            return run(*args)
        return run(*(pltpu.with_memory_space_constraint(a, pltpu.HBM) if x == "h" else a for x, a in zip(specs, args)))

    return apply


def run_copies(sem, pairs):
    todo = []
    for k, (src, dst) in enumerate(pairs):
        todo.append(pltpu.make_async_copy(src, dst, sem.at[k]))
        todo[-1].start()
    for done in todo:
        done.wait()


def edges_kernel(d, r, row_u, row_d, col_l, col_r, sem):
    pairs = []
    for n, at, x in ((DR, 0, d), (RR, DR, r)):
        pairs.append((x.at[pl.ds(0, n), :], row_u.at[pl.ds(at, n), :]))
        pairs.append((x.at[pl.ds(ROWS - n, n), :], row_d.at[pl.ds(at, n), :]))
    for at, x in ((0, d), (128, r)):
        pairs.append((x.at[:, pl.ds(0, 128)], col_l.at[:, pl.ds(at, 128)]))
        pairs.append((x.at[:, pl.ds(COLS - 128, 128)], col_r.at[:, pl.ds(at, 128)]))
    run_copies(sem, pairs)


def corners_kernel(from_u, from_d, cor_l, cor_r):
    for lane, x in ((0, from_u), (128, from_d)):
        cor_l[:, lane : lane + 128] = x[:, 0:128]
        cor_r[:, lane : lane + 128] = x[:, COLS - 128 :]


def solution(mesh):
    n_grp, n_slab, n_col = mesh.shape["grp"], mesh.shape["slab"], mesh.shape["col"]
    n_gc = n_grp * n_col
    n_dev = n_slab * n_col

    def forward(n):
        return [(i, i + 1) for i in range(n - 1)]

    def backward(n):
        return [(i + 1, i) for i in range(n - 1)]

    def body(sol, r, d, row_taps, col_taps, damping, rho, diag, coupling):
        idx = jnp.stack([lax.axis_index("slab"), lax.axis_index(GC)]).astype(jnp.int32)
        row_u, row_d, col_l, col_r = call(
            edges_kernel, "hh", [((DR + RR, COLS), F32)] * 2 + [((ROWS, 256), F32)] * 2, "vvvv", [], 8
        )(d, r)
        from_u = lax.ppermute(row_d, "slab", forward(n_slab))
        from_d = lax.ppermute(row_u, "slab", backward(n_slab))
        from_l = lax.ppermute(col_r, GC, forward(n_gc))
        from_r = lax.ppermute(col_l, GC, backward(n_gc))
        par = (damping[None], rho[None], diag, coupling)
        mat_shapes = [((352, WIN), BF16)] * 2 + [((6, 512, 256), BF16)] * 2
        mat_shapes += [((EXT, 384), BF16), ((384, 256), BF16), ((256, 128), BF16), ((128, 128), BF16)]
        back_shapes = [((384, COLS), BF16), ((256, 384), BF16), ((128, 256), BF16), ((128, 128), BF16)]
        mats = call(
            matrices_kernel(n_slab, n_gc),
            "shh",
            mat_shapes + back_shapes,
            "h" * 12,
            mat_shapes + back_shapes,
            14,
            [pltpu.SMEM((TAPS,), F32)] * 2,
        )(idx, row_taps, col_taps)
        lh, ll, gh, gl, rc0, rc1, rc2, rc3, pc0, pc1, pc2, pc3 = mats
        send_l, send_r = call(corners_kernel, "vv", [((DR + RR, 256), F32)] * 2, "vv", [])(from_u, from_d)
        cor_l = lax.ppermute(send_r, GC, forward(n_gc))
        cor_r = lax.ppermute(send_l, GC, backward(n_gc))
        results = [((ROWS, COLS), F32), ((ROWS, EXT), F32), ((ROWS, EXT), F32)]
        results += [((96, 384), F32), ((48, 256), F32), ((32, 128), F32)]
        q, d2, r1, f0, f1, f2, e_up, e_dn, pay = call(
            halo_kernel(n_slab, n_gc, n_grp),
            "s" * 5 + "hh" + "v" * 6 + "h" * 8,
            results + [((64, COLS + 128), F32)] * 2 + [((n_dev, 384), F32)],
            "h" * 6 + "vvv",
            [((ROWS, EXT), F32)] * 2
            + mat_shapes
            + results
            + [((WIN, EXT), BF16)] * 4
            + [((304, EXT), BF16)] * 2
            + [((128, EXT), BF16)] * 2
            + [((304, EXT), F32)],
            40,
        )(idx, *par, d, r, from_u, from_d, from_l, from_r, cor_l, cor_r, lh, ll, gh, gl, rc0, rc1, rc2, rc3)
        edge_u = lax.ppermute(e_dn, "slab", forward(n_slab))
        edge_d = lax.ppermute(e_up, "slab", backward(n_slab))
        got = lax.all_to_all(pay, ("slab", "col"), 0, 0, tiled=True)
        swap = lax.ppermute(got, "grp", [(i, (i + 1) % n_grp) for i in range(n_grp)])
        tile = ((ROWS, COLS), F32)
        n_sol, n_res, pre, n_dir, energy = call(
            final_kernel(n_slab, n_gc, n_grp),
            "s" * 5 + "vvvv" + "h" * 17,
            [tile] * 4 + [((1, 1), F32)],
            "hhhhv",
            [((ROWS, EXT), F32)] * 2
            + [((128, WIN), BF16)] * 2
            + [((3, 512, 256), BF16)] * 2
            + [tile] * 4
            + [((96, 384), F32), ((48, 256), F32), ((32, 128), F32)]
            + back_shapes
            + [((WIN, EXT), BF16)] * 2
            + [((ROWS, EXT), BF16)] * 2
            + [(((n_slab + 2) * (n_gc + 16), 128), F32), ((ROWS, EXT), F32)]
            + [tile] * 4,
            24,
        )(idx, *par, got, swap, edge_u, edge_d, d2, r1, lh, ll, gh, gl, q, r, d, sol, f0, f1, f2, pc0, pc1, pc2, pc3)
        return n_sol, n_res, pre, n_dir, energy[0, 0]

    tile, rep = P("slab", GC), P()
    return jax.shard_map(
        body,
        mesh=mesh,
        in_specs=(tile,) * 3 + (rep,) * 6,
        out_specs=(tile,) * 4 + (rep,),
        check_vma=False,
    )
```

```python
import jax
import jax.numpy as jnp
from jax import lax
from jax.experimental import pallas as pl
from jax.experimental.pallas import tpu as pltpu
from jax.sharding import PartitionSpec as P


INTERPRET = False
W = 2.0 / 3.0
TAPS = 31
H = TAPS // 2
ROWS, COLS = 128, 1024
EXT = COLS + 256
WIN = ROWS + 128
DR, RR = 64, 32
IN0 = (0, 128, 384, 640, 768)
VARIANT = (0, 1, 1, 1, 2)
GC = ("grp", "col")
F32, BF16 = jnp.float32, jnp.bfloat16


def iota(shape, dim):
    return lax.broadcasted_iota(jnp.int32, shape, dim)


def split(x):
    high = x.astype(BF16)
    return high, (x - high.astype(F32)).astype(BF16)


def dot(a, b):
    return jnp.dot(a, b, preferred_element_type=F32)


def dot3(a, b):
    (ah, al), (bh, bl) = a, b
    return dot(ah, bh) + (dot(ah, bl) + dot(al, bh))


def dot2(a, b):
    return dot(a[0], b) + dot(a[1], b)


def dot2r(a, b):
    return dot(a, b[0]) + dot(a, b[1])


def hot(cond):
    return jnp.where(cond, 1.0, 0.0).astype(BF16)


def total(x):
    return jnp.sum(jnp.sum(x, axis=0, keepdims=True), axis=1, keepdims=True)


def dot_t(a, b):
    def nt(x, y):
        return lax.dot_general(x, y, (((1,), (1,)), ((), ())), preferred_element_type=F32)

    (ah, al), (bh, bl) = a, b
    return nt(ah, bh) + (nt(ah, bl) + nt(al, bh))


def toeplitz(taps):
    sum_taps = taps[0]
    for t in range(1, TAPS):
        sum_taps = sum_taps + taps[t]
    lane = iota((8, 384), 1)
    base = jnp.zeros((8, 384), F32)
    for t in range(TAPS):
        base = jnp.where(lane == 64 + H - t, taps[t], base)
    base = base / jnp.full((8, 384), sum_taps, F32)
    return pltpu.roll(jnp.broadcast_to(base[0:1], (256, 384)), 0, 1, stride=1, stride_axis=0)


def gram(kt, first, limit):
    ks = split(kt)
    left = ks
    if first is not None:
        m = iota((256, 384), 1) + (first - 128)
        left = split(jnp.where((m >= 0) & (m < limit), kt, 0.0))
    return left, ks


def block_powers(kt, first, limit):
    left, ks = gram(kt, first, limit)
    wide = dot_t(left, ks)
    g1 = dot_t(left, (ks[0][64:192], ks[1][64:192]))
    if first is not None:
        i = iota((256, 128), 0) + (first - 64)
        g1 = jnp.where((i >= 0) & (i < limit), g1, 0.0)
    g1s = split(g1)
    return g1s, split(dot3(split(wide), g1s))


def matrices_kernel(n_slab, n_gc):
    def kernel(idx, rt_in, ct_in, *refs):
        outs, scratch, sem, rt, ct = refs[:12], refs[12:24], refs[24], refs[25], refs[26]
        todo = []

        def copy(src, dst):
            todo.append(pltpu.make_async_copy(src, dst, sem.at[len(todo)]))
            todo[-1].start()

        copy(ct_in, ct)
        copy(rt_in, rt)
        lh, ll, gh, gl, rc0, rc1, rc2, rc3, pc0, pc1, pc2, pc3 = scratch
        slab, gc = idx[0], idx[1]
        gh[...], gl[...] = jnp.zeros(gh.shape, BF16), jnp.zeros(gl.shape, BF16)
        todo[0].wait()
        kt = toeplitz(ct)
        inner = block_powers(kt, None, None)
        end = block_powers(kt, jnp.where(gc == 0, 0, gc * COLS + COLS - 128), n_gc * COLS)
        at_l, at_r = gc == 0, gc == n_gc - 1
        has_l = jnp.where(gc > 0, 1.0, 0.0).astype(F32)
        has_r = jnp.where(gc < n_gc - 1, 1.0, 0.0).astype(F32)
        for power in range(2):
            for at, ref in enumerate((gh, gl)):
                mid = inner[power][at]
                wide, other = mid.astype(F32), end[power][at].astype(F32)
                low = jnp.where(at_l, other, wide).astype(BF16)
                high = jnp.where(at_r, other, wide).astype(BF16)
                outer_l, outer_r = (wide * has_l).astype(BF16), (wide * has_r).astype(BF16)
                for v, off, blocks in (
                    (0, 0, (outer_l, low)),
                    (1, 128, (mid, mid)),
                    (2, 256, (high, outer_r)),
                ):
                    for b in range(2):
                        start = off + 128 * b - 64
                        lo, hi = max(0, start), min(512, start + 256)
                        ref[3 * power + v, lo:hi, 128 * b : 128 * b + 128] = blocks[b][lo - start : hi - start]
        for k in (2, 3):
            copy(scratch[k], outs[k])
        first, limit = slab * ROWS, n_slab * ROWS
        todo[1].wait()
        left, ks = gram(toeplitz(rt), first, limit)
        g1 = dot_t(left, ks)
        g1s = split(g1)
        lh[0:128, :], ll[0:128, :] = g1s[0][64:192, :], g1s[1][64:192, :]
        c, i = iota((48, WIN), 0), iota((48, WIN), 1)
        inside = (i + (first - 64) >= 0) & (i + (first - 64) < limit)
        rr = jnp.where((i - 32 >= 4 * c) & (i - 32 < 4 * c + 4) & inside, 0.25, 0.0).astype(BF16)
        lh[128:176, :], ll[128:176, :] = split(dot2r(rr, g1s))
        lh[176:224, :], ll[176:224, :] = rr, jnp.zeros_like(rr)
        k = iota((128, WIN), 1) + (first - 64)
        tile = split(jnp.where((k >= 0) & (k < limit), g1[64:192, :], 0.0))
        lh[224:352, :], ll[224:352, :] = split(dot3(tile, g1s))
        for k in (0, 1):
            copy(scratch[k], outs[k])
        rc0[...] = hot((iota((EXT, 384), 0) >> 2) + 32 == iota((EXT, 384), 1))
        rc1[...] = hot((iota((384, 256), 0) >> 1) == iota((384, 256), 1))
        rc2[...] = hot((iota((256, 128), 0) >> 1) == iota((256, 128), 1))
        rc3[...] = hot((iota((128, 128), 0) >> 1) - 8 == (iota((128, 128), 1) & 31))
        pc0[...] = hot(iota((384, COLS), 0) == (iota((384, COLS), 1) >> 2) + 64)
        pc1[...] = hot(iota((256, 384), 0) == (iota((256, 384), 1) >> 1))
        pc2[...] = hot(iota((128, 256), 0) == (iota((128, 256), 1) >> 1))
        pc3[...] = hot(iota((128, 128), 0) == (iota((128, 128), 1) >> 1))
        for k in range(4, 12):
            copy(scratch[k], outs[k])
        for done in todo[2:]:
            done.wait()

    return kernel


def level_mask(level, shape, slab, gc, n_slab, n_gc):
    height, width = 32 >> level, 256 >> level
    i = iota(shape, 0) - (8 >> level) + slab * height
    j = iota(shape, 1) - (64 >> level) + gc * width
    return (i >= 0) & (i < n_slab * height) & (j >= 0) & (j < n_gc * width)


def tile_mask(level, shape):
    i, j = iota(shape, 0) - (8 >> level), iota(shape, 1) - (64 >> level)
    return (i >= 0) & (i < 32 >> level) & (j >= 0) & (j < 256 >> level)


def beside(v):
    n, m = v.shape
    rows = pltpu.roll(v, 1, 0) + pltpu.roll(v, n - 1, 0)
    return rows + pltpu.roll(v, 1, 1) + pltpu.roll(v, m - 1, 1)


def operator(v, dg, cp):
    return dg * v - cp * beside(v)


def halo_kernel(n_slab, n_gc, n_grp):
    n_dev = n_slab * n_gc // n_grp

    def kernel(idx, damping, rho_in, diag, coupling, d_in, r_in, row_u, row_d, col_l, col_r, cor_l, cor_r,
               lh_in, ll_in, gh_in, gl_in, rc0_in, rc1_in, rc2_in, rc3_in,
               q_out, d2_out, r1_out, f0_out, f1_out, f2_out, e_up, e_dn, pay,
               d, r, lh, ll, gh, gl, rc0, rc1, rc2, rc3, q, d2, r1, f0, f1, f2,
               dh, dl, rh, rl, sh, sl, th, tl, c1, sem):
        slab, gc = idx[0], idx[1]
        delta = damping[0]
        c = W / (1.0 + delta)
        ins, outs = [], []

        def copy(src, dst, todo):
            done = pltpu.make_async_copy(src, dst, sem.at[len(ins) + len(outs)])
            done.start()
            todo.append(done)

        for ref, main in ((d, d_in), (r, r_in)):
            copy(main, ref.at[:, pl.ds(128, COLS)], ins)
        for src, dst in ((lh_in, lh), (ll_in, ll), (gh_in, gh), (gl_in, gl), (rc0_in, rc0), (rc1_in, rc1), (rc2_in, rc2), (rc3_in, rc3)):
            copy(src, dst, ins)

        def put(hi_ref, lo_ref, r0, c0, x):
            hi, lo = split(x)
            hi_ref[r0 : r0 + x.shape[0], c0 : c0 + x.shape[1]] = hi
            lo_ref[r0 : r0 + x.shape[0], c0 : c0 + x.shape[1]] = lo

        zero = jnp.zeros((32, EXT), BF16)
        for ref in (rh, rl):
            ref[0:32, :] = zero
            ref[WIN - 32 : WIN, :] = zero
        for at, n, ref, hi, lo in ((0, DR, d, dh, dl), (1, RR, r, rh, rl)):
            cols = slice(128 * at, 128 * at + 128)
            rows = slice(DR * at, DR * at + n)
            ref[:, 0:128] = col_l[:, cols]
            ref[:, 128 + COLS :] = col_r[:, cols]
            for first, lane, main in ((64 - n, 0, row_u), (192, 128, row_d)):
                put(hi, lo, first, 128, main[rows, :])
                put(hi, lo, first, 0, cor_l[rows, lane : lane + 128])
                put(hi, lo, first, 128 + COLS, cor_r[rows, lane : lane + 128])
            ins[at].wait()
            put(hi, lo, 64, 0, ref[...])
        for done in ins[2:4]:
            done.wait()
        ds, rs = (dh[...], dl[...]), (rh[...], rl[...])

        def left(a, b):
            return (lh[a:b, :], ll[a:b, :])

        rows_d = dot3(left(0, 352), ds)
        put(sh, sl, 0, 0, rows_d[0:176])
        put(th, tl, 0, 0, rows_d[224:352])
        rd = rows_d[176:224]
        rows_r = dot3(left(0, 224), rs)
        put(sh, sl, 176, 0, rows_r[0:128])
        rres = rows_r[176:224]
        for done in ins[4:]:
            done.wait()
        for g in range(5):
            a, v, o = IN0[g], VARIANT[g], slice(256 * g, 256 * g + 256)
            c1[:, o] = dot3((sh[:, a : a + 512], sl[:, a : a + 512]), (gh[v], gl[v]))
        sums_of = []

        def coarse():
            fq = c1[128:176, :] + delta * rd
            f = dot2(split(jnp.concatenate([fq, rres], axis=0)), rc0[...])
            f0[...] = f
            yield None
            pair = (f[0:48], f[48:96])
            weight = 4.0
            for level, cols in ((0, rc1), (1, rc2), (2, rc3)):
                dg, cp = diag[level], coupling[level]
                sm = W / dg
                shape = pair[0].shape
                inside = level_mask(level, shape, slab, gc, n_slab, n_gc)
                mine = tile_mask(level, shape)
                bq, br = operator(pair[0], dg, cp), operator(pair[1], dg, cp)
                rest_q = jnp.where(inside, pair[0] - sm * bq, 0.0)
                rest_r = jnp.where(inside, pair[1] - sm * br, 0.0)
                low = dot2(split(jnp.concatenate([rest_q, rest_r], axis=0)), cols[...])
                own_q, own_r = jnp.where(mine, pair[0], 0.0), jnp.where(mine, pair[1], 0.0)
                sums_of.append(
                    (
                        weight * total(own_r * (2.0 * sm * pair[1] - (sm * sm) * br)),
                        weight * total(own_q * (2.0 * sm * pair[0] - (sm * sm) * bq)),
                        weight * total(own_r * (2.0 * sm * pair[0] - (sm * sm) * bq)),
                    )
                )
                weight = 2.0 * weight
                if level < 2:
                    yield None
                    n, m = (24, 48) if level == 0 else (16, 24)
                    half = jnp.where((iota((n, m), 1) >> 1) == iota((n, m), 0), 0.5, 0.0).astype(BF16)
                    pair = (dot2r(half, split(low[0:m])), dot2r(half, split(low[m : 2 * m])))
                    keep = level_mask(level + 1, pair[0].shape, slab, gc, n_slab, n_gc)
                    pair = (jnp.where(keep, pair[0], 0.0), jnp.where(keep, pair[1], 0.0))
                    out = (f1, f2)[level]
                    out[0:n, :], out[n : 2 * n, :] = pair
                    yield None
            yield pair, low

        steps = coarse()
        last = next(steps)
        for g in range(5):
            a, v, o = IN0[g], VARIANT[g], slice(256 * g, 256 * g + 256)
            d2[:, o] = dot3((th[:, a : a + 512], tl[:, a : a + 512]), (gh[3 + v], gl[3 + v]))
            last = next(steps)
        pair, low = last
        t = slice(128, 128 + COLS)
        p1 = c1[0:128, :]
        q[...] = c1[0:128, t] + delta * d[:, t]
        d2[...] = d2[...] + delta * (2.0 * p1 + delta * d[...])
        r1[...] = c1[176:304, :] + delta * r[...]
        copy(q, q_out, outs)
        copy(d2, d2_out, outs)
        copy(r1, r1_out, outs)
        near = iota((32, 128), 1) < 64
        for ref, rows in ((e_dn, slice(96, 128)), (e_up, slice(0, 32))):
            for at, x in ((0, d2), (32, r1)):
                ref[at : at + 32, 0:COLS] = x[rows, t]
                ref[at : at + 32, COLS:] = jnp.where(near, x[rows, 128 + COLS :], x[rows, 0:128])
        qv, rv, aq, ar = q[...], r[:, t], d2[:, t], r1[:, t]
        s_dq = total(d[:, t] * qv)
        e_rr = total(rv * (3.0 * rv - 3.0 * c * ar) + c * c * (ar * ar)) * c
        e_qq = total(qv * (3.0 * qv - 3.0 * c * aq) + c * c * (aq * aq)) * c
        e_rq = total(rv * (3.0 * qv - 3.0 * c * aq) + c * c * (ar * aq)) * c
        for x, y, z in sums_of:
            e_rr, e_qq, e_rq = e_rr + x, e_qq + y, e_rq + z
        for ref, to, first in ((e_up, 30, 2), (e_dn, 0, 8)):
            for at, x in ((0, pair[0]), (32, pair[1])):
                ref[at + to : at + to + 2, 0:128] = x[first : first + 2, :]
        for src, dst in ((f0, f0_out), (f1, f1_out), (f2, f2_out)):
            copy(src, dst, outs)
        i, lane = iota((16, 128), 0), iota((16, 128), 1)
        pick = (i >= 2) & (i < 10) & (((i - 2) >> 1) == (lane >> 5))
        gq = jnp.sum(jnp.where(pick, low[0:16], 0.0), axis=0, keepdims=True) * 0.5
        gr = jnp.sum(jnp.where(pick, low[16:32], 0.0), axis=0, keepdims=True) * 0.5
        lane = iota((1, 128), 1)
        sums = jnp.zeros((1, 128), F32)
        for k, x in enumerate((s_dq, e_rr, e_rq, e_qq)):
            sums = jnp.where(lane == k, x, sums)
        pay[:, 0:128] = jnp.broadcast_to(gq, (n_dev, 128))
        pay[:, 128:256] = jnp.broadcast_to(gr, (n_dev, 128))
        pay[:, 256:384] = jnp.broadcast_to(sums, (n_dev, 128))
        for done in outs:
            done.wait()

    return kernel


def final_kernel(n_slab, n_gc, n_grp):
    n_col = n_gc // n_grp

    def kernel(idx, damping, rho_in, diag, coupling, got, swap, e_u, e_d, d2_in, r1_in, lh_in, ll_in, gh_in, gl_in, q_in, r_in, d_in, sol_in,
               f0_in, f1_in, f2_in, pc0_in, pc1_in, pc2_in, pc3_in,
               o_sol, o_res, o_pre, o_dir, o_energy,
               d2, r1, lh, ll, gh, gl, q, r, d, sol, f0, f1, f2, pc0, pc1, pc2, pc3,
               uh, ul, yh, yl, vs, kk, v_sol, v_res, v_pre, v_dir, sem):
        ins, outs = [], []

        def copy(src, dst, todo):
            done = pltpu.make_async_copy(src, dst, sem.at[len(ins) + len(outs)])
            done.start()
            todo.append(done)

        for src, dst in (
            (d2_in, d2), (r1_in, r1), (lh_in.at[pl.ds(0, 128), :], lh), (ll_in.at[pl.ds(0, 128), :], ll),
            (gh_in.at[pl.ds(0, 3)], gh), (gl_in.at[pl.ds(0, 3)], gl), (r_in, r), (q_in, q), (sol_in, sol), (d_in, d),
            (f0_in, f0), (f1_in, f1), (f2_in, f2), (pc1_in, pc1), (pc2_in, pc2), (pc3_in, pc3), (pc0_in, pc0),
        ):
            copy(src, dst, ins)
        slab, gc = idx[0], idx[1]
        delta, rho = damping[0], rho_in[0]
        c = W / (1.0 + delta)
        lane = iota((1, 128), 1)
        sums = jnp.sum(got[:, 256:384] + swap[:, 256:384], axis=0, keepdims=True)
        s_dq, e_rr, e_rq, e_qq = (
            jnp.sum(jnp.where(lane == k, sums, 0.0), axis=1, keepdims=True) for k in range(4)
        )
        alpha = rho / s_dq
        dg, cp = diag[3], coupling[3]
        first = (iota((n_gc, 128), 1) & 31) == 0
        last = (iota((n_gc, 128), 1) & 31) == 31
        top, bottom = iota((n_gc, 128), 1) < 32, iota((n_gc, 128), 1) >= 96
        left_end, right_end = iota((n_gc, 128), 0) == 0, iota((n_gc, 128), 0) == n_gc - 1
        mine = gc < n_col
        rhs = []
        for s in range(n_slab):
            at = s * n_col
            a, b = (x[at : at + n_col, 128:256] - alpha * x[at : at + n_col, 0:128] for x in (got, swap))
            rhs.append(jnp.concatenate([jnp.where(mine, a, b), jnp.where(mine, b, a)], axis=0))
        zero = jnp.zeros((n_gc, 128), F32)
        v = [W * x / dg for x in rhs]
        for _ in range(3):
            ups = [pltpu.roll(x, 32, 1) for x in v]
            downs = [pltpu.roll(x, 96, 1) for x in v]
            new = []
            for s in range(n_slab):
                x = v[s]
                low = jnp.where(left_end, 0.0, pltpu.roll(pltpu.roll(x, 97, 1), 1, 0))
                high = jnp.where(right_end, 0.0, pltpu.roll(pltpu.roll(x, 31, 1), n_gc - 1, 0))
                beside_x = jnp.where(first, low, pltpu.roll(x, 1, 1))
                beside_x = beside_x + jnp.where(last, high, pltpu.roll(x, 127, 1))
                beside_x = beside_x + jnp.where(top, ups[s - 1] if s > 0 else zero, ups[s])
                beside_x = beside_x + jnp.where(bottom, downs[s + 1] if s < n_slab - 1 else zero, downs[s])
                new.append(x + W * (rhs[s] - (dg * x - cp * beside_x)) / dg)
            v = new
        e3 = total(sum(a * b for a, b in zip(rhs, v)))
        energy = e_rr - alpha * (2.0 * e_rq) + (alpha * alpha) * e_qq + 32.0 * e3
        o_energy[...] = energy
        pitch = n_gc + 16
        vs[...] = jnp.zeros(vs.shape, F32)
        for s in range(n_slab):
            at = (s + 1) * pitch + 8
            vs[at : at + n_gc, :] = v[s]
        v3 = jnp.zeros((8, 128), F32)
        lanes, rows8 = iota((1, 128), 1), iota((8, 128), 0)
        for k, i in ((-1, 3), (0, 0), (0, 1), (0, 2), (0, 3), (1, 0)):
            at = (slab + 1 + k) * pitch + 8 + gc
            mid, lo, hi = (vs[pl.ds(at + x, 1), :] for x in (0, -1, 1))
            line = pltpu.roll(mid, (8 - 32 * i) % 128, 1)
            line = jnp.where(lanes == 7, pltpu.roll(lo, (8 - 32 * i - 32) % 128, 1), line)
            line = jnp.where(lanes == 40, pltpu.roll(hi, (8 - 32 * i + 32) % 128, 1), line)
            line = jnp.where((lanes >= 7) & (lanes <= 40), line, 0.0)
            v3 = jnp.where(rows8 == 4 * k + i + 1, line, v3)
        for ref in (uh, ul):
            ref[0:32, :] = jnp.zeros((32, EXT), BF16)
            ref[WIN - 32 : WIN, :] = jnp.zeros((32, EXT), BF16)
        for done in ins[:4]:
            done.wait()
        near = iota((32, 128), 1) < 64
        for at, x, spare in ((32, e_u, 0), (192, e_d, 30)):
            edge = x[32:64, :] - alpha * x[0:32, :]
            place = iota((32, COLS + 128), 0)
            edge = jnp.where((place == spare) | (place == spare + 1), 0.0, edge)
            side = edge[:, COLS:]
            for first, part in ((128, edge[:, 0:COLS]), (0, jnp.where(near, 0.0, side)), (128 + COLS, jnp.where(near, side, 0.0))):
                hi, lo = split(part)
                uh[at : at + 32, first : first + part.shape[1]] = hi
                ul[at : at + 32, first : first + part.shape[1]] = lo
        uh[64:192, :], ul[64:192, :] = split(r1[...] - alpha * d2[...])
        yh[...], yl[...] = split(dot3((lh[...], ll[...]), (uh[...], ul[...])))
        for done in ins[4:19]:
            done.wait()
        v_res[...] = r[...] - alpha * q[...]
        copy(v_res, o_res, outs)
        v_sol[...] = sol[...] + alpha * d[...]
        copy(v_sol, o_sol, outs)
        edge_u = e_u[32:34, 0:128] - alpha * e_u[0:2, 0:128]
        edge_d = e_d[62:64, 0:128] - alpha * e_d[30:32, 0:128]
        own = f2[16:32, :] - alpha * f2[0:16, :]
        row = iota((16, 128), 0)
        own = jnp.where(row == 0, edge_u[0:1, :], jnp.where(row == 1, edge_u[1:2, :], own))
        own = jnp.where(row == 10, edge_d[0:1, :], jnp.where(row == 11, edge_d[1:2, :], own))
        own = jnp.where(row < 12, own, 0.0)
        f = [f0[48:96, :] - alpha * f0[0:48, :], f1[24:48, :] - alpha * f1[0:24, :], own]

        def upwards():
            low = v3
            for level, cols in ((2, pc3), (1, pc2), (0, pc1)):
                dg, cp = diag[level], coupling[level]
                sm = W / dg
                n, m = f[level].shape[0], low.shape[0]
                double = hot((iota((n, m), 0) >> 1) == iota((n, m), 1))
                wide = dot2r(double, split(dot2(split(low), cols[...])))
                inside = level_mask(level, f[level].shape, slab, gc, n_slab, n_gc)
                x = jnp.where(inside, sm * f[level] + wide, 0.0)
                low = jnp.where(inside, x + sm * (f[level] - operator(x, dg, cp)), 0.0)
                if level > 0:
                    yield None
            four = hot((iota((ROWS, 48), 0) >> 2) + 8 == iota((ROWS, 48), 1))
            yield split(dot2r(four, split(low)))

        steps = upwards()
        for g in range(5):
            a, v, o = IN0[g], VARIANT[g], slice(256 * g, 256 * g + 256)
            kk[:, o] = dot3((yh[:, a : a + 512], yl[:, a : a + 512]), (gh[v], gl[v]))
            if g in (0, 2, 4):
                spread = next(steps)
        t = slice(128, 128 + COLS)
        au = r1[:, t] - alpha * d2[:, t]
        smooth = c * (3.0 * v_res[...] - (3.0 * c) * au + (c * c) * (kk[:, t] + delta * au))
        pre = smooth + dot2(spread, pc0[...])
        v_pre[...] = pre
        copy(v_pre, o_pre, outs)
        v_dir[...] = pre + (energy / rho) * d[...]
        copy(v_dir, o_dir, outs)
        for done in outs:
            done.wait()

    return kernel


def call(kernel, specs, outs, out_specs, scratch, sems=0, more=()):
    where = {"s": pltpu.SMEM, "v": pltpu.VMEM, "h": pltpu.HBM}
    if INTERPRET:
        where["h"] = pl.ANY

    def out(x, shape, kind):
        if x == "h" and not INTERPRET:
            return pltpu.HBM(shape, kind)
        return jax.ShapeDtypeStruct(shape, kind)

    run = pl.pallas_call(
        kernel,
        out_shape=[out(x, s, t) for x, (s, t) in zip(out_specs, outs)],
        in_specs=[pl.BlockSpec(memory_space=where[x]) for x in specs],
        out_specs=[pl.BlockSpec(memory_space=where[x]) for x in out_specs],
        scratch_shapes=[pltpu.VMEM(s, t) for s, t in scratch] + ([pltpu.SemaphoreType.DMA((sems,))] if sems else []) + list(more),
        compiler_params=pltpu.CompilerParams(vmem_limit_bytes=40 * 1024 * 1024),
        interpret=INTERPRET,
    )

    def apply(*args):
        if INTERPRET:
            return run(*args)
        return run(*(pltpu.with_memory_space_constraint(a, pltpu.HBM) if x == "h" else a for x, a in zip(specs, args)))

    return apply


def run_copies(sem, pairs):
    todo = []
    for k, (src, dst) in enumerate(pairs):
        todo.append(pltpu.make_async_copy(src, dst, sem.at[k]))
        todo[-1].start()
    for done in todo:
        done.wait()


def edges_kernel(d, r, row_u, row_d, col_l, col_r, sem):
    pairs = []
    for n, at, x in ((DR, 0, d), (RR, DR, r)):
        pairs.append((x.at[pl.ds(0, n), :], row_u.at[pl.ds(at, n), :]))
        pairs.append((x.at[pl.ds(ROWS - n, n), :], row_d.at[pl.ds(at, n), :]))
    for at, x in ((0, d), (128, r)):
        pairs.append((x.at[:, pl.ds(0, 128)], col_l.at[:, pl.ds(at, 128)]))
        pairs.append((x.at[:, pl.ds(COLS - 128, 128)], col_r.at[:, pl.ds(at, 128)]))
    run_copies(sem, pairs)


def corners_kernel(from_u, from_d, cor_l, cor_r):
    for lane, x in ((0, from_u), (128, from_d)):
        cor_l[:, lane : lane + 128] = x[:, 0:128]
        cor_r[:, lane : lane + 128] = x[:, COLS - 128 :]


def solution(mesh):
    n_grp, n_slab, n_col = mesh.shape["grp"], mesh.shape["slab"], mesh.shape["col"]
    n_gc = n_grp * n_col
    n_dev = n_slab * n_col

    def forward(n):
        return [(i, i + 1) for i in range(n - 1)]

    def backward(n):
        return [(i + 1, i) for i in range(n - 1)]

    def body(sol, r, d, row_taps, col_taps, damping, rho, diag, coupling):
        idx = jnp.stack([lax.axis_index("slab"), lax.axis_index(GC)]).astype(jnp.int32)
        row_u, row_d, col_l, col_r = call(
            edges_kernel, "hh", [((DR + RR, COLS), F32)] * 2 + [((ROWS, 256), F32)] * 2, "vvvv", [], 8
        )(d, r)
        from_u = lax.ppermute(row_d, "slab", forward(n_slab))
        from_d = lax.ppermute(row_u, "slab", backward(n_slab))
        from_l = lax.ppermute(col_r, GC, forward(n_gc))
        from_r = lax.ppermute(col_l, GC, backward(n_gc))
        par = (damping[None], rho[None], diag, coupling)
        mat_shapes = [((352, WIN), BF16)] * 2 + [((6, 512, 256), BF16)] * 2
        mat_shapes += [((EXT, 384), BF16), ((384, 256), BF16), ((256, 128), BF16), ((128, 128), BF16)]
        back_shapes = [((384, COLS), BF16), ((256, 384), BF16), ((128, 256), BF16), ((128, 128), BF16)]
        mats = call(
            matrices_kernel(n_slab, n_gc),
            "shh",
            mat_shapes + back_shapes,
            "h" * 12,
            mat_shapes + back_shapes,
            14,
            [pltpu.SMEM((TAPS,), F32)] * 2,
        )(idx, row_taps, col_taps)
        lh, ll, gh, gl, rc0, rc1, rc2, rc3, pc0, pc1, pc2, pc3 = mats
        send_l, send_r = call(corners_kernel, "vv", [((DR + RR, 256), F32)] * 2, "vv", [])(from_u, from_d)
        cor_l = lax.ppermute(send_r, GC, forward(n_gc))
        cor_r = lax.ppermute(send_l, GC, backward(n_gc))
        results = [((ROWS, COLS), F32), ((ROWS, EXT), F32), ((ROWS, EXT), F32)]
        results += [((96, 384), F32), ((48, 256), F32), ((32, 128), F32)]
        q, d2, r1, f0, f1, f2, e_up, e_dn, pay = call(
            halo_kernel(n_slab, n_gc, n_grp),
            "s" * 5 + "hh" + "v" * 6 + "h" * 8,
            results + [((64, COLS + 128), F32)] * 2 + [((n_dev, 384), F32)],
            "h" * 6 + "vvv",
            [((ROWS, EXT), F32)] * 2
            + mat_shapes
            + results
            + [((WIN, EXT), BF16)] * 4
            + [((304, EXT), BF16)] * 2
            + [((128, EXT), BF16)] * 2
            + [((304, EXT), F32)],
            40,
        )(idx, *par, d, r, from_u, from_d, from_l, from_r, cor_l, cor_r, lh, ll, gh, gl, rc0, rc1, rc2, rc3)
        edge_u = lax.ppermute(e_dn, "slab", forward(n_slab))
        edge_d = lax.ppermute(e_up, "slab", backward(n_slab))
        got = lax.all_to_all(pay, ("slab", "col"), 0, 0, tiled=True)
        swap = lax.ppermute(got, "grp", [(i, (i + 1) % n_grp) for i in range(n_grp)])
        tile = ((ROWS, COLS), F32)
        n_sol, n_res, pre, n_dir, energy = call(
            final_kernel(n_slab, n_gc, n_grp),
            "s" * 5 + "vvvv" + "h" * 17,
            [tile] * 4 + [((1, 1), F32)],
            "hhhhv",
            [((ROWS, EXT), F32)] * 2
            + [((128, WIN), BF16)] * 2
            + [((3, 512, 256), BF16)] * 2
            + [tile] * 4
            + [((96, 384), F32), ((48, 256), F32), ((32, 128), F32)]
            + back_shapes
            + [((WIN, EXT), BF16)] * 2
            + [((ROWS, EXT), BF16)] * 2
            + [(((n_slab + 2) * (n_gc + 16), 128), F32), ((ROWS, EXT), F32)]
            + [tile] * 4,
            24,
        )(idx, *par, got, swap, edge_u, edge_d, d2, r1, lh, ll, gh, gl, q, r, d, sol, f0, f1, f2, pc0, pc1, pc2, pc3)
        return n_sol, n_res, pre, n_dir, energy[0, 0]

    tile, rep = P("slab", GC), P()
    return jax.shard_map(
        body,
        mesh=mesh,
        in_specs=(tile,) * 3 + (rep,) * 6,
        out_specs=(tile,) * 4 + (rep,),
        check_vma=False,
    )
```

```python
import jax
import jax.numpy as jnp
from jax import lax
from jax.experimental import pallas as pl
from jax.experimental.pallas import tpu as pltpu
from jax.sharding import PartitionSpec as P


INTERPRET = False
W = 2.0 / 3.0
TAPS = 31
H = TAPS // 2
ROWS, COLS = 128, 1024
EXT = COLS + 256
WIN = ROWS + 128
DR, RR = 64, 32
IN0 = (0, 128, 384, 640, 768)
VARIANT = (0, 1, 1, 1, 2)
GC = ("grp", "col")
F32, BF16 = jnp.float32, jnp.bfloat16


def iota(shape, dim):
    return lax.broadcasted_iota(jnp.int32, shape, dim)


def split(x):
    high = x.astype(BF16)
    return high, (x - high.astype(F32)).astype(BF16)


def dot(a, b):
    return jnp.dot(a, b, preferred_element_type=F32)


def dot3(a, b):
    (ah, al), (bh, bl) = a, b
    return dot(ah, bh) + (dot(ah, bl) + dot(al, bh))


def dot2(a, b):
    return dot(a[0], b) + dot(a[1], b)


def dot2r(a, b):
    return dot(a, b[0]) + dot(a, b[1])


def hot(cond):
    return jnp.where(cond, 1.0, 0.0).astype(BF16)


def total(x):
    return jnp.sum(jnp.sum(x, axis=0, keepdims=True), axis=1, keepdims=True)


def dot_t(a, b):
    def nt(x, y):
        return lax.dot_general(x, y, (((1,), (1,)), ((), ())), preferred_element_type=F32)

    (ah, al), (bh, bl) = a, b
    return nt(ah, bh) + (nt(ah, bl) + nt(al, bh))


def toeplitz(taps):
    sum_taps = taps[0]
    for t in range(1, TAPS):
        sum_taps = sum_taps + taps[t]
    lane = iota((8, 384), 1)
    base = jnp.zeros((8, 384), F32)
    for t in range(TAPS):
        base = jnp.where(lane == 64 + H - t, taps[t], base)
    base = base / jnp.full((8, 384), sum_taps, F32)
    return pltpu.roll(jnp.broadcast_to(base[0:1], (256, 384)), 0, 1, stride=1, stride_axis=0)


def gram(kt, first, limit):
    ks = split(kt)
    left = ks
    if first is not None:
        m = iota((256, 384), 1) + (first - 128)
        left = split(jnp.where((m >= 0) & (m < limit), kt, 0.0))
    return left, ks


def block_powers(kt, first, limit):
    left, ks = gram(kt, first, limit)
    wide = dot_t(left, ks)
    g1 = dot_t(left, (ks[0][64:192], ks[1][64:192]))
    if first is not None:
        i = iota((256, 128), 0) + (first - 64)
        g1 = jnp.where((i >= 0) & (i < limit), g1, 0.0)
    g1s = split(g1)
    return g1s, split(dot3(split(wide), g1s))


def matrices_kernel(n_slab, n_gc):
    def kernel(idx, rt_in, ct_in, *refs):
        outs, scratch, sem, rt, ct = refs[:12], refs[12:24], refs[24], refs[25], refs[26]
        todo = []

        def copy(src, dst):
            todo.append(pltpu.make_async_copy(src, dst, sem.at[len(todo)]))
            todo[-1].start()

        copy(ct_in, ct)
        copy(rt_in, rt)
        lh, ll, gh, gl, rc0, rc1, rc2, rc3, pc0, pc1, pc2, pc3 = scratch
        slab, gc = idx[0], idx[1]
        gh[...], gl[...] = jnp.zeros(gh.shape, BF16), jnp.zeros(gl.shape, BF16)
        todo[0].wait()
        kt = toeplitz(ct)
        inner = block_powers(kt, None, None)
        end = block_powers(kt, jnp.where(gc == 0, 0, gc * COLS + COLS - 128), n_gc * COLS)
        at_l, at_r = gc == 0, gc == n_gc - 1
        has_l = jnp.where(gc > 0, 1.0, 0.0).astype(F32)
        has_r = jnp.where(gc < n_gc - 1, 1.0, 0.0).astype(F32)
        for power in range(2):
            for at, ref in enumerate((gh, gl)):
                mid = inner[power][at]
                wide, other = mid.astype(F32), end[power][at].astype(F32)
                low = jnp.where(at_l, other, wide).astype(BF16)
                high = jnp.where(at_r, other, wide).astype(BF16)
                outer_l, outer_r = (wide * has_l).astype(BF16), (wide * has_r).astype(BF16)
                for v, off, blocks in (
                    (0, 0, (outer_l, low)),
                    (1, 128, (mid, mid)),
                    (2, 256, (high, outer_r)),
                ):
                    for b in range(2):
                        start = off + 128 * b - 64
                        lo, hi = max(0, start), min(512, start + 256)
                        ref[3 * power + v, lo:hi, 128 * b : 128 * b + 128] = blocks[b][lo - start : hi - start]
        for k in (2, 3):
            copy(scratch[k], outs[k])
        first, limit = slab * ROWS, n_slab * ROWS
        todo[1].wait()
        left, ks = gram(toeplitz(rt), first, limit)
        g1 = dot_t(left, ks)
        g1s = split(g1)
        lh[0:128, :], ll[0:128, :] = g1s[0][64:192, :], g1s[1][64:192, :]
        c, i = iota((48, WIN), 0), iota((48, WIN), 1)
        inside = (i + (first - 64) >= 0) & (i + (first - 64) < limit)
        rr = jnp.where((i - 32 >= 4 * c) & (i - 32 < 4 * c + 4) & inside, 0.25, 0.0).astype(BF16)
        lh[128:176, :], ll[128:176, :] = split(dot2r(rr, g1s))
        lh[176:224, :], ll[176:224, :] = rr, jnp.zeros_like(rr)
        k = iota((128, WIN), 1) + (first - 64)
        tile = split(jnp.where((k >= 0) & (k < limit), g1[64:192, :], 0.0))
        lh[224:352, :], ll[224:352, :] = split(dot3(tile, g1s))
        for k in (0, 1):
            copy(scratch[k], outs[k])
        rc0[...] = hot((iota((EXT, 384), 0) >> 2) + 32 == iota((EXT, 384), 1))
        rc1[...] = hot((iota((384, 256), 0) >> 1) == iota((384, 256), 1))
        rc2[...] = hot((iota((256, 128), 0) >> 1) == iota((256, 128), 1))
        rc3[...] = hot((iota((128, 128), 0) >> 1) - 8 == (iota((128, 128), 1) & 31))
        pc0[...] = hot(iota((384, COLS), 0) == (iota((384, COLS), 1) >> 2) + 64)
        pc1[...] = hot(iota((256, 384), 0) == (iota((256, 384), 1) >> 1))
        pc2[...] = hot(iota((128, 256), 0) == (iota((128, 256), 1) >> 1))
        pc3[...] = hot(iota((128, 128), 0) == (iota((128, 128), 1) >> 1))
        for k in range(4, 12):
            copy(scratch[k], outs[k])
        for done in todo[2:]:
            done.wait()

    return kernel


def level_mask(level, shape, slab, gc, n_slab, n_gc):
    height, width = 32 >> level, 256 >> level
    i = iota(shape, 0) - (8 >> level) + slab * height
    j = iota(shape, 1) - (64 >> level) + gc * width
    return (i >= 0) & (i < n_slab * height) & (j >= 0) & (j < n_gc * width)


def tile_mask(level, shape):
    i, j = iota(shape, 0) - (8 >> level), iota(shape, 1) - (64 >> level)
    return (i >= 0) & (i < 32 >> level) & (j >= 0) & (j < 256 >> level)


def beside(v):
    n, m = v.shape
    rows = pltpu.roll(v, 1, 0) + pltpu.roll(v, n - 1, 0)
    return rows + pltpu.roll(v, 1, 1) + pltpu.roll(v, m - 1, 1)


def operator(v, dg, cp):
    return dg * v - cp * beside(v)


def halo_kernel(n_slab, n_gc):
    n_dev = n_slab * n_gc

    def kernel(idx, damping, rho_in, diag, coupling, d_in, r_in, row_u, row_d, col_l, col_r, cor_l, cor_r,
               lh_in, ll_in, gh_in, gl_in, rc0_in, rc1_in, rc2_in, rc3_in,
               q_out, d2_out, r1_out, f0_out, f1_out, f2_out, e_up, e_dn, pay,
               d, r, lh, ll, gh, gl, rc0, rc1, rc2, rc3, q, d2, r1, f0, f1, f2,
               dh, dl, rh, rl, sh, sl, th, tl, c1, sem):
        slab, gc = idx[0], idx[1]
        delta = damping[0]
        c = W / (1.0 + delta)
        ins, outs = [], []

        def copy(src, dst, todo):
            done = pltpu.make_async_copy(src, dst, sem.at[len(ins) + len(outs)])
            done.start()
            todo.append(done)

        for ref, main in ((d, d_in), (r, r_in)):
            copy(main, ref.at[:, pl.ds(128, COLS)], ins)
        for src, dst in ((lh_in, lh), (ll_in, ll), (gh_in, gh), (gl_in, gl), (rc0_in, rc0), (rc1_in, rc1), (rc2_in, rc2), (rc3_in, rc3)):
            copy(src, dst, ins)

        def put(hi_ref, lo_ref, r0, c0, x):
            hi, lo = split(x)
            hi_ref[r0 : r0 + x.shape[0], c0 : c0 + x.shape[1]] = hi
            lo_ref[r0 : r0 + x.shape[0], c0 : c0 + x.shape[1]] = lo

        zero = jnp.zeros((32, EXT), BF16)
        for ref in (rh, rl):
            ref[0:32, :] = zero
            ref[WIN - 32 : WIN, :] = zero
        for at, n, ref, hi, lo in ((0, DR, d, dh, dl), (1, RR, r, rh, rl)):
            cols = slice(128 * at, 128 * at + 128)
            rows = slice(DR * at, DR * at + n)
            ref[:, 0:128] = col_l[:, cols]
            ref[:, 128 + COLS :] = col_r[:, cols]
            for first, lane, main in ((64 - n, 0, row_u), (192, 128, row_d)):
                put(hi, lo, first, 128, main[rows, :])
                put(hi, lo, first, 0, cor_l[rows, lane : lane + 128])
                put(hi, lo, first, 128 + COLS, cor_r[rows, lane : lane + 128])
            ins[at].wait()
            put(hi, lo, 64, 0, ref[...])
        for done in ins[2:4]:
            done.wait()
        ds, rs = (dh[...], dl[...]), (rh[...], rl[...])

        def left(a, b):
            return (lh[a:b, :], ll[a:b, :])

        put(sh, sl, 0, 0, dot3(left(0, 176), ds))
        put(sh, sl, 176, 0, dot3(left(0, 128), rs))
        put(th, tl, 0, 0, dot3(left(224, 352), ds))
        rd = dot2r(lh[176:224, :], ds)
        rres = dot2r(lh[176:224, :], rs)
        for done in ins[4:]:
            done.wait()
        for g in range(5):
            a, v, o = IN0[g], VARIANT[g], slice(256 * g, 256 * g + 256)
            c1[:, o] = dot3((sh[:, a : a + 512], sl[:, a : a + 512]), (gh[v], gl[v]))
        sums_of = []

        def coarse():
            fq = c1[128:176, :] + delta * rd
            f = dot2(split(jnp.concatenate([fq, rres], axis=0)), rc0[...])
            f0[...] = f
            yield None
            pair = (f[0:48], f[48:96])
            weight = 4.0
            for level, cols in ((0, rc1), (1, rc2), (2, rc3)):
                dg, cp = diag[level], coupling[level]
                sm = W / dg
                shape = pair[0].shape
                inside = level_mask(level, shape, slab, gc, n_slab, n_gc)
                mine = tile_mask(level, shape)
                bq, br = operator(pair[0], dg, cp), operator(pair[1], dg, cp)
                rest_q = jnp.where(inside, pair[0] - sm * bq, 0.0)
                rest_r = jnp.where(inside, pair[1] - sm * br, 0.0)
                low = dot2(split(jnp.concatenate([rest_q, rest_r], axis=0)), cols[...])
                own_q, own_r = jnp.where(mine, pair[0], 0.0), jnp.where(mine, pair[1], 0.0)
                sums_of.append(
                    (
                        weight * total(own_r * (2.0 * sm * pair[1] - (sm * sm) * br)),
                        weight * total(own_q * (2.0 * sm * pair[0] - (sm * sm) * bq)),
                        weight * total(own_r * (2.0 * sm * pair[0] - (sm * sm) * bq)),
                    )
                )
                weight = 2.0 * weight
                if level < 2:
                    yield None
                    n, m = (24, 48) if level == 0 else (16, 24)
                    half = jnp.where((iota((n, m), 1) >> 1) == iota((n, m), 0), 0.5, 0.0).astype(BF16)
                    pair = (dot2r(half, split(low[0:m])), dot2r(half, split(low[m : 2 * m])))
                    keep = level_mask(level + 1, pair[0].shape, slab, gc, n_slab, n_gc)
                    pair = (jnp.where(keep, pair[0], 0.0), jnp.where(keep, pair[1], 0.0))
                    out = (f1, f2)[level]
                    out[0:n, :], out[n : 2 * n, :] = pair
                    yield None
            yield pair, low

        steps = coarse()
        last = next(steps)
        for g in range(5):
            a, v, o = IN0[g], VARIANT[g], slice(256 * g, 256 * g + 256)
            d2[:, o] = dot3((th[:, a : a + 512], tl[:, a : a + 512]), (gh[3 + v], gl[3 + v]))
            last = next(steps)
        pair, low = last
        t = slice(128, 128 + COLS)
        p1 = c1[0:128, :]
        q[...] = c1[0:128, t] + delta * d[:, t]
        d2[...] = d2[...] + delta * (2.0 * p1 + delta * d[...])
        r1[...] = c1[176:304, :] + delta * r[...]
        copy(q, q_out, outs)
        copy(d2, d2_out, outs)
        copy(r1, r1_out, outs)
        near = iota((32, 128), 1) < 64
        for ref, rows in ((e_dn, slice(96, 128)), (e_up, slice(0, 32))):
            for at, x in ((0, d2), (32, r1)):
                ref[at : at + 32, 0:COLS] = x[rows, t]
                ref[at : at + 32, COLS:] = jnp.where(near, x[rows, 128 + COLS :], x[rows, 0:128])
        qv, rv, aq, ar = q[...], r[:, t], d2[:, t], r1[:, t]
        s_dq = total(d[:, t] * qv)
        e_rr = total(rv * (3.0 * rv - 3.0 * c * ar) + c * c * (ar * ar)) * c
        e_qq = total(qv * (3.0 * qv - 3.0 * c * aq) + c * c * (aq * aq)) * c
        e_rq = total(rv * (3.0 * qv - 3.0 * c * aq) + c * c * (ar * aq)) * c
        for x, y, z in sums_of:
            e_rr, e_qq, e_rq = e_rr + x, e_qq + y, e_rq + z
        for ref, to, first in ((e_up, 30, 2), (e_dn, 0, 8)):
            for at, x in ((0, pair[0]), (32, pair[1])):
                ref[at + to : at + to + 2, 0:128] = x[first : first + 2, :]
        for src, dst in ((f0, f0_out), (f1, f1_out), (f2, f2_out)):
            copy(src, dst, outs)
        i, lane = iota((16, 128), 0), iota((16, 128), 1)
        pick = (i >= 2) & (i < 10) & (((i - 2) >> 1) == (lane >> 5))
        gq = jnp.sum(jnp.where(pick, low[0:16], 0.0), axis=0, keepdims=True) * 0.5
        gr = jnp.sum(jnp.where(pick, low[16:32], 0.0), axis=0, keepdims=True) * 0.5
        lane = iota((1, 128), 1)
        sums = jnp.zeros((1, 128), F32)
        for k, x in enumerate((s_dq, e_rr, e_rq, e_qq)):
            sums = jnp.where(lane == k, x, sums)
        pay[:, 0:128] = jnp.broadcast_to(gq, (n_dev, 128))
        pay[:, 128:256] = jnp.broadcast_to(gr, (n_dev, 128))
        pay[:, 256:384] = jnp.broadcast_to(sums, (n_dev, 128))
        for done in outs:
            done.wait()

    return kernel


def final_kernel(n_slab, n_gc, n_grp):
    n_col = n_gc // n_grp

    def kernel(idx, damping, rho_in, diag, coupling, got, e_u, e_d, d2_in, r1_in, lh_in, ll_in, gh_in, gl_in, q_in, r_in, d_in, sol_in,
               f0_in, f1_in, f2_in, pc0_in, pc1_in, pc2_in, pc3_in,
               o_sol, o_res, o_pre, o_dir, o_energy,
               d2, r1, lh, ll, gh, gl, q, r, d, sol, f0, f1, f2, pc0, pc1, pc2, pc3,
               uh, ul, yh, yl, vs, kk, v_sol, v_res, v_pre, v_dir, sem):
        ins, outs = [], []

        def copy(src, dst, todo):
            done = pltpu.make_async_copy(src, dst, sem.at[len(ins) + len(outs)])
            done.start()
            todo.append(done)

        for src, dst in (
            (d2_in, d2), (r1_in, r1), (lh_in.at[pl.ds(0, 128), :], lh), (ll_in.at[pl.ds(0, 128), :], ll),
            (gh_in.at[pl.ds(0, 3)], gh), (gl_in.at[pl.ds(0, 3)], gl), (r_in, r), (q_in, q), (sol_in, sol), (d_in, d),
            (f0_in, f0), (f1_in, f1), (f2_in, f2), (pc1_in, pc1), (pc2_in, pc2), (pc3_in, pc3), (pc0_in, pc0),
        ):
            copy(src, dst, ins)
        slab, gc = idx[0], idx[1]
        delta, rho = damping[0], rho_in[0]
        c = W / (1.0 + delta)
        lane = iota((1, 128), 1)
        sums = jnp.sum(got[:, 256:384], axis=0, keepdims=True)
        s_dq, e_rr, e_rq, e_qq = (
            jnp.sum(jnp.where(lane == k, sums, 0.0), axis=1, keepdims=True) for k in range(4)
        )
        alpha = rho / s_dq
        dg, cp = diag[3], coupling[3]
        first = (iota((n_gc, 128), 1) & 31) == 0
        last = (iota((n_gc, 128), 1) & 31) == 31
        top, bottom = iota((n_gc, 128), 1) < 32, iota((n_gc, 128), 1) >= 96
        left_end, right_end = iota((n_gc, 128), 0) == 0, iota((n_gc, 128), 0) == n_gc - 1
        rhs = []
        for s in range(n_slab):
            rows = []
            for g in range(n_grp):
                at = (g * n_slab + s) * n_col
                rows.append(got[at : at + n_col, 128:256] - alpha * got[at : at + n_col, 0:128])
            rhs.append(jnp.concatenate(rows, axis=0))
        zero = jnp.zeros((n_gc, 128), F32)
        v = [W * x / dg for x in rhs]
        for _ in range(3):
            ups = [pltpu.roll(x, 32, 1) for x in v]
            downs = [pltpu.roll(x, 96, 1) for x in v]
            new = []
            for s in range(n_slab):
                x = v[s]
                low = jnp.where(left_end, 0.0, pltpu.roll(pltpu.roll(x, 97, 1), 1, 0))
                high = jnp.where(right_end, 0.0, pltpu.roll(pltpu.roll(x, 31, 1), n_gc - 1, 0))
                beside_x = jnp.where(first, low, pltpu.roll(x, 1, 1))
                beside_x = beside_x + jnp.where(last, high, pltpu.roll(x, 127, 1))
                beside_x = beside_x + jnp.where(top, ups[s - 1] if s > 0 else zero, ups[s])
                beside_x = beside_x + jnp.where(bottom, downs[s + 1] if s < n_slab - 1 else zero, downs[s])
                new.append(x + W * (rhs[s] - (dg * x - cp * beside_x)) / dg)
            v = new
        e3 = total(sum(a * b for a, b in zip(rhs, v)))
        energy = e_rr - alpha * (2.0 * e_rq) + (alpha * alpha) * e_qq + 32.0 * e3
        o_energy[...] = energy
        pitch = n_gc + 16
        vs[...] = jnp.zeros(vs.shape, F32)
        for s in range(n_slab):
            at = (s + 1) * pitch + 8
            vs[at : at + n_gc, :] = v[s]
        v3 = jnp.zeros((8, 128), F32)
        lanes, rows8 = iota((1, 128), 1), iota((8, 128), 0)
        for k, i in ((-1, 3), (0, 0), (0, 1), (0, 2), (0, 3), (1, 0)):
            at = (slab + 1 + k) * pitch + 8 + gc
            mid, lo, hi = (vs[pl.ds(at + x, 1), :] for x in (0, -1, 1))
            line = pltpu.roll(mid, (8 - 32 * i) % 128, 1)
            line = jnp.where(lanes == 7, pltpu.roll(lo, (8 - 32 * i - 32) % 128, 1), line)
            line = jnp.where(lanes == 40, pltpu.roll(hi, (8 - 32 * i + 32) % 128, 1), line)
            line = jnp.where((lanes >= 7) & (lanes <= 40), line, 0.0)
            v3 = jnp.where(rows8 == 4 * k + i + 1, line, v3)
        for ref in (uh, ul):
            ref[0:32, :] = jnp.zeros((32, EXT), BF16)
            ref[WIN - 32 : WIN, :] = jnp.zeros((32, EXT), BF16)
        for done in ins[:4]:
            done.wait()
        near = iota((32, 128), 1) < 64
        for at, x, spare in ((32, e_u, 0), (192, e_d, 30)):
            edge = x[32:64, :] - alpha * x[0:32, :]
            place = iota((32, COLS + 128), 0)
            edge = jnp.where((place == spare) | (place == spare + 1), 0.0, edge)
            side = edge[:, COLS:]
            for first, part in ((128, edge[:, 0:COLS]), (0, jnp.where(near, 0.0, side)), (128 + COLS, jnp.where(near, side, 0.0))):
                hi, lo = split(part)
                uh[at : at + 32, first : first + part.shape[1]] = hi
                ul[at : at + 32, first : first + part.shape[1]] = lo
        uh[64:192, :], ul[64:192, :] = split(r1[...] - alpha * d2[...])
        yh[...], yl[...] = split(dot3((lh[...], ll[...]), (uh[...], ul[...])))
        for done in ins[4:19]:
            done.wait()
        v_res[...] = r[...] - alpha * q[...]
        copy(v_res, o_res, outs)
        v_sol[...] = sol[...] + alpha * d[...]
        copy(v_sol, o_sol, outs)
        edge_u = e_u[32:34, 0:128] - alpha * e_u[0:2, 0:128]
        edge_d = e_d[62:64, 0:128] - alpha * e_d[30:32, 0:128]
        own = f2[16:32, :] - alpha * f2[0:16, :]
        row = iota((16, 128), 0)
        own = jnp.where(row == 0, edge_u[0:1, :], jnp.where(row == 1, edge_u[1:2, :], own))
        own = jnp.where(row == 10, edge_d[0:1, :], jnp.where(row == 11, edge_d[1:2, :], own))
        own = jnp.where(row < 12, own, 0.0)
        f = [f0[48:96, :] - alpha * f0[0:48, :], f1[24:48, :] - alpha * f1[0:24, :], own]

        def upwards():
            low = v3
            for level, cols in ((2, pc3), (1, pc2), (0, pc1)):
                dg, cp = diag[level], coupling[level]
                sm = W / dg
                n, m = f[level].shape[0], low.shape[0]
                double = hot((iota((n, m), 0) >> 1) == iota((n, m), 1))
                wide = dot2r(double, split(dot2(split(low), cols[...])))
                inside = level_mask(level, f[level].shape, slab, gc, n_slab, n_gc)
                x = jnp.where(inside, sm * f[level] + wide, 0.0)
                low = jnp.where(inside, x + sm * (f[level] - operator(x, dg, cp)), 0.0)
                if level > 0:
                    yield None
            four = hot((iota((ROWS, 48), 0) >> 2) + 8 == iota((ROWS, 48), 1))
            yield split(dot2r(four, split(low)))

        steps = upwards()
        for g in range(5):
            a, v, o = IN0[g], VARIANT[g], slice(256 * g, 256 * g + 256)
            kk[:, o] = dot3((yh[:, a : a + 512], yl[:, a : a + 512]), (gh[v], gl[v]))
            if g in (0, 2, 4):
                spread = next(steps)
        t = slice(128, 128 + COLS)
        au = r1[:, t] - alpha * d2[:, t]
        smooth = c * (3.0 * v_res[...] - (3.0 * c) * au + (c * c) * (kk[:, t] + delta * au))
        pre = smooth + dot2(spread, pc0[...])
        v_pre[...] = pre
        copy(v_pre, o_pre, outs)
        v_dir[...] = pre + (energy / rho) * d[...]
        copy(v_dir, o_dir, outs)
        for done in outs:
            done.wait()

    return kernel


def call(kernel, specs, outs, out_specs, scratch, sems=0, more=()):
    where = {"s": pltpu.SMEM, "v": pltpu.VMEM, "h": pltpu.HBM}
    if INTERPRET:
        where["h"] = pl.ANY

    def out(x, shape, kind):
        if x == "h" and not INTERPRET:
            return pltpu.HBM(shape, kind)
        return jax.ShapeDtypeStruct(shape, kind)

    run = pl.pallas_call(
        kernel,
        out_shape=[out(x, s, t) for x, (s, t) in zip(out_specs, outs)],
        in_specs=[pl.BlockSpec(memory_space=where[x]) for x in specs],
        out_specs=[pl.BlockSpec(memory_space=where[x]) for x in out_specs],
        scratch_shapes=[pltpu.VMEM(s, t) for s, t in scratch] + ([pltpu.SemaphoreType.DMA((sems,))] if sems else []) + list(more),
        compiler_params=pltpu.CompilerParams(vmem_limit_bytes=40 * 1024 * 1024),
        interpret=INTERPRET,
    )

    def apply(*args):
        if INTERPRET:
            return run(*args)
        return run(*(pltpu.with_memory_space_constraint(a, pltpu.HBM) if x == "h" else a for x, a in zip(specs, args)))

    return apply


def run_copies(sem, pairs):
    todo = []
    for k, (src, dst) in enumerate(pairs):
        todo.append(pltpu.make_async_copy(src, dst, sem.at[k]))
        todo[-1].start()
    for done in todo:
        done.wait()


def edges_kernel(d, r, row_u, row_d, col_l, col_r, sem):
    pairs = []
    for n, at, x in ((DR, 0, d), (RR, DR, r)):
        pairs.append((x.at[pl.ds(0, n), :], row_u.at[pl.ds(at, n), :]))
        pairs.append((x.at[pl.ds(ROWS - n, n), :], row_d.at[pl.ds(at, n), :]))
    for at, x in ((0, d), (128, r)):
        pairs.append((x.at[:, pl.ds(0, 128)], col_l.at[:, pl.ds(at, 128)]))
        pairs.append((x.at[:, pl.ds(COLS - 128, 128)], col_r.at[:, pl.ds(at, 128)]))
    run_copies(sem, pairs)


def corners_kernel(from_u, from_d, cor_l, cor_r):
    for lane, x in ((0, from_u), (128, from_d)):
        cor_l[:, lane : lane + 128] = x[:, 0:128]
        cor_r[:, lane : lane + 128] = x[:, COLS - 128 :]


def solution(mesh):
    n_grp, n_slab, n_col = mesh.shape["grp"], mesh.shape["slab"], mesh.shape["col"]
    n_gc = n_grp * n_col
    n_dev = n_slab * n_gc

    def forward(n):
        return [(i, i + 1) for i in range(n - 1)]

    def backward(n):
        return [(i + 1, i) for i in range(n - 1)]

    def body(sol, r, d, row_taps, col_taps, damping, rho, diag, coupling):
        idx = jnp.stack([lax.axis_index("slab"), lax.axis_index(GC)]).astype(jnp.int32)
        row_u, row_d, col_l, col_r = call(
            edges_kernel, "hh", [((DR + RR, COLS), F32)] * 2 + [((ROWS, 256), F32)] * 2, "vvvv", [], 8
        )(d, r)
        from_u = lax.ppermute(row_d, "slab", forward(n_slab))
        from_d = lax.ppermute(row_u, "slab", backward(n_slab))
        from_l = lax.ppermute(col_r, GC, forward(n_gc))
        from_r = lax.ppermute(col_l, GC, backward(n_gc))
        par = (damping[None], rho[None], diag, coupling)
        mat_shapes = [((352, WIN), BF16)] * 2 + [((6, 512, 256), BF16)] * 2
        mat_shapes += [((EXT, 384), BF16), ((384, 256), BF16), ((256, 128), BF16), ((128, 128), BF16)]
        back_shapes = [((384, COLS), BF16), ((256, 384), BF16), ((128, 256), BF16), ((128, 128), BF16)]
        mats = call(
            matrices_kernel(n_slab, n_gc),
            "shh",
            mat_shapes + back_shapes,
            "h" * 12,
            mat_shapes + back_shapes,
            14,
            [pltpu.SMEM((TAPS,), F32)] * 2,
        )(idx, row_taps, col_taps)
        lh, ll, gh, gl, rc0, rc1, rc2, rc3, pc0, pc1, pc2, pc3 = mats
        send_l, send_r = call(corners_kernel, "vv", [((DR + RR, 256), F32)] * 2, "vv", [])(from_u, from_d)
        cor_l = lax.ppermute(send_r, GC, forward(n_gc))
        cor_r = lax.ppermute(send_l, GC, backward(n_gc))
        results = [((ROWS, COLS), F32), ((ROWS, EXT), F32), ((ROWS, EXT), F32)]
        results += [((96, 384), F32), ((48, 256), F32), ((32, 128), F32)]
        q, d2, r1, f0, f1, f2, e_up, e_dn, pay = call(
            halo_kernel(n_slab, n_gc),
            "s" * 5 + "hh" + "v" * 6 + "h" * 8,
            results + [((64, COLS + 128), F32)] * 2 + [((n_dev, 384), F32)],
            "h" * 6 + "vvv",
            [((ROWS, EXT), F32)] * 2
            + mat_shapes
            + results
            + [((WIN, EXT), BF16)] * 4
            + [((304, EXT), BF16)] * 2
            + [((128, EXT), BF16)] * 2
            + [((304, EXT), F32)],
            40,
        )(idx, *par, d, r, from_u, from_d, from_l, from_r, cor_l, cor_r, lh, ll, gh, gl, rc0, rc1, rc2, rc3)
        edge_u = lax.ppermute(e_dn, "slab", forward(n_slab))
        edge_d = lax.ppermute(e_up, "slab", backward(n_slab))
        got = lax.all_to_all(pay, ("grp", "slab", "col"), 0, 0, tiled=True)
        tile = ((ROWS, COLS), F32)
        n_sol, n_res, pre, n_dir, energy = call(
            final_kernel(n_slab, n_gc, n_grp),
            "s" * 5 + "vvv" + "h" * 17,
            [tile] * 4 + [((1, 1), F32)],
            "hhhhv",
            [((ROWS, EXT), F32)] * 2
            + [((128, WIN), BF16)] * 2
            + [((3, 512, 256), BF16)] * 2
            + [tile] * 4
            + [((96, 384), F32), ((48, 256), F32), ((32, 128), F32)]
            + back_shapes
            + [((WIN, EXT), BF16)] * 2
            + [((ROWS, EXT), BF16)] * 2
            + [(((n_slab + 2) * (n_gc + 16), 128), F32), ((ROWS, EXT), F32)]
            + [tile] * 4,
            24,
        )(idx, *par, got, edge_u, edge_d, d2, r1, lh, ll, gh, gl, q, r, d, sol, f0, f1, f2, pc0, pc1, pc2, pc3)
        return n_sol, n_res, pre, n_dir, energy[0, 0]

    tile, rep = P("slab", GC), P()
    return jax.shard_map(
        body,
        mesh=mesh,
        in_specs=(tile,) * 3 + (rep,) * 6,
        out_specs=(tile,) * 4 + (rep,),
        check_vma=False,
    )
```
